128 devices in a mesh: curve: 128 (over y, z, x, core).
Axes of the slice: x: 4, y: 4, z: 4, core: 2. Of those that a mesh axis runs over, the one named last changes fastest.
Arguments:
- nodal_state: float32 [5, 64, 65536], P(None, None, 'curve'), may hold values from -9 to 9, as said below
- inverse_jacobian: float32 [65536], P('curve'), may hold values from 1 to 4
- speeds: float32 [3, 5], replicated, may hold values from -1.5 to 1.5
- refine_flags: int32 [65536], P('curve'), may hold values from 0 to 1, as said below
- send_index: int32 [49152], P('curve'), may hold values from 0 to 3071, as said below
- face_source: int32 [6, 65536], P(None, 'curve'), may hold values from 0 to 3455, as said below
Outputs:
- refined_state: float32 [5, 64, 122880], P(None, None, 'curve')
- refined_jacobian: float32 [122880], P('curve')
The draws below stay inside these ranges and needn't reach their ends.
Inputs may be any that keep to these rules, and one draw needn't show every extreme that they name: `nodal_state`: each element's 64 node values are a level plus a linear part plus noise of an amplitude that varies from element to element. `refine_flags`: exactly 64 flags per device on average over all devices, at most 128 on one device, a number that is reached; the refined elements of a device go only to itself and its two curve neighbours, at most 224 to each neighbour, a number that is reached. `send_index`: per device, four blocks of 96 entries for destination offsets -2, -1, 1, 2 along the curve (cyclically): entries f * 512 + n of the traces that device reads, in increasing order, then zeros in unused slots; the blocks for offsets -1 and 1 are always full. `face_source`: face pairing is symmetric: across face 2 d of an element lies face 2 d + 1 of its neighbour; neighbours are on the same device or on one within two curve offsets.
All inputs are finite; a program needn't handle non-finite values.
Results may differ from the reference program's by a relative error of at most 0.0003.
Values sent between devices are 32-bit elements; how exact they have to be, the bound alone decides.
A program may use at most 64 MiB of HBM per device.

```python
import math
import jax
import jax.numpy as jnp
import numpy as np
from jax import lax

VARS = 5
E_DEV = 512
FLAG_DEV = 64
HALO_W = 16
HALO_SLOTS = 96
ELEMS = 65536
NEW_ELEMS = 122880
N_CURVE = 128


def random_orders(key, count_rows, length):
    return jax.vmap(lambda single: jax.random.permutation(single, length))(jax.random.split(key, count_rows)).astype(jnp.int32)


def band_offsets(key, length, band_width):
    far_counts = jax.random.randint(key, (2,), 1, band_width + 1).astype(jnp.int32)
    edge_one = far_counts[0]
    edge_two = edge_one + band_width
    edge_three = edge_two + band_width
    edge_four = edge_three + far_counts[1]
    ranks = jnp.arange(length, dtype=jnp.int32)
    return jnp.where(ranks < edge_one, -2, jnp.where(ranks < edge_two, -1, jnp.where(ranks < edge_three, 1, jnp.where(ranks < edge_four, 2, 0)))).astype(jnp.int32)


def offset_slot(offset):
    return jnp.where(offset < 0, offset + 2, offset + 1).astype(jnp.int32)


def forest_tables(key):
    devices = N_CURVE
    elements = E_DEV
    slot_count = HALO_SLOTS
    base_key = jax.random.fold_in(key, 11)
    device_ids = jnp.arange(devices, dtype=jnp.int32)[:, None]
    neighbours = []
    for direction in range(3):
        dir_key = jax.random.fold_in(base_key, direction)
        first_key, second_key, band_key = jax.random.split(dir_key, 3)
        first = random_orders(first_key, devices, elements)
        second = random_orders(second_key, devices, elements)
        first_inverse = jnp.argsort(first, axis=1).astype(jnp.int32)
        second_inverse = jnp.argsort(second, axis=1).astype(jnp.int32)
        bands = band_offsets(band_key, elements, HALO_W)
        ahead = bands[first]
        target = (device_ids + ahead) % devices
        forward = target * elements + second[target, first]
        behind = bands[second_inverse]
        anchor = (device_ids - behind) % devices
        backward = anchor * elements + first_inverse[anchor, second_inverse]
        neighbours.append(forward)
        neighbours.append(backward)
    near_ids = jnp.stack(neighbours).astype(jnp.int32)
    owner = near_ids // elements
    relative = (owner - device_ids[None] + 2) % devices - 2
    slot_of = jnp.where(relative == 0, 4, offset_slot(relative)).astype(jnp.int32)
    flat_slot = jnp.transpose(slot_of, (1, 0, 2)).reshape(devices, 6 * elements)
    flat_ids = jnp.arange(6 * elements, dtype=jnp.int32)[None, :]
    sort_keys = flat_slot * (6 * elements) + flat_ids
    ordering = jnp.argsort(sort_keys, axis=1).astype(jnp.int32)
    position = jnp.argsort(ordering, axis=1).astype(jnp.int32)
    starts = jnp.stack([jnp.sum(flat_slot < block, axis=1) for block in range(4)], axis=1).astype(jnp.int32)
    counts = jnp.stack([jnp.sum(flat_slot == block, axis=1) for block in range(4)], axis=1).astype(jnp.int32)
    lanes = jnp.arange(slot_count, dtype=jnp.int32)
    picks = jnp.minimum(starts[:, :, None] + lanes[None, None, :], 6 * elements - 1)
    sent = jnp.take_along_axis(ordering, picks.reshape(devices, 4 * slot_count), axis=1).reshape(devices, 4, slot_count)
    sent = jnp.where(lanes[None, None, :] < counts[:, :, None], sent, 0).astype(jnp.int32)
    faces = jnp.arange(6, dtype=jnp.int32)[:, None, None]
    partner = faces + 1 - 2 * (faces % 2)
    sender_flat = partner * elements + near_ids % elements
    rank_at = position[owner, sender_flat] - starts[owner, offset_slot(-relative)]
    ghost_index = 6 * elements + offset_slot(relative) * slot_count + rank_at
    source = jnp.where(relative == 0, sender_flat, ghost_index).astype(jnp.int32)
    return (sent.reshape(-1), source.reshape(6, devices * elements))


def draw_send_index(key, part):
    return forest_tables(key)[0]


def draw_face_source(key, part):
    return forest_tables(key)[1]


def draw_refine_flags(key, part):
    devices = N_CURVE
    elements = E_DEV
    half_flags = FLAG_DEV // 2
    drift_key, spot_key, order_key = jax.random.split(jax.random.fold_in(key, 5), 3)
    drift_by = jax.random.randint(drift_key, (devices,), -half_flags, half_flags + 1).astype(jnp.int32)
    spot_at = jax.random.randint(spot_key, (), 1, devices - 1).astype(jnp.int32)
    device_ids = jnp.arange(devices, dtype=jnp.int32)
    drift_by = jnp.where(device_ids == spot_at - 1, -half_flags, drift_by)
    drift_by = jnp.where(device_ids == spot_at, half_flags, drift_by)
    drift_by = jnp.where(device_ids == devices - 1, 0, drift_by).astype(jnp.int32)
    before = jnp.concatenate([jnp.zeros((1,), jnp.int32), drift_by[:-1]])
    counts = FLAG_DEV + drift_by - before
    orders = random_orders(order_key, devices, elements)
    return (orders < counts[:, None]).astype(jnp.int32).reshape(-1)


def draw_nodal_state(key, part):
    first_key, second_key, third_key, fourth_key = jax.random.split(jax.random.fold_in(key, 3), 4)
    element_total = ELEMS
    root = 1.0 / math.sqrt(5.0)
    points = jnp.array([-1.0, -root, root, 1.0], jnp.float32)
    node_ids = jnp.arange(64, dtype=jnp.int32)
    node_positions = jnp.stack([points[node_ids % 4], points[node_ids // 4 % 4], points[node_ids // 16]])
    level = 0.6 * jax.random.truncated_normal(first_key, -3.0, 3.0, (5, 1, element_total), jnp.float32)
    gradient_slopes = 0.4 * jax.random.truncated_normal(second_key, -3.0, 3.0, (5, 3, element_total), jnp.float32)
    incline_factor = jnp.einsum('whz,hq->wqz', gradient_slopes, node_positions)
    rough = jnp.exp(jax.random.uniform(third_key, (1, 1, element_total), jnp.float32, math.log(0.03), 0.0))
    noise = jax.random.truncated_normal(fourth_key, -3.0, 3.0, (5, 64, element_total), jnp.float32)
    return (level + incline_factor + rough * noise).astype(jnp.float32)


def level_of(rng, shape, cuts, smallest, top_value):
    def one(dim, parts):
        draws = jax.random.uniform(jax.random.fold_in(jax.random.fold_in(rng, 6), dim), (parts,), jnp.float32, smallest / len(cuts), top_value / len(cuts))
        return jnp.repeat(jnp.exp(draws), shape[dim] // parts).reshape((-1,) + (1,) * (len(shape) - dim - 1))

    level = one(*cuts[0])
    for cut in cuts[1:]:
        level = level * one(*cut)
    return level


def setup_inputs(seed: int = 0) -> dict:
    streams_of = jax.random.split(jax.random.key(seed), 7)
    return {
        "nodal_state": draw_nodal_state(jax.random.fold_in(streams_of[6], 71), 0),
        "inverse_jacobian": jnp.clip(jnp.exp(math.log(4.0) - 1.3862944 * jax.random.uniform(streams_of[1], (ELEMS,), jnp.float32) ** level_of(streams_of[1], (ELEMS,), ((0, 128),), -0.2, 0.2)), 1.0, 4.0),
        "speeds": jnp.clip(jax.random.uniform(streams_of[2], (3, VARS), jnp.float32, -1.5, 1.5), -1.5, 1.5),
        "refine_flags": draw_refine_flags(jax.random.fold_in(streams_of[6], 71), 0),
        "send_index": draw_send_index(jax.random.fold_in(streams_of[6], 71), 0),
        "face_source": draw_face_source(jax.random.fold_in(streams_of[6], 71), 0),
    }


time_step = 0.02

def lagrange_at(points, targets):
    values_at = np.ones((len(targets), 4))
    for basis_id in range(4):
        for partner in range(4):
            if partner != basis_id:
                values_at[:, basis_id] *= (targets - points[partner]) / (points[basis_id] - points[partner])
    return values_at

def modes_table(points):
    mono_to_legendre = np.array([[1.0, 0.0, 0.0, 0.0], [0.0, 1.0, 0.0, 0.0], [1.0 / 3.0, 0.0, 2.0 / 3.0, 0.0], [0.0, 0.6, 0.0, 0.4]])
    table = np.zeros((4, 4))
    for basis_id in range(4):
        coef = [1.0, 0.0, 0.0, 0.0]
        for partner in range(4):
            if partner != basis_id:
                denom = points[basis_id] - points[partner]
                fresh = [0.0, 0.0, 0.0, 0.0]
                for power in range(4):
                    lower = coef[power - 1] if power > 0 else 0.0
                    fresh[power] = (lower - points[partner] * coef[power]) / denom
                coef = fresh
        legendre = np.zeros(4)
        for power in range(4):
            legendre = legendre + coef[power] * mono_to_legendre[power]
        table[:, basis_id] = legendre
    return table

def node_constants():
    root = 1.0 / math.sqrt(5.0)
    points = np.array([-1.0, -root, root, 1.0])
    weights = np.array([1.0, 5.0, 5.0, 1.0]) / 6.0
    barycentric = np.ones(4)
    for node_row in range(4):
        for node_col in range(4):
            if node_row != node_col:
                barycentric[node_row] /= points[node_row] - points[node_col]
    deriv = np.zeros((4, 4))
    for node_row in range(4):
        for node_col in range(4):
            if node_row != node_col:
                deriv[node_row, node_col] = barycentric[node_col] / barycentric[node_row] / (points[node_row] - points[node_col])
        deriv[node_row, node_row] = -np.sum(deriv[node_row])
    to_modes = modes_table(points)
    sides = [lagrange_at(points, (points - 1.0) / 2.0), lagrange_at(points, (points + 1.0) / 2.0)]
    prolong = np.stack([np.kron(sides[child_id >> 2 & 1], np.kron(sides[child_id >> 1 & 1], sides[child_id & 1])) for child_id in range(8)])
    degrees = np.arange(4)
    levels = np.maximum(np.maximum(degrees[:, None, None], degrees[None, :, None]), degrees[None, None, :])
    top_mask = np.where(levels == 3, 1.0, 0.0)
    return (jnp.asarray(deriv, jnp.float32), jnp.asarray(weights, jnp.float32), jnp.asarray(to_modes, jnp.float32), jnp.asarray(prolong, jnp.float32), jnp.asarray(top_mask, jnp.float32))

def apply_along(matrix, values, node_axis):
    forms = {1: 'ak,vkjie->vajie', 2: 'aj,vkjie->vkaie', 3: 'ai,vkjie->vkjae'}
    return jnp.einsum(forms[node_axis], matrix, values, precision=lax.Precision.HIGHEST)

def face_flux(left_side, right_side, speed_dim):
    central = speed_dim * (left_side * left_side + left_side * right_side + right_side * right_side) / 6.0
    reach_by = jnp.abs(speed_dim) * jnp.maximum(jnp.abs(left_side), jnp.abs(right_side))
    return central - 0.5 * reach_by * (right_side - left_side)

def face_traces(shaped):
    element_count = shaped.shape[4]
    layers = []
    for dim_id in range(3):
        node_axis = 3 - dim_id
        for side_at in (0, 3):
            layers.append(lax.slice_in_dim(shaped, side_at, side_at + 1, axis=node_axis).reshape(5, 16, element_count))
    return jnp.stack(layers, axis=2)

def section_update(shaped, outside, speeds, inverse_jacobian):
    deriv, weights, to_modes, prolong, top_mask = node_constants()
    modal_coef = apply_along(to_modes, apply_along(to_modes, apply_along(to_modes, shaped[0:1], 1), 2), 3)[0]
    energy = modal_coef * modal_coef
    high_part = lax.optimization_barrier(jnp.sum(energy * top_mask[:, :, :, None], axis=(0, 1, 2)))
    all_part = lax.optimization_barrier(jnp.sum(energy, axis=(0, 1, 2)))
    top_ratio = high_part / (all_part + 1e-06)
    blend_weight = 0.5 * top_ratio / (top_ratio + 0.1)
    high_rate = jnp.zeros_like(shaped)
    lower_order_rate = jnp.zeros_like(shaped)
    for dim_id in range(3):
        node_axis = 3 - dim_id
        shape_w = [1, 1, 1, 1, 1]
        shape_w[node_axis] = 4
        node_weights = weights.reshape(shape_w)
        speed_dim = speeds[dim_id].reshape(5, 1, 1, 1, 1)
        volume = -(speed_dim / 3.0) * (shaped * apply_along(deriv, shaped, node_axis) + apply_along(deriv, shaped * shaped, node_axis))
        first_layer = lax.slice_in_dim(shaped, 0, 1, axis=node_axis)
        last_layer = lax.slice_in_dim(shaped, 3, 4, axis=node_axis)
        outer_left = outside[:, :, 2 * dim_id, :].reshape(first_layer.shape)
        outer_right = outside[:, :, 2 * dim_id + 1, :].reshape(first_layer.shape)
        flux_left = face_flux(outer_left, first_layer, speed_dim)
        flux_right = face_flux(last_layer, outer_right, speed_dim)
        middle = jnp.zeros_like(lax.slice_in_dim(shaped, 1, 3, axis=node_axis))
        surface_terms = jnp.concatenate([6.0 * (flux_left - 0.5 * speed_dim * first_layer * first_layer), middle, -6.0 * (flux_right - 0.5 * speed_dim * last_layer * last_layer)], axis=node_axis)
        inner_flux = face_flux(lax.slice_in_dim(shaped, 0, 3, axis=node_axis), lax.slice_in_dim(shaped, 1, 4, axis=node_axis), speed_dim)
        fluxes = jnp.concatenate([flux_left, inner_flux, flux_right], axis=node_axis)
        low_dim = -(lax.slice_in_dim(fluxes, 1, 5, axis=node_axis) - lax.slice_in_dim(fluxes, 0, 4, axis=node_axis)) / node_weights
        high_rate = high_rate + volume + surface_terms
        lower_order_rate = lower_order_rate + low_dim
    rate_all = inverse_jacobian * ((1.0 - blend_weight) * high_rate + blend_weight * lower_order_rate)
    return shaped + time_step * rate_all

def refine_block(updated, jacobian, flag_ids, flag_most):
    deriv, weights, to_modes, prolong, top_mask = node_constants()
    element_count = updated.shape[2]
    capacity = element_count + 7 * flag_most
    flag_ids = flag_ids.astype(jnp.int32)
    before = jnp.cumsum(flag_ids).astype(jnp.int32) - flag_ids
    element_ids = jnp.arange(element_count, dtype=jnp.int32)
    slot_ids = jnp.where(flag_ids == 1, before, flag_most).astype(jnp.int32)
    listing = jnp.zeros((flag_most,), jnp.int32).at[slot_ids].set(element_ids, mode='drop')
    chosen = jnp.take(updated, listing, axis=2)
    stacked = jnp.transpose(chosen, (1, 0, 2)).reshape(64, 5 * flag_most)
    children = jnp.dot(prolong.reshape(512, 64), stacked, precision=lax.Precision.HIGHEST, preferred_element_type=jnp.float32)
    children = jnp.transpose(children.reshape(8, 64, 5, flag_most), (2, 1, 0, 3)).reshape(5, 64, 8 * flag_most)
    placed = element_ids + 7 * before
    updated_refine_marks = jnp.zeros((capacity,), jnp.int32).at[placed].add(1)
    parent = jnp.clip(jnp.cumsum(updated_refine_marks).astype(jnp.int32) - 1, 0, element_count - 1)
    new_ids = jnp.arange(capacity, dtype=jnp.int32)
    child_id = new_ids - placed[parent]
    parent_flag = flag_ids[parent]
    new_total = (element_count + 7 * jnp.sum(flag_ids)).astype(jnp.int32)
    source = jnp.where(parent_flag == 1, element_count + child_id * flag_most + before[parent], parent)
    source = jnp.where(new_ids < new_total, source, 0).astype(jnp.int32)
    refined = jnp.take(jnp.concatenate([updated, children], axis=2), source, axis=2)
    new_jac = jacobian[parent] * jnp.where(parent_flag == 1, 2.0, 1.0).astype(jacobian.dtype)
    return (refined, new_jac, new_total)

def reference(nodal_state, inverse_jacobian, speeds, refine_flags, send_index, face_source):
    devices = N_CURVE
    elements = E_DEV
    slot_count = HALO_SLOTS
    element_total = devices * elements
    shaped = nodal_state.reshape(5, 4, 4, 4, element_total)
    traces = face_traces(shaped)
    trace_table = jnp.transpose(traces.reshape(5, 16, 6, devices, elements), (0, 1, 3, 2, 4)).reshape(5, 16, devices * 6 * elements)
    receiver = (jnp.arange(element_total, dtype=jnp.int32) // elements)[None, :]
    ghost_id = face_source - 6 * elements
    place_id = jnp.clip(ghost_id // slot_count, 0, 3)
    lane_id = jnp.clip(ghost_id - place_id * slot_count, 0, slot_count - 1)
    shifts = jnp.array([-2, -1, 1, 2], jnp.int32)
    sender = (receiver + shifts[place_id]) % devices
    blocks = send_index.reshape(devices, 4, slot_count)
    sent_flat = blocks[sender, 3 - place_id, lane_id]
    global_ids = jnp.where(face_source < 6 * elements, receiver * 6 * elements + face_source, sender * 6 * elements + sent_flat).astype(jnp.int32)
    outside = jnp.take(trace_table, global_ids.reshape(-1), axis=2).reshape(5, 16, 6, element_total)
    updated = section_update(shaped, outside, speeds, inverse_jacobian).reshape(5, 64, element_total)
    refined, new_jac, new_total = refine_block(updated, inverse_jacobian, refine_flags, FLAG_DEV * devices)
    return (refined[:, :, :NEW_ELEMS], new_jac[:NEW_ELEMS])
```

```python
import functools
import math

import jax
import jax.numpy as jnp
import numpy as np
from jax import lax
from jax.experimental import pallas as pl
from jax.experimental.pallas import tpu as pltpu
from jax.sharding import PartitionSpec as P

TIME_STEP = 0.02
VARS = 5
E_DEV = 512
E_NEW = 960
SLOTS = 96
ROWS = 64 * VARS
LANES = 128
GROUPS = E_DEV // LANES
ROW_OF = 8
COL_OF = 16
F32 = jnp.float32
BF16 = jnp.bfloat16
MESH = pl.DeviceIdType.MESH


def lagrange_at(points, targets):
    values_at = np.ones((len(targets), 4))
    for basis_id in range(4):
        for partner in range(4):
            if partner != basis_id:
                values_at[:, basis_id] *= (targets - points[partner]) / (
                    points[basis_id] - points[partner]
                )
    return values_at


def tables():
    root = 1.0 / math.sqrt(5.0)
    points = np.array([-1.0, -root, root, 1.0])
    weights = np.array([1.0, 5.0, 5.0, 1.0]) / 6.0
    bary = np.ones(4)
    for a in range(4):
        for b in range(4):
            if a != b:
                bary[a] /= points[a] - points[b]
    deriv = np.zeros((4, 4))
    for a in range(4):
        for b in range(4):
            if a != b:
                deriv[a, b] = bary[b] / bary[a] / (points[a] - points[b])
        deriv[a, a] = -np.sum(deriv[a])
    skew = weights[:, None] * deriv
    legendre = np.stack(
        [points**0, points, 0.5 * (3 * points**2 - 1), 0.5 * (5 * points**3 - 3 * points)], axis=1
    )
    to_modes = np.linalg.inv(legendre)
    sides = [lagrange_at(points, (points - 1.0) / 2.0), lagrange_at(points, (points + 1.0) / 2.0)]
    return skew, np.kron(to_modes, np.kron(to_modes, to_modes)), sides


SKEW, MODES, SIDES = tables()
Q01, Q02, Q03, Q12 = (float(SKEW[0, 1]), float(SKEW[0, 2]), float(SKEW[0, 3]), float(SKEW[1, 2]))
END, MID = 6.0, 1.2


def split2(x):
    high = x.astype(BF16)
    return high, (x - high.astype(F32)).astype(BF16)


def low_half(shape):
    return (lax.broadcasted_iota(jnp.int32, shape, 0) & 7) < 4


def turn(x):
    return pltpu.roll(x, 4, 0)


def fetch_state(x_ref, tile_ref, sems):
    copies = []
    for g in range(GROUPS):
        copy = pltpu.make_async_copy(
            x_ref.at[:, g * LANES : (g + 1) * LANES], tile_ref.at[g], sems.at[g]
        )
        copy.start()
        copies.append(copy)
    return copies


def build_traces(tile_ref, trace_ref, g):
    low = low_half((8, LANES))
    cols = slice(g * LANES, (g + 1) * LANES)
    for v in range(VARS):
        base = 64 * v
        tiles = [tile_ref[g, base + 8 * t : base + 8 * t + 8, :] for t in range(8)]
        first, last = tiles[0::2], tiles[1::2]
        sets = {
            0: [tile_ref[g, pl.ds(base + 32 * h, 8, stride=4), :] for h in range(2)],
            1: [tile_ref[g, pl.ds(base + 32 * h + 3, 8, stride=4), :] for h in range(2)],
            2: [jnp.where(low, first[k], turn(first[k + 1])) for k in (0, 2)],
            3: [jnp.where(low, turn(last[k]), last[k + 1]) for k in (0, 2)],
            4: tiles[0:2],
            5: tiles[6:8],
        }
        for f, rows in sets.items():
            high, rest = split2(jnp.concatenate(rows, axis=0))
            trace_ref[f, 16 * v : 16 * v + 16, cols] = high
            trace_ref[f, 80 + 16 * v : 96 + 16 * v, cols] = rest


def one_hot(index, size, width):
    rows = lax.broadcasted_iota(jnp.int32, (size, width), 0)
    return jnp.where(rows == index, 1.0, 0.0).astype(BF16)


def gather_sends(send_ref, trace_ref, out_ref):
    packed = jnp.broadcast_to(send_ref[...], (8, 4 * SLOTS))
    for block in range(4):
        shift = (4 * SLOTS - SLOTS * block) % (4 * SLOTS)
        moved = packed if shift == 0 else pltpu.roll(packed, shift, 1)
        index = moved[0:1, 0:LANES]
        total = jnp.zeros((160, LANES), F32)
        for f in range(6):
            total = total + jnp.dot(
                trace_ref[f],
                one_hot(index - f * E_DEV, E_DEV, LANES),
                preferred_element_type=F32,
            )
        out_ref[block] = total[0:80] + total[80:160]


def halo_kernel(
    x_ref, send_ref, flag_ref, ghost_ref, before_ref,
    tile_ref, trace_ref, out_buf, row_buf, col_buf, mine, group,
    fetch_sems, send_sems, recv_sems, row_send, row_recv, col_send, col_recv,
):
    fetches = fetch_state(x_ref, tile_ref, fetch_sems)
    me = lax.axis_index("curve")
    devices = ROW_OF * COL_OF
    row_at = me % ROW_OF
    col_at = me // ROW_OF
    offsets = (-2, -1, 1, 2)
    near = [(me + devices + o) % devices for o in offsets]
    row_mates = [col_at * ROW_OF + (row_at + k) % ROW_OF for k in range(1, ROW_OF)]
    col_mates = [((col_at + k) % COL_OF) * ROW_OF + row_at for k in range(1, COL_OF)]
    partners = near + row_mates + col_mates
    barrier = pltpu.get_barrier_semaphore()
    for partner in partners:
        pl.semaphore_signal(barrier, inc=1, device_id=(partner,), device_id_type=MESH)

    count = jnp.sum(flag_ref[...].astype(F32), axis=1, keepdims=True)
    mine[...] = jnp.broadcast_to(count - 64.0, (1, LANES))
    for g in range(GROUPS):
        fetches[g].wait()
        build_traces(tile_ref, trace_ref, g)
    gather_sends(send_ref, trace_ref, out_buf)

    pl.semaphore_wait(barrier, len(partners))
    row_copies = []
    for k, mate in enumerate(row_mates):
        copy = pltpu.make_async_remote_copy(
            src_ref=mine, dst_ref=row_buf.at[k], send_sem=row_send.at[k], recv_sem=row_recv.at[k],
            device_id=(mate,), device_id_type=MESH,
        )
        copy.start()
        row_copies.append(copy)
    copies = []
    for block, mate in enumerate(near):
        copy = pltpu.make_async_remote_copy(
            src_ref=out_buf.at[block], dst_ref=ghost_ref.at[3 - block],
            send_sem=send_sems.at[block], recv_sem=recv_sems.at[3 - block],
            device_id=(mate,), device_id_type=MESH,
        )
        copy.start()
        copies.append(copy)
    for copy in row_copies:
        copy.wait()
    total = mine[...]
    behind = jnp.zeros((1, LANES), F32)
    for k in range(ROW_OF - 1):
        value = row_buf[k]
        total = total + value
        behind = behind + jnp.where(row_at >= k + 1, value, 0.0)
    group[...] = total
    col_copies = []
    for k, mate in enumerate(col_mates):
        copy = pltpu.make_async_remote_copy(
            src_ref=group, dst_ref=col_buf.at[k], send_sem=col_send.at[k], recv_sem=col_recv.at[k],
            device_id=(mate,), device_id_type=MESH,
        )
        copy.start()
        col_copies.append(copy)
    for copy in col_copies:
        copy.wait()
    for k in range(COL_OF - 1):
        behind = behind + jnp.where(col_at >= k + 1, col_buf[k], 0.0)
    before_ref[...] = jnp.broadcast_to(behind, (8, LANES))
    for block in range(4):
        copies[block].wait_send()
        copies[3 - block].wait_recv()


def pair_sum(ui, um, si, sm):
    return (si + sm) + ui * um


def line_update(u, coef):
    ca, cb, c02, c03, cd = coef
    s = [x * x for x in u]
    m = [jnp.abs(x) for x in u]
    e = []
    for n, c in ((0, ca), (1, cb), (2, ca)):
        g = pair_sum(u[n], u[n + 1], s[n], s[n + 1])
        e.append(c * g - cd * (jnp.maximum(m[n], m[n + 1]) * (u[n + 1] - u[n])))
    r02 = c02 * pair_sum(u[0], u[2], s[0], s[2])
    r13 = c02 * pair_sum(u[1], u[3], s[1], s[3])
    r03 = c03 * pair_sum(u[0], u[3], s[0], s[3])
    t0 = -(e[0] + r02 + r03)
    t1 = e[0] - e[1] - r13
    t2 = e[1] - e[2] + r02
    t3 = e[2] + r13 + r03
    return t0, t1, t2, t3


def edge(u, o, cg, cd):
    g = pair_sum(u, o, u * u, o * o)
    return cg * g - cd * (jnp.maximum(jnp.abs(u), jnp.abs(o)) * (u - o))


def rows8(x):
    return jnp.broadcast_to(x, (8, LANES))


def blend_rates(tile_ref, modes_ref, jac_ref, rate_ref):
    n = lax.broadcasted_iota(jnp.int32, (64, LANES), 0)
    top = ((n & 3) == 3) | ((n & 12) == 12) | (n >= 48)
    for g in range(GROUPS):
        cols = slice(g * LANES, (g + 1) * LANES)
        modal = jnp.dot(
            modes_ref[...], tile_ref[g, 0:64, :], precision=lax.Precision.HIGHEST,
            preferred_element_type=F32,
        )
        energy = modal * modal
        high = jnp.sum(jnp.where(top, energy, 0.0), axis=0, keepdims=True)
        full = jnp.sum(energy, axis=0, keepdims=True)
        ratio = high / (full + 1e-06)
        blend = 0.5 * ratio / (ratio + 0.1)
        step = TIME_STEP * jac_ref[0:1, cols]
        rate_ref[0:1, cols] = step * (1.0 - blend)
        rate_ref[1:2, cols] = step * blend
        rate_ref[2:3, cols] = step


def outside_of(source_ref, trace_ref, ghost_ref, ghost_bf, outside_ref):
    for slot in range(4):
        high, rest = split2(ghost_ref[slot])
        ghost_bf[0:80, slot * LANES : (slot + 1) * LANES] = high
        ghost_bf[80:160, slot * LANES : (slot + 1) * LANES] = rest
    for f in range(6):
        index = source_ref[f : f + 1, :]
        far = index - 6 * E_DEV
        slot = (
            (far >= SLOTS).astype(jnp.int32)
            + (far >= 2 * SLOTS).astype(jnp.int32)
            + (far >= 3 * SLOTS).astype(jnp.int32)
        )
        far_row = jnp.where(far >= 0, far + (LANES - SLOTS) * slot, -1)
        near_row = index - (f ^ 1) * E_DEV
        total = jnp.dot(
            trace_ref[f ^ 1], one_hot(near_row, E_DEV, E_DEV), preferred_element_type=F32
        ) + jnp.dot(ghost_bf[...], one_hot(far_row, E_DEV, E_DEV), preferred_element_type=F32)
        outside_ref[f] = total[0:80] + total[80:160]


def update_block(v, g, tile_ref, speed_ref, rate_ref, outside_ref, acc_ref, up_ref):
    base = pl.multiple_of(64 * v, 64)
    face = pl.multiple_of(16 * v, 16)
    cols = pl.ds(pl.multiple_of(g * LANES, LANES), LANES)
    hi = rate_ref[0:1, cols]
    lo = rate_ref[1:2, cols]
    step = rate_ref[2:3, cols]
    low = low_half((8, LANES))

    def coefs(d):
        a = speed_ref[d, v]
        third = (a / 3.0) * hi
        sixth = (a / 6.0) * lo
        return (
            Q01 * third + sixth, Q12 * third + sixth, Q02 * third, Q03 * third,
            (0.5 * jnp.abs(a)) * lo, (a * (END / 6.0)) * step, (0.5 * END) * jnp.abs(a) * step,
        )

    ca, cb, c02, c03, cd, bg, bd = [rows8(c) for c in coefs(0)]
    for h in range(2):
        u = [tile_ref[g, pl.ds(base + 32 * h + i, 8, stride=4), :] for i in range(4)]
        t = line_update(u, (ca, cb, c02, c03, cd))
        ol = outside_ref[0, pl.ds(face + 8 * h, 8), cols]
        orr = outside_ref[1, pl.ds(face + 8 * h, 8), cols]
        acc = [
            END * t[0] + edge(u[0], ol, bg, bd), MID * t[1], MID * t[2],
            END * t[3] + edge(u[3], orr, -bg, bd),
        ]
        for i in range(4):
            acc_ref[pl.ds(32 * h + i, 8, stride=4), :] = acc[i]
    tiles = [tile_ref[g, pl.ds(base + 8 * t, 8), :] for t in range(8)]
    ca, cb, c02, c03, cd, bg, bd = [rows8(c) for c in coefs(2)]
    total = [None] * 8
    for h in range(2):
        u = [tiles[2 * k + h] for k in range(4)]
        t = line_update(u, (ca, cb, c02, c03, cd))
        ol = outside_ref[4, pl.ds(face + 8 * h, 8), cols]
        orr = outside_ref[5, pl.ds(face + 8 * h, 8), cols]
        acc = [
            END * t[0] + edge(u[0], ol, bg, bd), MID * t[1], MID * t[2],
            END * t[3] + edge(u[3], orr, -bg, bd),
        ]
        for k in range(4):
            total[2 * k + h] = acc[k]
    ca, cb, c02, c03, cd, bg, bd = [rows8(c) for c in coefs(1)]
    signed = jnp.where(low, -ca, ca)
    cross = jnp.where(low, -c03, -cb)
    cross_d = jnp.where(low, 0.0, cd)
    wa = jnp.where(low, END, MID)
    wb = jnp.where(low, MID, END)
    bgs = jnp.where(low, bg, -bg)
    outer_l = [outside_ref[2, pl.ds(face + 8 * h, 8), cols] for h in range(2)]
    outer_r = [outside_ref[3, pl.ds(face + 8 * h, 8), cols] for h in range(2)]
    for k in range(4):
        a, b = tiles[2 * k], tiles[2 * k + 1]
        at, bt = turn(a), turn(b)
        sa, sb, sat, sbt = a * a, b * b, at * at, bt * bt
        ma, mb, mat, mbt = jnp.abs(a), jnp.abs(b), jnp.abs(at), jnp.abs(bt)
        x1 = signed * pair_sum(a, at, sa, sat) + cd * (jnp.maximum(ma, mat) * (at - a))
        x2 = signed * pair_sum(b, bt, sb, sbt) + cd * (jnp.maximum(mb, mbt) * (bt - b))
        x3 = c02 * pair_sum(a, b, sa, sb)
        x4 = cross * pair_sum(a, bt, sa, sbt) + cross_d * (jnp.maximum(ma, mbt) * (bt - a))
        ol = outer_l[k // 2]
        orr = outer_r[k // 2]
        outer = jnp.where(low, ol, turn(orr)) if k % 2 == 0 else jnp.where(low, turn(ol), orr)
        bound = edge(jnp.where(low, a, b), outer, bgs, bd)
        total[2 * k] += wa * (x1 - x3 + x4) + jnp.where(low, bound, 0.0)
        total[2 * k + 1] += wb * (x2 + x3 - turn(x4)) + jnp.where(low, 0.0, bound)
    for t in range(8):
        total[t] += tiles[t] + acc_ref[8 * t : 8 * t + 8, :]
    for t in range(4):
        high, rest = split2(jnp.concatenate(total[2 * t : 2 * t + 2], axis=0))
        up_ref[pl.ds(pl.multiple_of(base + 16 * t, 16), 16), cols] = high
        up_ref[pl.ds(pl.multiple_of(ROWS + base + 16 * t, 16), 16), cols] = rest


def refine_tables(flag_ref, jac_ref, start_ref, aux_ref):
    flags = flag_ref[...].astype(F32)
    wide = jnp.broadcast_to(flags, (LANES, E_DEV)).astype(BF16)
    row = lax.broadcasted_iota(jnp.int32, (E_DEV, E_DEV), 0)
    col = lax.broadcasted_iota(jnp.int32, (E_DEV, E_DEV), 1)
    ahead = jnp.where(col < row, 1.0, 0.0).astype(BF16)
    within = jnp.where(col <= row, 1.0, 0.0).astype(BF16)
    dims = (((1,), (1,)), ((), ()))
    place = lax.broadcasted_iota(jnp.int32, (E_DEV, LANES), 0).astype(F32)
    start_ref[0] = place + 7.0 * lax.dot_general(ahead, wide, dims, preferred_element_type=F32)
    start_ref[1] = (
        place + 1.0 + 7.0 * lax.dot_general(within, wide, dims, preferred_element_type=F32)
    )
    count = lax.dot_general(wide[0:16], ahead, dims, preferred_element_type=F32)[0:1]
    at = lax.broadcasted_iota(jnp.int32, (1, E_DEV), 1).astype(F32) + 7.0 * count
    at_high = jnp.floor(at * (1.0 / 16.0))
    jac = jac_ref[...]
    j0, rest = split2(jac)
    rest = jac - j0.astype(F32)
    j1 = rest.astype(BF16)
    j2 = (rest - j1.astype(F32)).astype(BF16)
    zero = jnp.zeros((10, E_DEV), F32)
    aux_ref[...] = jnp.concatenate(
        [
            at_high, at - 16.0 * at_high, flags, j0.astype(F32), j1.astype(F32), j2.astype(F32),
            zero,
        ],
        axis=0,
    ).astype(BF16)


def column_tables(first, before, start_ref, aux_ref, coef_ref, hot_ref):
    lane = lax.broadcasted_iota(jnp.int32, (1, LANES), 1) + first
    place = lane.astype(F32) - 7.0 * before[0:1, :]
    inside = (place >= start_ref[0]) & (place < start_ref[1])
    hot = jnp.where(inside, 1.0, 0.0).astype(BF16)
    hot_ref[...] = hot
    aux = jnp.dot(aux_ref[...], hot, preferred_element_type=F32)
    child = place - (16.0 * aux[0:1] + aux[1:2])
    refined = aux[2:3] > 0.5
    z = child >= 4.0
    child = child - jnp.where(z, 4.0, 0.0)
    y = child >= 2.0
    child = child - jnp.where(y, 2.0, 0.0)
    x = child >= 1.0
    jac = (aux[3:4] + aux[4:5] + aux[5:6]) * jnp.where(refined, 2.0, 1.0)

    def table(bit):
        return [
            [
                rows8(
                    jnp.where(
                        refined,
                        jnp.where(bit, float(SIDES[1][i, m]), float(SIDES[0][i, m])),
                        1.0 if i == m else 0.0,
                    )
                )
                for m in range(4)
            ]
            for i in range(4)
        ]

    cx, cy, cz = table(x), table(y), table(z)
    low = low_half((8, LANES))
    n = 0
    for i in range(4):
        for m in range(4):
            coef_ref[n] = cx[i][m]
            coef_ref[16 + n] = cz[i][m]
            n += 1
    order = [(0, 1), (1, 0), (2, 3), (3, 2)]
    for at, (first_j, last_j) in enumerate(((0, 1), (2, 3))):
        for k, (lo_m, hi_m) in enumerate(order):
            coef_ref[32 + 4 * at + k] = jnp.where(low, cy[first_j][lo_m], cy[last_j][hi_m])
    return jac


def combine4(c, u):
    return (c[0] * u[0] + c[1] * u[1]) + (c[2] * u[2] + c[3] * u[3])


def interpolate(v, pick_ref, coef_ref, line_ref, put):
    base = pl.multiple_of(64 * v, 64)
    tiles = [
        pick_ref[pl.ds(base + 8 * t, 8), :] + pick_ref[pl.ds(ROWS + base + 8 * t, 8), :]
        for t in range(8)
    ]
    mid = [None] * 8
    for h in range(2):
        u = [tiles[2 * k + h] for k in range(4)]
        for k in range(4):
            mid[2 * k + h] = combine4([coef_ref[16 + 4 * k + m] for m in range(4)], u)
    for k in range(4):
        a, b = mid[2 * k], mid[2 * k + 1]
        u = [a, turn(a), b, turn(b)]
        for at in range(2):
            line_ref[16 * k + 8 * at : 16 * k + 8 * at + 8, :] = combine4(
                [coef_ref[32 + 4 * at + m] for m in range(4)], u
            )
    for h in range(2):
        u = [line_ref[pl.ds(32 * h + i, 8, stride=4), :] for i in range(4)]
        for i in range(4):
            put(base + 32 * h + i, combine4([coef_ref[4 * i + m] for m in range(4)], u))


def local_kernel(
    x_ref, jac_ref, speed_ref, flag_ref, source_ref, ghost_ref, before_ref, modes_ref,
    own_ref, own_jac_ref, blocks_ref,
    tile_ref, trace_ref, ghost_bf, outside_ref, rate_ref, acc_ref, up_ref, start_ref, aux_ref, coef_ref,
    hot_ref, pick_ref, line_ref, fetch_sems,
):
    fetches = fetch_state(x_ref, tile_ref, fetch_sems)
    for g in range(GROUPS):
        fetches[g].wait()
        build_traces(tile_ref, trace_ref, g)
    blend_rates(tile_ref, modes_ref, jac_ref, rate_ref)
    outside_of(source_ref, trace_ref, ghost_ref, ghost_bf, outside_ref)

    def step(n, carry):
        update_block(n // GROUPS, n % GROUPS, tile_ref, speed_ref, rate_ref, outside_ref, acc_ref, up_ref)
        return carry

    lax.fori_loop(0, VARS * GROUPS, step, 0)
    refine_tables(flag_ref, jac_ref, start_ref, aux_ref)
    before = before_ref[...]

    def columns(first, put, put_jac):
        put_jac(column_tables(first, before, start_ref, aux_ref, coef_ref, hot_ref))
        pick_ref[...] = jnp.dot(up_ref[...], hot_ref[...], preferred_element_type=F32)

        def one(v, carry):
            interpolate(v, pick_ref, coef_ref, line_ref, put)
            return carry

        lax.fori_loop(0, VARS, one, 0)

    def block_step(n, carry):
        first = jnp.where(n < 2, -2 * LANES + n * LANES, E_NEW + (n - 2) * LANES)
        at = n // 2
        half = n % 2

        def put(row, value):
            blocks_ref[at, half, pl.ds(row, 8, stride=4), :] = value

        def put_jac(value):
            blocks_ref[at, half, ROWS : ROWS + 8, :] = rows8(value)

        columns(first, put, put_jac)
        return carry

    lax.fori_loop(0, 4, block_step, 0)

    def own_step(n, carry):
        first = pl.multiple_of(n * LANES, LANES)
        cols = pl.ds(first, LANES)

        def put(row, value):
            own_ref[n, pl.ds(row, 8, stride=4), :] = value

        def put_jac(value):
            own_jac_ref[0:1, cols] = value

        columns(first, put, put_jac)
        return carry

    lax.fori_loop(0, 8, own_step, 0)


def exchange_kernel(blocks_ref, landed_ref, send_sems, recv_sems):
    me = lax.axis_index("curve")
    devices = ROW_OF * COL_OF
    mates = ((me + devices - 1) % devices, (me + 1) % devices)
    barrier = pltpu.get_barrier_semaphore()
    for mate in mates:
        pl.semaphore_signal(barrier, inc=1, device_id=(mate,), device_id_type=MESH)
    pl.semaphore_wait(barrier, 2)
    copies = []
    for at, mate in enumerate(mates):
        copy = pltpu.make_async_remote_copy(
            src_ref=blocks_ref.at[at], dst_ref=landed_ref.at[at],
            send_sem=send_sems.at[at], recv_sem=recv_sems.at[at],
            device_id=(mate,), device_id_type=MESH,
        )
        copy.start()
        copies.append(copy)
    for copy in copies:
        copy.wait()


def merge_kernel(own_ref, own_jac_ref, landed_ref, out_ref, jac_ref):
    left = lax.broadcasted_iota(jnp.int32, (8, LANES), 1) < LANES // 2

    def rows_of(r, get_own, put):
        own = [get_own(c) for c in range(8)]
        low = [landed_ref[1, c, r, :] for c in range(2)]
        far = [
            pltpu.roll(landed_ref[0, c, r, :], LANES // 2, 1)
            for c in range(2)
        ]
        own[0] += low[0]
        own[1] += low[1]
        own[5] += jnp.where(left, 0.0, far[0])
        own[6] += jnp.where(left, far[0], far[1])
        own[7] += far[1]
        for c in range(8):
            put(c, own[c])

    def step(n, carry):
        r = pl.ds(pl.multiple_of(8 * n, 8), 8)

        def put(c, value):
            if c < 7:
                out_ref[r, c * LANES : (c + 1) * LANES] = value
            else:
                out_ref[r, c * LANES : E_NEW] = value[:, : E_NEW - 7 * LANES]

        rows_of(r, lambda c: own_ref[c, r, :], put)
        return carry

    lax.fori_loop(0, ROWS // 8, step, 0)

    def put_jac(c, value):
        width = min(LANES, E_NEW - c * LANES)
        jac_ref[0:1, c * LANES : c * LANES + width] = value[0:1, :width]

    rows_of(
        pl.ds(ROWS, 8), lambda c: rows8(own_jac_ref[0:1, c * LANES : (c + 1) * LANES]), put_jac
    )


def vmem(count):
    return [pl.BlockSpec(memory_space=pltpu.VMEM)] * count


def shards(nodal_state, inverse_jacobian, speeds, refine_flags, send_index, face_source):
    x = nodal_state.reshape(ROWS, E_DEV)
    jac = inverse_jacobian.reshape(1, E_DEV)
    flags = refine_flags.reshape(1, E_DEV)
    sends = send_index.reshape(1, 4 * SLOTS)
    dma = pltpu.SemaphoreType.DMA
    ghost, before = pl.pallas_call(
        halo_kernel,
        out_shape=(
            jax.ShapeDtypeStruct((4, 80, LANES), F32),
            jax.ShapeDtypeStruct((8, LANES), F32),
        ),
        in_specs=[pl.BlockSpec(memory_space=pl.ANY)] + vmem(2),
        out_specs=tuple(vmem(2)),
        scratch_shapes=[
            pltpu.VMEM((GROUPS, ROWS, LANES), F32),
            pltpu.VMEM((6, 160, E_DEV), BF16),
            pltpu.VMEM((4, 80, LANES), F32),
            pltpu.VMEM((ROW_OF - 1, 1, LANES), F32),
            pltpu.VMEM((COL_OF - 1, 1, LANES), F32),
            pltpu.VMEM((1, LANES), F32),
            pltpu.VMEM((1, LANES), F32),
            dma((GROUPS,)), dma((4,)), dma((4,)), dma((ROW_OF - 1,)), dma((ROW_OF - 1,)),
            dma((COL_OF - 1,)), dma((COL_OF - 1,)),
        ],
        compiler_params=pltpu.CompilerParams(collective_id=0, has_side_effects=True),
        name="halo",
    )(x, sends, flags)
    modes = jnp.asarray(MODES, F32)
    specs = vmem(8)
    specs[0] = pl.BlockSpec(memory_space=pl.ANY)
    specs[2] = pl.BlockSpec(memory_space=pltpu.SMEM)
    own, own_jac, blocks = pl.pallas_call(
        local_kernel,
        out_shape=(
            jax.ShapeDtypeStruct((8, ROWS, LANES), F32),
            jax.ShapeDtypeStruct((1, 1024), F32),
            jax.ShapeDtypeStruct((2, 2, ROWS + 8, LANES), F32),
        ),
        in_specs=specs,
        out_specs=tuple(vmem(3)),
        scratch_shapes=[
            pltpu.VMEM((GROUPS, ROWS, LANES), F32),
            pltpu.VMEM((6, 160, E_DEV), BF16),
            pltpu.VMEM((160, E_DEV), BF16),
            pltpu.VMEM((6, 80, E_DEV), F32),
            pltpu.VMEM((8, E_DEV), F32),
            pltpu.VMEM((64, LANES), F32),
            pltpu.VMEM((2 * ROWS, E_DEV), BF16),
            pltpu.VMEM((2, E_DEV, LANES), F32),
            pltpu.VMEM((16, E_DEV), BF16),
            pltpu.VMEM((40, 8, LANES), F32),
            pltpu.VMEM((E_DEV, LANES), BF16),
            pltpu.VMEM((2 * ROWS, LANES), F32),
            pltpu.VMEM((64, LANES), F32),
            dma((GROUPS,)),
        ],
        name="local",
    )(x, jac, speeds, flags, face_source, ghost, before, modes)
    landed = pl.pallas_call(
        exchange_kernel,
        out_shape=jax.ShapeDtypeStruct((2, 2, ROWS + 8, LANES), F32),
        in_specs=vmem(1),
        out_specs=vmem(1)[0],
        scratch_shapes=[dma((2,)), dma((2,))],
        compiler_params=pltpu.CompilerParams(collective_id=1, has_side_effects=True),
        name="exchange",
    )(blocks)
    out, out_jac = pl.pallas_call(
        merge_kernel,
        out_shape=(
            jax.ShapeDtypeStruct((ROWS, E_NEW), F32),
            jax.ShapeDtypeStruct((1, E_NEW), F32),
        ),
        in_specs=vmem(3),
        out_specs=tuple(vmem(2)),
        name="merge",
    )(own, own_jac, landed)
    return out.reshape(VARS, 64, E_NEW), out_jac.reshape(E_NEW)


def solution(mesh):
    axis = P("curve")
    wide = P(None, None, "curve")
    return jax.shard_map(
        shards,
        mesh=mesh,
        in_specs=(wide, axis, P(), axis, axis, P(None, "curve")),
        out_specs=(wide, axis),
        check_vma=False,
    )
```

```python
import functools
import math

import jax
import jax.numpy as jnp
import numpy as np
from jax import lax
from jax.experimental import pallas as pl
from jax.experimental.pallas import tpu as pltpu
from jax.sharding import PartitionSpec as P

TIME_STEP = 0.02
VARS = 5
E_DEV = 512
E_NEW = 960
SLOTS = 96
ROWS = 64 * VARS
LANES = 128
GROUPS = E_DEV // LANES
ROW_OF = 8
COL_OF = 16
F32 = jnp.float32
BF16 = jnp.bfloat16
MESH = pl.DeviceIdType.MESH


def lagrange_at(points, targets):
    values_at = np.ones((len(targets), 4))
    for basis_id in range(4):
        for partner in range(4):
            if partner != basis_id:
                values_at[:, basis_id] *= (targets - points[partner]) / (
                    points[basis_id] - points[partner]
                )
    return values_at


def tables():
    root = 1.0 / math.sqrt(5.0)
    points = np.array([-1.0, -root, root, 1.0])
    weights = np.array([1.0, 5.0, 5.0, 1.0]) / 6.0
    bary = np.ones(4)
    for a in range(4):
        for b in range(4):
            if a != b:
                bary[a] /= points[a] - points[b]
    deriv = np.zeros((4, 4))
    for a in range(4):
        for b in range(4):
            if a != b:
                deriv[a, b] = bary[b] / bary[a] / (points[a] - points[b])
        deriv[a, a] = -np.sum(deriv[a])
    skew = weights[:, None] * deriv
    legendre = np.stack(
        [points**0, points, 0.5 * (3 * points**2 - 1), 0.5 * (5 * points**3 - 3 * points)], axis=1
    )
    to_modes = np.linalg.inv(legendre)
    sides = [lagrange_at(points, (points - 1.0) / 2.0), lagrange_at(points, (points + 1.0) / 2.0)]
    return skew, np.kron(to_modes, np.kron(to_modes, to_modes)), sides


SKEW, MODES, SIDES = tables()
Q01, Q02, Q03, Q12 = (float(SKEW[0, 1]), float(SKEW[0, 2]), float(SKEW[0, 3]), float(SKEW[1, 2]))
END, MID = 6.0, 1.2


def split2(x):
    high = x.astype(BF16)
    return high, (x - high.astype(F32)).astype(BF16)


def low_half(shape):
    return (lax.broadcasted_iota(jnp.int32, shape, 0) & 7) < 4


def turn(x):
    return pltpu.roll(x, 4, 0)


def fetch_state(x_ref, tile_ref, sems):
    copies = []
    for g in range(GROUPS):
        copy = pltpu.make_async_copy(
            x_ref.at[:, g * LANES : (g + 1) * LANES], tile_ref.at[g], sems.at[g]
        )
        copy.start()
        copies.append(copy)
    return copies


def build_traces(tile_ref, trace_ref, g):
    low = low_half((8, LANES))
    cols = slice(g * LANES, (g + 1) * LANES)
    for v in range(VARS):
        base = 64 * v
        tiles = [tile_ref[g, base + 8 * t : base + 8 * t + 8, :] for t in range(8)]
        first, last = tiles[0::2], tiles[1::2]
        sets = {
            0: [tile_ref[g, pl.ds(base + 32 * h, 8, stride=4), :] for h in range(2)],
            1: [tile_ref[g, pl.ds(base + 32 * h + 3, 8, stride=4), :] for h in range(2)],
            2: [jnp.where(low, first[k], turn(first[k + 1])) for k in (0, 2)],
            3: [jnp.where(low, turn(last[k]), last[k + 1]) for k in (0, 2)],
            4: tiles[0:2],
            5: tiles[6:8],
        }
        for f, rows in sets.items():
            high, rest = split2(jnp.concatenate(rows, axis=0))
            trace_ref[f, 16 * v : 16 * v + 16, cols] = high
            trace_ref[f, 80 + 16 * v : 96 + 16 * v, cols] = rest


def one_hot(index, size, width):
    rows = lax.broadcasted_iota(jnp.int32, (size, width), 0)
    return jnp.where(rows == index, 1.0, 0.0).astype(BF16)


def gather_sends(send_ref, trace_ref, out_ref):
    packed = jnp.broadcast_to(send_ref[...].reshape(1, 4 * SLOTS), (8, 4 * SLOTS))
    for block in range(4):
        shift = (4 * SLOTS - SLOTS * block) % (4 * SLOTS)
        moved = packed if shift == 0 else pltpu.roll(packed, shift, 1)
        index = moved[0:1, 0:LANES]
        total = jnp.zeros((160, LANES), F32)
        for f in range(6):
            total = total + jnp.dot(
                trace_ref[f],
                one_hot(index - f * E_DEV, E_DEV, LANES),
                preferred_element_type=F32,
            )
        out_ref[block] = total[0:80] + total[80:160]


def pair_sum(ui, um, si, sm):
    return (si + sm) + ui * um


def line_update(u, coef):
    ca, cb, c02, c03, cd = coef
    s = [x * x for x in u]
    m = [jnp.abs(x) for x in u]
    e = []
    for n, c in ((0, ca), (1, cb), (2, ca)):
        g = pair_sum(u[n], u[n + 1], s[n], s[n + 1])
        e.append(c * g - cd * (jnp.maximum(m[n], m[n + 1]) * (u[n + 1] - u[n])))
    r02 = c02 * pair_sum(u[0], u[2], s[0], s[2])
    r13 = c02 * pair_sum(u[1], u[3], s[1], s[3])
    r03 = c03 * pair_sum(u[0], u[3], s[0], s[3])
    t0 = -(e[0] + r02 + r03)
    t1 = e[0] - e[1] - r13
    t2 = e[1] - e[2] + r02
    t3 = e[2] + r13 + r03
    return t0, t1, t2, t3


def edge(u, o, cg, cd):
    g = pair_sum(u, o, u * u, o * o)
    return cg * g - cd * (jnp.maximum(jnp.abs(u), jnp.abs(o)) * (u - o))


def rows8(x):
    return jnp.broadcast_to(x, (8, LANES))


def blend_rates(tile_ref, modes_ref, jac_ref, rate_ref):
    n = lax.broadcasted_iota(jnp.int32, (64, LANES), 0)
    top = ((n & 3) == 3) | ((n & 12) == 12) | (n >= 48)
    for g in range(GROUPS):
        cols = slice(g * LANES, (g + 1) * LANES)
        modal = jnp.dot(
            modes_ref[...], tile_ref[g, 0:64, :], precision=lax.Precision.HIGHEST,
            preferred_element_type=F32,
        )
        energy = modal * modal
        high = jnp.sum(jnp.where(top, energy, 0.0), axis=0, keepdims=True)
        full = jnp.sum(energy, axis=0, keepdims=True)
        ratio = high / (full + 1e-06)
        blend = 0.5 * ratio / (ratio + 0.1)
        step = TIME_STEP * jac_ref[0:1, cols]
        rate_ref[0:1, cols] = step * (1.0 - blend)
        rate_ref[1:2, cols] = step * blend
        rate_ref[2:3, cols] = step


def outside_near(source_ref, trace_ref, outside_ref):
    for f in range(6):
        near_row = source_ref[f : f + 1, :] - (f ^ 1) * E_DEV
        total = jnp.dot(
            trace_ref[f ^ 1], one_hot(near_row, E_DEV, E_DEV), preferred_element_type=F32
        )
        outside_ref[f] = total[0:80] + total[80:160]


def outside_far(source_ref, ghost_ref, ghost_bf, outside_ref):
    for slot in range(4):
        high, rest = split2(ghost_ref[slot])
        ghost_bf[0:80, slot * LANES : (slot + 1) * LANES] = high
        ghost_bf[80:160, slot * LANES : (slot + 1) * LANES] = rest
    for f in range(6):
        far = source_ref[f : f + 1, :] - 6 * E_DEV
        slot = (
            (far >= SLOTS).astype(jnp.int32)
            + (far >= 2 * SLOTS).astype(jnp.int32)
            + (far >= 3 * SLOTS).astype(jnp.int32)
        )
        far_row = jnp.where(far >= 0, far + (LANES - SLOTS) * slot, -1)
        total = jnp.dot(ghost_bf[...], one_hot(far_row, E_DEV, E_DEV), preferred_element_type=F32)
        outside_ref[f] += total[0:80] + total[80:160]


def coefs_of(d, v, speed_ref, hi, lo):
    a = speed_ref[d, v]
    third = (a / 3.0) * hi
    sixth = (a / 6.0) * lo
    return [
        rows8(c)
        for c in (
            Q01 * third + sixth, Q12 * third + sixth, Q02 * third, Q03 * third,
            (0.5 * jnp.abs(a)) * lo,
        )
    ]


def interior_block(v, g, tile_ref, speed_ref, rate_ref, state_ref):
    base = pl.multiple_of(64 * v, 64)
    cols = pl.ds(pl.multiple_of(g * LANES, LANES), LANES)
    hi = rate_ref[0:1, cols]
    lo = rate_ref[1:2, cols]
    low = low_half((8, LANES))
    coef = coefs_of(0, v, speed_ref, hi, lo)
    for h in range(2):
        u = [tile_ref[g, pl.ds(base + 32 * h + i, 8, stride=4), :] for i in range(4)]
        t = line_update(u, coef)
        for i, w in enumerate((END, MID, MID, END)):
            state_ref[g, pl.ds(base + 32 * h + i, 8, stride=4), :] = u[i] + w * t[i]
    tiles = [tile_ref[g, pl.ds(base + 8 * t, 8), :] for t in range(8)]
    coef = coefs_of(2, v, speed_ref, hi, lo)
    total = [None] * 8
    for h in range(2):
        t = line_update([tiles[2 * k + h] for k in range(4)], coef)
        for k, w in enumerate((END, MID, MID, END)):
            total[2 * k + h] = w * t[k]
    ca, cb, c02, c03, cd = coefs_of(1, v, speed_ref, hi, lo)
    signed = jnp.where(low, -ca, ca)
    cross = jnp.where(low, -c03, -cb)
    cross_d = jnp.where(low, 0.0, cd)
    wa = jnp.where(low, END, MID)
    wb = jnp.where(low, MID, END)
    for k in range(4):
        a, b = tiles[2 * k], tiles[2 * k + 1]
        at, bt = turn(a), turn(b)
        sa, sb, sat, sbt = a * a, b * b, at * at, bt * bt
        ma, mb, mat, mbt = jnp.abs(a), jnp.abs(b), jnp.abs(at), jnp.abs(bt)
        x1 = signed * pair_sum(a, at, sa, sat) + cd * (jnp.maximum(ma, mat) * (at - a))
        x2 = signed * pair_sum(b, bt, sb, sbt) + cd * (jnp.maximum(mb, mbt) * (bt - b))
        x3 = c02 * pair_sum(a, b, sa, sb)
        x4 = cross * pair_sum(a, bt, sa, sbt) + cross_d * (jnp.maximum(ma, mbt) * (bt - a))
        total[2 * k] += wa * (x1 - x3 + x4)
        total[2 * k + 1] += wb * (x2 + x3 - turn(x4))
    for t in range(8):
        state_ref[g, pl.ds(base + 8 * t, 8), :] += total[t]


def edge_block(v, g, tile_ref, speed_ref, rate_ref, outside_ref, state_ref, up_ref):
    base = pl.multiple_of(64 * v, 64)
    face = pl.multiple_of(16 * v, 16)
    cols = pl.ds(pl.multiple_of(g * LANES, LANES), LANES)
    step = rate_ref[2:3, cols]
    low = low_half((8, LANES))

    def coefs(d):
        a = speed_ref[d, v]
        return rows8((a * (END / 6.0)) * step), rows8((0.5 * END) * jnp.abs(a) * step)

    bg, bd = coefs(0)
    for h in range(2):
        for f, i, sign in ((0, 0, bg), (1, 3, -bg)):
            rows = pl.ds(base + 32 * h + i, 8, stride=4)
            outer = outside_ref[f, pl.ds(face + 8 * h, 8), cols]
            state_ref[g, rows, :] += edge(tile_ref[g, rows, :], outer, sign, bd)
    tiles = [tile_ref[g, pl.ds(base + 8 * t, 8), :] for t in range(8)]
    total = [state_ref[g, pl.ds(base + 8 * t, 8), :] for t in range(8)]
    bg, bd = coefs(2)
    for h in range(2):
        for f, k, sign in ((4, 0, bg), (5, 3, -bg)):
            outer = outside_ref[f, pl.ds(face + 8 * h, 8), cols]
            total[2 * k + h] += edge(tiles[2 * k + h], outer, sign, bd)
    bg, bd = coefs(1)
    bgs = jnp.where(low, bg, -bg)
    outer_l = [outside_ref[2, pl.ds(face + 8 * h, 8), cols] for h in range(2)]
    outer_r = [outside_ref[3, pl.ds(face + 8 * h, 8), cols] for h in range(2)]
    for k in range(4):
        ol = outer_l[k // 2]
        orr = outer_r[k // 2]
        outer = jnp.where(low, ol, turn(orr)) if k % 2 == 0 else jnp.where(low, turn(ol), orr)
        bound = edge(jnp.where(low, tiles[2 * k], tiles[2 * k + 1]), outer, bgs, bd)
        total[2 * k] += jnp.where(low, bound, 0.0)
        total[2 * k + 1] += jnp.where(low, 0.0, bound)
    for t in range(4):
        high, rest = split2(jnp.concatenate(total[2 * t : 2 * t + 2], axis=0))
        up_ref[pl.ds(pl.multiple_of(base + 16 * t, 16), 16), cols] = high
        up_ref[pl.ds(pl.multiple_of(ROWS + base + 16 * t, 16), 16), cols] = rest


def refine_tables(flag_ref, jac_ref, start_ref, aux_ref):
    flags = flag_ref[...].astype(F32)
    wide = jnp.broadcast_to(flags, (LANES, E_DEV)).astype(BF16)
    row = lax.broadcasted_iota(jnp.int32, (E_DEV, E_DEV), 0)
    col = lax.broadcasted_iota(jnp.int32, (E_DEV, E_DEV), 1)
    ahead = jnp.where(col < row, 1.0, 0.0).astype(BF16)
    within = jnp.where(col <= row, 1.0, 0.0).astype(BF16)
    dims = (((1,), (1,)), ((), ()))
    place = lax.broadcasted_iota(jnp.int32, (E_DEV, LANES), 0).astype(F32)
    start_ref[0] = place + 7.0 * lax.dot_general(ahead, wide, dims, preferred_element_type=F32)
    start_ref[1] = (
        place + 1.0 + 7.0 * lax.dot_general(within, wide, dims, preferred_element_type=F32)
    )
    count = lax.dot_general(wide[0:16], ahead, dims, preferred_element_type=F32)[0:1]
    at = lax.broadcasted_iota(jnp.int32, (1, E_DEV), 1).astype(F32) + 7.0 * count
    at_high = jnp.floor(at * (1.0 / 16.0))
    jac = jac_ref[...]
    j0, rest = split2(jac)
    rest = jac - j0.astype(F32)
    j1 = rest.astype(BF16)
    j2 = (rest - j1.astype(F32)).astype(BF16)
    zero = jnp.zeros((10, E_DEV), F32)
    aux_ref[...] = jnp.concatenate(
        [
            at_high, at - 16.0 * at_high, flags, j0.astype(F32), j1.astype(F32), j2.astype(F32),
            zero,
        ],
        axis=0,
    ).astype(BF16)


def column_tables(tile, first, before, start_ref, aux_ref, coef_ref, hot_ref):
    lane = lax.broadcasted_iota(jnp.int32, (1, LANES), 1) + first
    place = lane.astype(F32) - 7.0 * before[0:1, :]
    inside = (place >= start_ref[0]) & (place < start_ref[1])
    hot = jnp.where(inside, 1.0, 0.0).astype(BF16)
    cols = pl.ds(pl.multiple_of((tile % 2) * LANES, LANES), LANES)
    hot_ref[tile // 2, :, cols] = hot
    aux = jnp.dot(aux_ref[...], hot, preferred_element_type=F32)
    child = place - (16.0 * aux[0:1] + aux[1:2])
    refined = aux[2:3] > 0.5
    z = child >= 4.0
    child = child - jnp.where(z, 4.0, 0.0)
    y = child >= 2.0
    child = child - jnp.where(y, 2.0, 0.0)
    x = child >= 1.0
    jac = (aux[3:4] + aux[4:5] + aux[5:6]) * jnp.where(refined, 2.0, 1.0)

    def table(bit):
        return [
            [
                rows8(
                    jnp.where(
                        refined,
                        jnp.where(bit, float(SIDES[1][i, m]), float(SIDES[0][i, m])),
                        1.0 if i == m else 0.0,
                    )
                )
                for m in range(4)
            ]
            for i in range(4)
        ]

    cx, cy, cz = table(x), table(y), table(z)
    low = low_half((8, LANES))
    n = 0
    for i in range(4):
        for m in range(4):
            coef_ref[tile, n] = cx[i][m]
            coef_ref[tile, 16 + n] = cz[i][m]
            n += 1
    order = [(0, 1), (1, 0), (2, 3), (3, 2)]
    for at, (first_j, last_j) in enumerate(((0, 1), (2, 3))):
        for k, (lo_m, hi_m) in enumerate(order):
            coef_ref[tile, 32 + 4 * at + k] = jnp.where(low, cy[first_j][lo_m], cy[last_j][hi_m])
    return jac


def combine4(c, u):
    return (c[0] * u[0] + c[1] * u[1]) + (c[2] * u[2] + c[3] * u[3])


def interpolate(v, tile, half, pick_ref, coef_ref, line_ref, put):
    base = pl.multiple_of(64 * v, 64)
    cols = slice(half * LANES, half * LANES + LANES)
    tiles = [
        pick_ref[pl.ds(base + 8 * t, 8), cols] + pick_ref[pl.ds(ROWS + base + 8 * t, 8), cols]
        for t in range(8)
    ]
    mid = [None] * 8
    for h in range(2):
        u = [tiles[2 * k + h] for k in range(4)]
        for k in range(4):
            mid[2 * k + h] = combine4([coef_ref[tile, 16 + 4 * k + m] for m in range(4)], u)
    for k in range(4):
        a, b = mid[2 * k], mid[2 * k + 1]
        u = [a, turn(a), b, turn(b)]
        for at in range(2):
            line_ref[16 * k + 8 * at : 16 * k + 8 * at + 8, :] = combine4(
                [coef_ref[tile, 32 + 4 * at + m] for m in range(4)], u
            )
    for h in range(2):
        u = [line_ref[pl.ds(32 * h + i, 8, stride=4), :] for i in range(4)]
        for i in range(4):
            put(base + 32 * h + i, combine4([coef_ref[tile, 4 * i + m] for m in range(4)], u))


def merge(own_ref, own_jac_ref, landed_ref, out_ref, jac_ref):
    left = lax.broadcasted_iota(jnp.int32, (8, LANES), 1) < LANES // 2

    def rows_of(r, own, put):
        low = [landed_ref[1, c, r, :] for c in range(2)]
        far = [pltpu.roll(landed_ref[0, c, r, :], LANES // 2, 1) for c in range(2)]
        own[0] += low[0]
        own[1] += low[1]
        own[5] += jnp.where(left, 0.0, far[0])
        own[6] += jnp.where(left, far[0], far[1])
        own[7] += far[1]
        for c in range(8):
            put(c, own[c])

    def step(n, carry):
        r = pl.ds(pl.multiple_of(8 * n, 8), 8)

        def put(c, value):
            if c < 7:
                out_ref[r, c * LANES : (c + 1) * LANES] = value
            else:
                out_ref[r, c * LANES : E_NEW] = value[:, : E_NEW - 7 * LANES]

        rows_of(r, [own_ref[c, r, :] for c in range(8)], put)
        return carry

    lax.fori_loop(0, ROWS // 8, step, 0, unroll=4)

    def put_jac(c, value):
        width = min(LANES, E_NEW - c * LANES)
        jac_ref[0:1, c * LANES : c * LANES + width] = value[0:1, :width]

    rows_of(pl.ds(ROWS, 8), [own_jac_ref[c] for c in range(8)], put_jac)


def kernel(
    x_ref, jac_ref, speed_ref, flag_ref, send_ref, source_ref, modes_ref,
    out_ref, out_jac_ref,
    tile_ref, trace_ref, out_buf, ghost_ref, ghost_bf, outside_ref, rate_ref, state_ref, up_ref,
    start_ref, aux_ref, coef_ref, hot_ref, pick_ref, line_ref, own_ref, own_jac_ref,
    blocks_ref, landed_ref, row_buf, col_buf, mine, group,
    fetch_sems, send_sems, recv_sems, row_send, row_recv, col_send, col_recv,
    block_send, block_recv,
):
    me = lax.axis_index("curve")
    devices = ROW_OF * COL_OF
    row_at = me % ROW_OF
    col_at = me // ROW_OF
    near = [(me + devices + o) % devices for o in (-2, -1, 1, 2)]
    row_mates = [col_at * ROW_OF + (row_at + k) % ROW_OF for k in range(1, ROW_OF)]
    col_mates = [((col_at + k) % COL_OF) * ROW_OF + row_at for k in range(1, COL_OF)]
    partners = near + row_mates + col_mates
    barrier = pltpu.get_barrier_semaphore()
    for partner in partners:
        pl.semaphore_signal(barrier, inc=1, device_id=(partner,), device_id_type=MESH)
    fetches = fetch_state(x_ref, tile_ref, fetch_sems)

    def send(src, dst, send_sem, recv_sem, mate):
        copy = pltpu.make_async_remote_copy(
            src_ref=src, dst_ref=dst, send_sem=send_sem, recv_sem=recv_sem,
            device_id=(mate,), device_id_type=MESH,
        )
        copy.start()
        return copy

    count = jnp.sum(flag_ref[...].astype(F32), axis=1, keepdims=True)
    mine[...] = jnp.broadcast_to(count - 64.0, (1, LANES))
    for g in range(GROUPS):
        fetches[g].wait()
        build_traces(tile_ref, trace_ref, g)
    gather_sends(send_ref, trace_ref, out_buf)
    pl.semaphore_wait(barrier, len(partners))
    row_copies = [
        send(mine, row_buf.at[k], row_send.at[k], row_recv.at[k], mate)
        for k, mate in enumerate(row_mates)
    ]
    halo = [
        send(out_buf.at[b], ghost_ref.at[3 - b], send_sems.at[b], recv_sems.at[3 - b], mate)
        for b, mate in enumerate(near)
    ]
    outside_near(source_ref, trace_ref, outside_ref)
    blend_rates(tile_ref, modes_ref, jac_ref, rate_ref)
    for copy in row_copies:
        copy.wait()
    total = mine[...]
    behind = jnp.zeros((1, LANES), F32)
    for k in range(ROW_OF - 1):
        value = row_buf[k]
        total = total + value
        behind = behind + jnp.where(row_at >= k + 1, value, 0.0)
    group[...] = total
    col_copies = [
        send(group, col_buf.at[k], col_send.at[k], col_recv.at[k], mate)
        for k, mate in enumerate(col_mates)
    ]

    def interior_step(n, carry):
        interior_block(n // GROUPS, n % GROUPS, tile_ref, speed_ref, rate_ref, state_ref)
        return carry

    lax.fori_loop(0, VARS * GROUPS, interior_step, 0)
    refine_tables(flag_ref, jac_ref, start_ref, aux_ref)
    for b in range(4):
        halo[b].wait_send()
        halo[3 - b].wait_recv()
    outside_far(source_ref, ghost_ref, ghost_bf, outside_ref)

    def edge_step(n, carry):
        edge_block(
            n // GROUPS, n % GROUPS, tile_ref, speed_ref, rate_ref, outside_ref, state_ref, up_ref
        )
        return carry

    lax.fori_loop(0, VARS * GROUPS, edge_step, 0)
    for copy in col_copies:
        copy.wait()
    for k in range(COL_OF - 1):
        behind = behind + jnp.where(col_at >= k + 1, col_buf[k], 0.0)

    def table(tile, first):
        return rows8(
            column_tables(tile, first, behind, start_ref, aux_ref, coef_ref, hot_ref)
        )

    def pick(pair):
        pick_ref[...] = jnp.dot(up_ref[...], hot_ref[pair], preferred_element_type=F32)

    blocks = []
    for at, first in enumerate((-2 * LANES, E_NEW)):
        for half in range(2):
            blocks_ref[at, half, ROWS : ROWS + 8, :] = table(2 * at + half, first + half * LANES)
        pick(at)
        for half in range(2):

            def block_step(v, carry, at=at, half=half):
                def put(row, value):
                    blocks_ref[at, half, pl.ds(row, 8, stride=4), :] = value

                interpolate(v, 2 * at + half, half, pick_ref, coef_ref, line_ref, put)
                return carry

            lax.fori_loop(0, VARS, block_step, 0)
            blocks.append(
                send(
                    blocks_ref.at[at, half], landed_ref.at[at, half],
                    block_send.at[2 * at + half], block_recv.at[2 * at + half], near[1 + at],
                )
            )

    def own_step(pair, carry):
        for half in range(2):
            c = 2 * pair + half
            own_jac_ref[c] = table(c + 4, c * LANES)
        pick(pair + 2)
        for half in range(2):

            def one(v, carry, half=half):
                def put(row, value):
                    own_ref[2 * pair + half, pl.ds(row, 8, stride=4), :] = value

                interpolate(v, 2 * pair + half + 4, half, pick_ref, coef_ref, line_ref, put)
                return carry

            lax.fori_loop(0, VARS, one, 0)
        return carry

    lax.fori_loop(0, 4, own_step, 0)
    for copy in blocks:
        copy.wait()
    merge(own_ref, own_jac_ref, landed_ref, out_ref, out_jac_ref)


def vmem(count):
    return [pl.BlockSpec(memory_space=pltpu.VMEM)] * count


def shards(nodal_state, inverse_jacobian, speeds, refine_flags, send_index, face_source):
    x = nodal_state.reshape(ROWS, E_DEV)
    jac = inverse_jacobian.reshape(1, E_DEV)
    flags = refine_flags.reshape(1, E_DEV)
    dma = pltpu.SemaphoreType.DMA
    specs = vmem(7)
    specs[0] = pl.BlockSpec(memory_space=pl.ANY)
    specs[2] = pl.BlockSpec(memory_space=pltpu.SMEM)
    out, out_jac = pl.pallas_call(
        kernel,
        out_shape=(
            jax.ShapeDtypeStruct((ROWS, E_NEW), F32),
            jax.ShapeDtypeStruct((1, E_NEW), F32),
        ),
        in_specs=specs,
        out_specs=tuple(vmem(2)),
        scratch_shapes=[
            pltpu.VMEM((GROUPS, ROWS, LANES), F32),
            pltpu.VMEM((6, 160, E_DEV), BF16),
            pltpu.VMEM((4, 80, LANES), F32),
            pltpu.VMEM((4, 80, LANES), F32),
            pltpu.VMEM((160, E_DEV), BF16),
            pltpu.VMEM((6, 80, E_DEV), F32),
            pltpu.VMEM((8, E_DEV), F32),
            pltpu.VMEM((GROUPS, ROWS, LANES), F32),
            pltpu.VMEM((2 * ROWS, E_DEV), BF16),
            pltpu.VMEM((2, E_DEV, LANES), F32),
            pltpu.VMEM((16, E_DEV), BF16),
            pltpu.VMEM((12, 40, 8, LANES), F32),
            pltpu.VMEM((6, E_DEV, 2 * LANES), BF16),
            pltpu.VMEM((2 * ROWS, 2 * LANES), F32),
            pltpu.VMEM((64, LANES), F32),
            pltpu.VMEM((8, ROWS, LANES), F32),
            pltpu.VMEM((8, 8, LANES), F32),
            pltpu.VMEM((2, 2, ROWS + 8, LANES), F32),
            pltpu.VMEM((2, 2, ROWS + 8, LANES), F32),
            pltpu.VMEM((ROW_OF - 1, 1, LANES), F32),
            pltpu.VMEM((COL_OF - 1, 1, LANES), F32),
            pltpu.VMEM((1, LANES), F32),
            pltpu.VMEM((1, LANES), F32),
            dma((GROUPS,)), dma((4,)), dma((4,)), dma((ROW_OF - 1,)), dma((ROW_OF - 1,)),
            dma((COL_OF - 1,)), dma((COL_OF - 1,)), dma((4,)), dma((4,)),
        ],
        compiler_params=pltpu.CompilerParams(collective_id=0, has_side_effects=True),
        name="step",
    )(x, jac, speeds, flags, send_index, face_source, jnp.asarray(MODES, F32))
    return out.reshape(VARS, 64, E_NEW), out_jac.reshape(E_NEW)


def solution(mesh):
    axis = P("curve")
    wide = P(None, None, "curve")
    return jax.shard_map(
        shards,
        mesh=mesh,
        in_specs=(wide, axis, P(), axis, axis, P(None, "curve")),
        out_specs=(wide, axis),
        check_vma=False,
    )
```

```python
import functools
import math

import jax
import jax.numpy as jnp
import numpy as np
from jax import lax
from jax.experimental import pallas as pl
from jax.experimental.pallas import tpu as pltpu
from jax.sharding import PartitionSpec as P

TIME_STEP = 0.02
VARS = 5
E_DEV = 512
E_NEW = 960
SLOTS = 96
ROWS = 64 * VARS
LANES = 128
GROUPS = E_DEV // LANES
ROW_OF = 8
COL_OF = 16
F32 = jnp.float32
BF16 = jnp.bfloat16
MESH = pl.DeviceIdType.MESH


def lagrange_at(points, targets):
    values_at = np.ones((len(targets), 4))
    for basis_id in range(4):
        for partner in range(4):
            if partner != basis_id:
                values_at[:, basis_id] *= (targets - points[partner]) / (
                    points[basis_id] - points[partner]
                )
    return values_at


def tables():
    root = 1.0 / math.sqrt(5.0)
    points = np.array([-1.0, -root, root, 1.0])
    weights = np.array([1.0, 5.0, 5.0, 1.0]) / 6.0
    bary = np.ones(4)
    for a in range(4):
        for b in range(4):
            if a != b:
                bary[a] /= points[a] - points[b]
    deriv = np.zeros((4, 4))
    for a in range(4):
        for b in range(4):
            if a != b:
                deriv[a, b] = bary[b] / bary[a] / (points[a] - points[b])
        deriv[a, a] = -np.sum(deriv[a])
    skew = weights[:, None] * deriv
    legendre = np.stack(
        [points**0, points, 0.5 * (3 * points**2 - 1), 0.5 * (5 * points**3 - 3 * points)], axis=1
    )
    to_modes = np.linalg.inv(legendre)
    sides = [lagrange_at(points, (points - 1.0) / 2.0), lagrange_at(points, (points + 1.0) / 2.0)]
    return skew, np.kron(to_modes, np.kron(to_modes, to_modes)), sides


SKEW, MODES, SIDES = tables()
Q01, Q02, Q03, Q12 = (float(SKEW[0, 1]), float(SKEW[0, 2]), float(SKEW[0, 3]), float(SKEW[1, 2]))
END, MID = 6.0, 1.2


def split2(x):
    high = x.astype(BF16)
    return high, (x - high.astype(F32)).astype(BF16)


def low_half(shape):
    return (lax.broadcasted_iota(jnp.int32, shape, 0) & 7) < 4


def turn(x):
    return pltpu.roll(x, 4, 0)


def fetch_state(x_ref, tile_ref, sems):
    copies = []
    for g in range(GROUPS):
        copy = pltpu.make_async_copy(
            x_ref.at[:, g * LANES : (g + 1) * LANES], tile_ref.at[g], sems.at[g]
        )
        copy.start()
        copies.append(copy)
    return copies


def build_traces(tile_ref, trace_ref, g):
    low = low_half((8, LANES))
    cols = slice(g * LANES, (g + 1) * LANES)
    for v in range(VARS):
        base = 64 * v
        tiles = [tile_ref[g, base + 8 * t : base + 8 * t + 8, :] for t in range(8)]
        first, last = tiles[0::2], tiles[1::2]
        sets = {
            0: [tile_ref[g, pl.ds(base + 32 * h, 8, stride=4), :] for h in range(2)],
            1: [tile_ref[g, pl.ds(base + 32 * h + 3, 8, stride=4), :] for h in range(2)],
            2: [jnp.where(low, first[k], turn(first[k + 1])) for k in (0, 2)],
            3: [jnp.where(low, turn(last[k]), last[k + 1]) for k in (0, 2)],
            4: tiles[0:2],
            5: tiles[6:8],
        }
        for f, rows in sets.items():
            high, rest = split2(jnp.concatenate(rows, axis=0))
            trace_ref[f, 16 * v : 16 * v + 16, cols] = high
            trace_ref[f, 80 + 16 * v : 96 + 16 * v, cols] = rest


def one_hot(index, size, width):
    rows = lax.broadcasted_iota(jnp.int32, (size, width), 0)
    return jnp.where(rows == index, 1.0, 0.0).astype(BF16)


def gather_sends(send_ref, trace_ref, out_ref):
    packed = jnp.broadcast_to(send_ref[...].reshape(1, 4 * SLOTS), (8, 4 * SLOTS))
    for pair in range(2):
        moved = [
            packed if block == 0 else pltpu.roll(packed, 4 * SLOTS - SLOTS * block, 1)
            for block in (2 * pair, 2 * pair + 1)
        ]
        index = jnp.concatenate([m[0:1, 0:LANES] for m in moved], axis=1)
        total = jnp.zeros((160, 2 * LANES), F32)
        for f in range(6):
            total = total + jnp.dot(
                trace_ref[f],
                one_hot(index - f * E_DEV, E_DEV, 2 * LANES),
                preferred_element_type=F32,
            )
        total = total[0:80] + total[80:160]
        for half in range(2):
            out_ref[2 * pair + half] = total[:, half * LANES : (half + 1) * LANES]


def pair_sum(ui, um, si, sm):
    return (si + sm) + ui * um


def line_update(u, coef):
    ca, cb, c02, c03, cd = coef
    s = [x * x for x in u]
    m = [jnp.abs(x) for x in u]
    e = []
    for n, c in ((0, ca), (1, cb), (2, ca)):
        g = pair_sum(u[n], u[n + 1], s[n], s[n + 1])
        e.append(c * g - cd * (jnp.maximum(m[n], m[n + 1]) * (u[n + 1] - u[n])))
    r02 = c02 * pair_sum(u[0], u[2], s[0], s[2])
    r13 = c02 * pair_sum(u[1], u[3], s[1], s[3])
    r03 = c03 * pair_sum(u[0], u[3], s[0], s[3])
    t0 = -(e[0] + r02 + r03)
    t1 = e[0] - e[1] - r13
    t2 = e[1] - e[2] + r02
    t3 = e[2] + r13 + r03
    return t0, t1, t2, t3


def edge(u, o, cg, cd):
    g = pair_sum(u, o, u * u, o * o)
    return cg * g - cd * (jnp.maximum(jnp.abs(u), jnp.abs(o)) * (u - o))


def rows8(x):
    return jnp.broadcast_to(x, (8, LANES))


def blend_rates(tile_ref, modes_ref, jac_ref, rate_ref):
    n = lax.broadcasted_iota(jnp.int32, (64, LANES), 0)
    top = ((n & 3) == 3) | ((n & 12) == 12) | (n >= 48)
    for g in range(GROUPS):
        cols = slice(g * LANES, (g + 1) * LANES)
        modal = jnp.dot(
            modes_ref[...], tile_ref[g, 0:64, :], precision=lax.Precision.HIGHEST,
            preferred_element_type=F32,
        )
        energy = modal * modal
        high = jnp.sum(jnp.where(top, energy, 0.0), axis=0, keepdims=True)
        full = jnp.sum(energy, axis=0, keepdims=True)
        ratio = high / (full + 1e-06)
        blend = 0.5 * ratio / (ratio + 0.1)
        step = TIME_STEP * jac_ref[0:1, cols]
        rate_ref[0:1, cols] = step * (1.0 - blend)
        rate_ref[1:2, cols] = step * blend
        rate_ref[2:3, cols] = step


def outside_near(source_ref, trace_ref, outside_ref):
    for f in range(6):
        near_row = source_ref[f : f + 1, :] - (f ^ 1) * E_DEV
        total = jnp.dot(
            trace_ref[f ^ 1], one_hot(near_row, E_DEV, E_DEV), preferred_element_type=F32
        )
        outside_ref[f] = total[0:80] + total[80:160]


def outside_far(source_ref, ghost_ref, ghost_bf, outside_ref):
    for slot in range(4):
        high, rest = split2(ghost_ref[slot])
        ghost_bf[0:80, slot * LANES : (slot + 1) * LANES] = high
        ghost_bf[80:160, slot * LANES : (slot + 1) * LANES] = rest
    for f in range(6):
        far = source_ref[f : f + 1, :] - 6 * E_DEV
        slot = (
            (far >= SLOTS).astype(jnp.int32)
            + (far >= 2 * SLOTS).astype(jnp.int32)
            + (far >= 3 * SLOTS).astype(jnp.int32)
        )
        far_row = jnp.where(far >= 0, far + (LANES - SLOTS) * slot, -1)
        total = jnp.dot(ghost_bf[...], one_hot(far_row, E_DEV, E_DEV), preferred_element_type=F32)
        outside_ref[f] += total[0:80] + total[80:160]


def coefs_of(d, v, speed_ref, hi, lo):
    a = speed_ref[d, v]
    third = (a / 3.0) * hi
    sixth = (a / 6.0) * lo
    return [
        rows8(c)
        for c in (
            Q01 * third + sixth, Q12 * third + sixth, Q02 * third, Q03 * third,
            (0.5 * jnp.abs(a)) * lo,
        )
    ]


def interior_block(v, g, tile_ref, speed_ref, rate_ref, state_ref):
    base = pl.multiple_of(64 * v, 64)
    cols = pl.ds(pl.multiple_of(g * LANES, LANES), LANES)
    hi = rate_ref[0:1, cols]
    lo = rate_ref[1:2, cols]
    low = low_half((8, LANES))
    coef = coefs_of(0, v, speed_ref, hi, lo)
    for h in range(2):
        u = [tile_ref[g, pl.ds(base + 32 * h + i, 8, stride=4), :] for i in range(4)]
        t = line_update(u, coef)
        for i, w in enumerate((END, MID, MID, END)):
            state_ref[g, pl.ds(base + 32 * h + i, 8, stride=4), :] = u[i] + w * t[i]
    tiles = [tile_ref[g, pl.ds(base + 8 * t, 8), :] for t in range(8)]
    coef = coefs_of(2, v, speed_ref, hi, lo)
    total = [None] * 8
    for h in range(2):
        t = line_update([tiles[2 * k + h] for k in range(4)], coef)
        for k, w in enumerate((END, MID, MID, END)):
            total[2 * k + h] = w * t[k]
    ca, cb, c02, c03, cd = coefs_of(1, v, speed_ref, hi, lo)
    signed = jnp.where(low, -ca, ca)
    cross = jnp.where(low, -c03, -cb)
    cross_d = jnp.where(low, 0.0, cd)
    wa = jnp.where(low, END, MID)
    wb = jnp.where(low, MID, END)
    for k in range(4):
        a, b = tiles[2 * k], tiles[2 * k + 1]
        at, bt = turn(a), turn(b)
        sa, sb, sat, sbt = a * a, b * b, at * at, bt * bt
        ma, mb, mat, mbt = jnp.abs(a), jnp.abs(b), jnp.abs(at), jnp.abs(bt)
        x1 = signed * pair_sum(a, at, sa, sat) + cd * (jnp.maximum(ma, mat) * (at - a))
        x2 = signed * pair_sum(b, bt, sb, sbt) + cd * (jnp.maximum(mb, mbt) * (bt - b))
        x3 = c02 * pair_sum(a, b, sa, sb)
        x4 = cross * pair_sum(a, bt, sa, sbt) + cross_d * (jnp.maximum(ma, mbt) * (bt - a))
        total[2 * k] += wa * (x1 - x3 + x4)
        total[2 * k + 1] += wb * (x2 + x3 - turn(x4))
    for t in range(8):
        state_ref[g, pl.ds(base + 8 * t, 8), :] += total[t]


def edge_block(v, g, tile_ref, speed_ref, rate_ref, outside_ref, state_ref, up_ref):
    base = pl.multiple_of(64 * v, 64)
    face = pl.multiple_of(16 * v, 16)
    cols = pl.ds(pl.multiple_of(g * LANES, LANES), LANES)
    step = rate_ref[2:3, cols]
    low = low_half((8, LANES))

    def coefs(d):
        a = speed_ref[d, v]
        return rows8((a * (END / 6.0)) * step), rows8((0.5 * END) * jnp.abs(a) * step)

    bg, bd = coefs(0)
    for h in range(2):
        for f, i, sign in ((0, 0, bg), (1, 3, -bg)):
            rows = pl.ds(base + 32 * h + i, 8, stride=4)
            outer = outside_ref[f, pl.ds(face + 8 * h, 8), cols]
            state_ref[g, rows, :] += edge(tile_ref[g, rows, :], outer, sign, bd)
    tiles = [tile_ref[g, pl.ds(base + 8 * t, 8), :] for t in range(8)]
    total = [state_ref[g, pl.ds(base + 8 * t, 8), :] for t in range(8)]
    bg, bd = coefs(2)
    for h in range(2):
        for f, k, sign in ((4, 0, bg), (5, 3, -bg)):
            outer = outside_ref[f, pl.ds(face + 8 * h, 8), cols]
            total[2 * k + h] += edge(tiles[2 * k + h], outer, sign, bd)
    bg, bd = coefs(1)
    bgs = jnp.where(low, bg, -bg)
    outer_l = [outside_ref[2, pl.ds(face + 8 * h, 8), cols] for h in range(2)]
    outer_r = [outside_ref[3, pl.ds(face + 8 * h, 8), cols] for h in range(2)]
    for k in range(4):
        ol = outer_l[k // 2]
        orr = outer_r[k // 2]
        outer = jnp.where(low, ol, turn(orr)) if k % 2 == 0 else jnp.where(low, turn(ol), orr)
        bound = edge(jnp.where(low, tiles[2 * k], tiles[2 * k + 1]), outer, bgs, bd)
        total[2 * k] += jnp.where(low, bound, 0.0)
        total[2 * k + 1] += jnp.where(low, 0.0, bound)
    for t in range(4):
        high, rest = split2(jnp.concatenate(total[2 * t : 2 * t + 2], axis=0))
        up_ref[pl.ds(pl.multiple_of(base + 16 * t, 16), 16), cols] = high
        up_ref[pl.ds(pl.multiple_of(ROWS + base + 16 * t, 16), 16), cols] = rest


def refine_tables(flag_ref, jac_ref, start_ref, aux_ref):
    flags = flag_ref[...].astype(F32)
    wide = jnp.broadcast_to(flags, (LANES, E_DEV)).astype(BF16)
    row = lax.broadcasted_iota(jnp.int32, (E_DEV, E_DEV), 0)
    col = lax.broadcasted_iota(jnp.int32, (E_DEV, E_DEV), 1)
    ahead = jnp.where(col < row, 1.0, 0.0).astype(BF16)
    within = jnp.where(col <= row, 1.0, 0.0).astype(BF16)
    dims = (((1,), (1,)), ((), ()))
    place = lax.broadcasted_iota(jnp.int32, (E_DEV, LANES), 0).astype(F32)
    start_ref[0] = place + 7.0 * lax.dot_general(ahead, wide, dims, preferred_element_type=F32)
    start_ref[1] = (
        place + 1.0 + 7.0 * lax.dot_general(within, wide, dims, preferred_element_type=F32)
    )
    count = lax.dot_general(wide[0:16], ahead, dims, preferred_element_type=F32)[0:1]
    at = lax.broadcasted_iota(jnp.int32, (1, E_DEV), 1).astype(F32) + 7.0 * count
    at_high = jnp.floor(at * (1.0 / 16.0))
    jac = jac_ref[...]
    j0, rest = split2(jac)
    rest = jac - j0.astype(F32)
    j1 = rest.astype(BF16)
    j2 = (rest - j1.astype(F32)).astype(BF16)
    zero = jnp.zeros((10, E_DEV), F32)
    aux_ref[...] = jnp.concatenate(
        [
            at_high, at - 16.0 * at_high, flags, j0.astype(F32), j1.astype(F32), j2.astype(F32),
            zero,
        ],
        axis=0,
    ).astype(BF16)


def column_tables(tile, first, start_ref, aux_ref, coef_ref, hot_ref):
    place = lax.broadcasted_iota(jnp.int32, (1, LANES), 1).astype(F32) + first
    inside = (place >= start_ref[0]) & (place < start_ref[1])
    hot = jnp.where(inside, 1.0, 0.0).astype(BF16)
    cols = pl.ds(pl.multiple_of((tile % 2) * LANES, LANES), LANES)
    hot_ref[tile // 2, :, cols] = hot
    aux = jnp.dot(aux_ref[...], hot, preferred_element_type=F32)
    child = place - (16.0 * aux[0:1] + aux[1:2])
    refined = aux[2:3] > 0.5
    z = child >= 4.0
    child = child - jnp.where(z, 4.0, 0.0)
    y = child >= 2.0
    child = child - jnp.where(y, 2.0, 0.0)
    x = child >= 1.0
    jac = (aux[3:4] + aux[4:5] + aux[5:6]) * jnp.where(refined, 2.0, 1.0)

    def table(bit):
        return [
            [
                rows8(
                    jnp.where(
                        refined,
                        jnp.where(bit, float(SIDES[1][i, m]), float(SIDES[0][i, m])),
                        1.0 if i == m else 0.0,
                    )
                )
                for m in range(4)
            ]
            for i in range(4)
        ]

    cx, cy, cz = table(x), table(y), table(z)
    low = low_half((8, LANES))
    n = 0
    for i in range(4):
        for m in range(4):
            coef_ref[tile, n] = cx[i][m]
            coef_ref[tile, 16 + n] = cz[i][m]
            n += 1
    order = [(0, 1), (1, 0), (2, 3), (3, 2)]
    for at, (first_j, last_j) in enumerate(((0, 1), (2, 3))):
        for k, (lo_m, hi_m) in enumerate(order):
            coef_ref[tile, 32 + 4 * at + k] = jnp.where(low, cy[first_j][lo_m], cy[last_j][hi_m])
    return jac


def combine4(c, u):
    return (c[0] * u[0] + c[1] * u[1]) + (c[2] * u[2] + c[3] * u[3])


def interpolate(v, tile, half, pick_ref, coef_ref, line_ref, put):
    base = pl.multiple_of(64 * v, 64)
    cols = slice(half * LANES, half * LANES + LANES)
    tiles = [
        pick_ref[pl.ds(base + 8 * t, 8), cols] + pick_ref[pl.ds(ROWS + base + 8 * t, 8), cols]
        for t in range(8)
    ]
    mid = [None] * 8
    for h in range(2):
        u = [tiles[2 * k + h] for k in range(4)]
        for k in range(4):
            mid[2 * k + h] = combine4([coef_ref[tile, 16 + 4 * k + m] for m in range(4)], u)
    for k in range(4):
        a, b = mid[2 * k], mid[2 * k + 1]
        u = [a, turn(a), b, turn(b)]
        for at in range(2):
            line_ref[16 * k + 8 * at : 16 * k + 8 * at + 8, :] = combine4(
                [coef_ref[tile, 32 + 4 * at + m] for m in range(4)], u
            )
    for h in range(2):
        u = [line_ref[pl.ds(32 * h + i, 8, stride=4), :] for i in range(4)]
        for i in range(4):
            put(base + 32 * h + i, combine4([coef_ref[tile, 4 * i + m] for m in range(4)], u))


TILES = 13
FRAME = ROWS + 8


def kernel(
    x_hbm, jac_hbm, speed_hbm, flag_hbm, send_hbm, source_hbm, modes_hbm,
    frame_ref, head_ref, info_ref,
    jac_ref, speed_ref, flag_ref, send_ref, source_ref, modes_ref,
    tile_ref, trace_ref, out_buf, ghost_ref, ghost_bf, outside_ref, rate_ref, state_ref, up_ref,
    start_ref, aux_ref, coef_ref, hot_ref, pick_ref, line_ref, tail_ref,
    row_buf, col_buf, mine, group,
    small_sems, fetch_sems, send_sems, recv_sems, row_send, row_recv, col_send, col_recv,
    head_send, head_recv, tail_send, tail_recv,
):
    me = lax.axis_index("curve")
    devices = ROW_OF * COL_OF
    row_at = me % ROW_OF
    col_at = me // ROW_OF
    near = [(me + devices + o) % devices for o in (-2, -1, 1, 2)]
    row_mates = [col_at * ROW_OF + (row_at + k) % ROW_OF for k in range(1, ROW_OF)]
    barrier = pltpu.get_barrier_semaphore()
    for partner in near + row_mates:
        pl.semaphore_signal(barrier, inc=1, device_id=(partner,), device_id_type=MESH)
    for k in range(1, COL_OF):

        @pl.when(col_at >= k)
        def _(k=k):
            pl.semaphore_signal(
                barrier, inc=1, device_id=(me - k * ROW_OF,), device_id_type=MESH
            )

    fetches = fetch_state(x_hbm, tile_ref, fetch_sems)
    small = []
    for at, (src, dst) in enumerate(
        (
            (send_hbm, send_ref), (flag_hbm, flag_ref), (source_hbm, source_ref),
            (jac_hbm, jac_ref), (modes_hbm, modes_ref), (speed_hbm, speed_ref),
        )
    ):
        copy = pltpu.make_async_copy(src, dst, small_sems.at[at])
        copy.start()
        small.append(copy)

    def send(src, dst, send_sem, recv_sem, mate):
        copy = remote(src, dst, send_sem, recv_sem, mate)
        copy.start()
        return copy

    def remote(src, dst, send_sem, recv_sem, mate):
        return pltpu.make_async_remote_copy(
            src_ref=src, dst_ref=dst, send_sem=send_sem, recv_sem=recv_sem,
            device_id=(mate,), device_id_type=MESH,
        )

    for g in range(GROUPS):
        fetches[g].wait()
        build_traces(tile_ref, trace_ref, g)
    for copy in small:
        copy.wait()
    gather_sends(send_ref, trace_ref, out_buf)
    count = jnp.sum(flag_ref[...].astype(F32), axis=1, keepdims=True)
    mine[...] = jnp.broadcast_to(count, (1, LANES)).astype(jnp.int32) - 64
    pl.semaphore_wait(barrier, 4 + ROW_OF - 1 + COL_OF - 1 - col_at)
    halo = [
        send(out_buf.at[b], ghost_ref.at[3 - b], send_sems.at[b], recv_sems.at[3 - b], mate)
        for b, mate in enumerate(near)
    ]
    row_copies = [
        send(mine, row_buf.at[k], row_send.at[k], row_recv.at[k], mate)
        for k, mate in enumerate(row_mates)
    ]
    outside_near(source_ref, trace_ref, outside_ref)
    blend_rates(tile_ref, modes_ref, jac_ref, rate_ref)

    def interior_step(n, carry):
        interior_block(n // GROUPS, n % GROUPS, tile_ref, speed_ref, rate_ref, state_ref)
        return carry

    lax.fori_loop(0, VARS * GROUPS, interior_step, 0)
    refine_tables(flag_ref, jac_ref, start_ref, aux_ref)
    total_new = 7.0 * jnp.broadcast_to(count, (1, LANES)) + float(E_DEV)

    def table_step(tile, carry):
        shift = (jnp.full((1, LANES), tile, jnp.int32) * LANES).astype(F32)
        first = shift - 2.0 * LANES + jnp.where(tile < 2, total_new, 0.0)
        jac_row = rows8(column_tables(tile, first, start_ref, aux_ref, coef_ref, hot_ref))

        @pl.when(tile < 2)
        def _():
            tail_ref[tile, ROWS:FRAME, :] = jac_row

        @pl.when(tile >= 2)
        def _():
            frame_ref[tile, ROWS:FRAME, :] = jac_row

        return carry

    lax.fori_loop(0, TILES, table_step, 0)

    for copy in row_copies:
        copy.wait()
    total = mine[...]
    behind = jnp.zeros((1, LANES), jnp.int32)
    for k in range(ROW_OF - 1):
        value = row_buf[k]
        total = total + value
        behind = behind + jnp.where(row_at >= k + 1, value, 0)
    group[...] = total
    col_copies = [
        remote(
            group, col_buf.at[k - 1], col_send.at[k - 1], col_recv.at[k - 1],
            (me + k * ROW_OF) % devices,
        )
        for k in range(1, COL_OF)
    ]
    for k in range(1, COL_OF):

        @pl.when(col_at + k < COL_OF)
        def _(k=k):
            col_copies[k - 1].start()

    for b in range(4):
        halo[b].wait_send()
        halo[3 - b].wait_recv()
    outside_far(source_ref, ghost_ref, ghost_bf, outside_ref)

    def edge_step(n, carry):
        edge_block(
            n // GROUPS, n % GROUPS, tile_ref, speed_ref, rate_ref, outside_ref, state_ref, up_ref
        )
        return carry

    lax.fori_loop(0, VARS * GROUPS, edge_step, 0)

    def pick(pair):
        pick_ref[...] = jnp.dot(up_ref[...], hot_ref[pair], preferred_element_type=F32)

    def fill(dst_ref, dst, tile, half):
        def one(v, carry):
            def put(row, value):
                dst_ref[dst, pl.ds(row, 8, stride=4), :] = value

            interpolate(v, tile, half, pick_ref, coef_ref, line_ref, put)
            return carry

        lax.fori_loop(0, VARS, one, 0)

    first, last = me == 0, me == devices - 1
    tails = [
        remote(tail_ref.at[h], frame_ref.at[h], tail_send.at[h], tail_recv.at[h], near[2])
        for h in range(2)
    ]
    heads = [
        remote(frame_ref.at[2 + h], head_ref.at[h], head_send.at[h], head_recv.at[h], near[1])
        for h in range(2)
    ]
    pick(0)
    for half in range(2):
        fill(tail_ref, half, half, half)
        pl.when(jnp.logical_not(last))(tails[half].start)
    pick(1)
    for half in range(2):
        fill(frame_ref, 2 + half, 2 + half, half)
        pl.when(jnp.logical_not(first))(heads[half].start)

    def own_step(pair, carry):
        pick(pair)
        for half in range(2):
            fill(frame_ref, 2 * pair + half, 2 * pair + half, half)
        return carry

    lax.fori_loop(2, 6, own_step, 0)
    pick_ref[:, 0:LANES] = jnp.dot(
        up_ref[...], hot_ref[6, :, 0:LANES], preferred_element_type=F32
    )
    fill(frame_ref, TILES - 1, TILES - 1, 0)

    for k in range(1, COL_OF):

        @pl.when(col_at + k < COL_OF)
        def _(k=k):
            col_copies[k - 1].wait_send()

        @pl.when(col_at >= k)
        def _(k=k):
            col_copies[k - 1].wait_recv()

    for k in range(1, COL_OF):
        behind = behind + jnp.where(col_at >= k, col_buf[k - 1], 0)
    info_ref[0:1, :] = behind
    info_ref[1:2, :] = total_new.astype(jnp.int32)
    for half in range(2):

        @pl.when(jnp.logical_not(last))
        def _(half=half):
            tails[half].wait_send()
            heads[half].wait_recv()

        @pl.when(jnp.logical_not(first))
        def _(half=half):
            heads[half].wait_send()
            tails[half].wait_recv()


def place_kernel(frame_ref, head_ref, info_ref, out_ref, jac_ref):
    shift = 7 * jnp.max(info_ref[0:1, :])
    size = jnp.max(info_ref[1:2, :])
    begin = 2 * LANES - shift
    tile = begin // LANES
    turn_by = begin - tile * LANES
    over = -(size + shift)
    head_tile = over // LANES
    head_turn = over - head_tile * LANES
    lane = lax.broadcasted_iota(jnp.int32, (8, LANES), 1)
    kept = lane < LANES - turn_by
    head_kept = lane < LANES - head_turn
    back = (LANES - turn_by) % LANES
    head_back = (LANES - head_turn) % LANES

    def row_tile(rows):
        parts = [pltpu.roll(frame_ref[tile + c, rows, :], back, 1) for c in range(9)]
        out = [jnp.where(kept, parts[c], parts[c + 1]) for c in range(8)]
        ends = []
        for c in range(4):
            at = head_tile + 5 + c
            part = pltpu.roll(head_ref[jnp.clip(at, 0, 1), rows, :], head_back, 1)
            ends.append(jnp.where((at >= 0) & (at < 2), part, 0.0))
        for c in range(3):
            value = jnp.where(head_kept, ends[c], ends[c + 1])
            out[5 + c] = out[5 + c] + value
        return out

    base = pl.program_id(0) * 64

    def step(n, carry):
        out = row_tile(pl.ds(pl.multiple_of(base + 8 * n, 8), 8))
        rows = pl.ds(pl.multiple_of(8 * n, 8), 8)
        for c in range(7):
            out_ref[rows, c * LANES : (c + 1) * LANES] = out[c]
        out_ref[rows, 7 * LANES : E_NEW] = out[7][:, : E_NEW - 7 * LANES]
        return carry

    lax.fori_loop(0, 8, step, 0, unroll=2)

    @pl.when(pl.program_id(0) == 0)
    def _():
        out = row_tile(pl.ds(ROWS, 8))
        for c in range(8):
            width = min(LANES, E_NEW - c * LANES)
            jac_ref[0:1, c * LANES : c * LANES + width] = out[c][0:1, :width]


def vmem(count):
    return [pl.BlockSpec(memory_space=pltpu.VMEM)] * count


def shards(nodal_state, inverse_jacobian, speeds, refine_flags, send_index, face_source):
    x = nodal_state.reshape(ROWS, E_DEV)
    jac = inverse_jacobian.reshape(1, E_DEV)
    flags = refine_flags.reshape(1, E_DEV)
    dma = pltpu.SemaphoreType.DMA
    frame, head, info = pl.pallas_call(
        kernel,
        out_shape=(
            jax.ShapeDtypeStruct((TILES, FRAME, LANES), F32),
            jax.ShapeDtypeStruct((2, FRAME, LANES), F32),
            jax.ShapeDtypeStruct((2, LANES), jnp.int32),
        ),
        in_specs=[pl.BlockSpec(memory_space=pltpu.HBM)] * 7,
        out_specs=tuple(vmem(3)),
        scratch_shapes=[
            pltpu.VMEM((1, E_DEV), F32),
            pltpu.SMEM((3, VARS), F32),
            pltpu.VMEM((1, E_DEV), jnp.int32),
            pltpu.VMEM((4 * SLOTS,), jnp.int32),
            pltpu.VMEM((6, E_DEV), jnp.int32),
            pltpu.VMEM((64, 64), F32),
            pltpu.VMEM((GROUPS, ROWS, LANES), F32),
            pltpu.VMEM((6, 160, E_DEV), BF16),
            pltpu.VMEM((4, 80, LANES), F32),
            pltpu.VMEM((4, 80, LANES), F32),
            pltpu.VMEM((160, E_DEV), BF16),
            pltpu.VMEM((6, 80, E_DEV), F32),
            pltpu.VMEM((8, E_DEV), F32),
            pltpu.VMEM((GROUPS, ROWS, LANES), F32),
            pltpu.VMEM((2 * ROWS, E_DEV), BF16),
            pltpu.VMEM((2, E_DEV, LANES), F32),
            pltpu.VMEM((16, E_DEV), BF16),
            pltpu.VMEM((TILES, 40, 8, LANES), F32),
            pltpu.VMEM((7, E_DEV, 2 * LANES), BF16),
            pltpu.VMEM((2 * ROWS, 2 * LANES), F32),
            pltpu.VMEM((64, LANES), F32),
            pltpu.VMEM((2, FRAME, LANES), F32),
            pltpu.VMEM((ROW_OF - 1, 1, LANES), jnp.int32),
            pltpu.VMEM((COL_OF - 1, 1, LANES), jnp.int32),
            pltpu.VMEM((1, LANES), jnp.int32),
            pltpu.VMEM((1, LANES), jnp.int32),
            dma((6,)), dma((GROUPS,)), dma((4,)), dma((4,)), dma((ROW_OF - 1,)),
            dma((ROW_OF - 1,)), dma((COL_OF - 1,)), dma((COL_OF - 1,)),
            dma((2,)), dma((2,)), dma((2,)), dma((2,)),
        ],
        compiler_params=pltpu.CompilerParams(
            collective_id=0, has_side_effects=True, vmem_limit_bytes=24 << 20
        ),
        name="step",
    )(*[
        pltpu.with_memory_space_constraint(a, pltpu.HBM)
        for a in (x, jac, speeds, flags, send_index, face_source, jnp.asarray(MODES, F32))
    ])
    out, out_jac = pl.pallas_call(
        place_kernel,
        grid=(VARS,),
        out_shape=(
            jax.ShapeDtypeStruct((ROWS, E_NEW), F32),
            jax.ShapeDtypeStruct((1, E_NEW), F32),
        ),
        in_specs=vmem(3),
        out_specs=(
            pl.BlockSpec((64, E_NEW), lambda v: (v, 0)),
            pl.BlockSpec((1, E_NEW), lambda v: (0, 0)),
        ),
        compiler_params=pltpu.CompilerParams(vmem_limit_bytes=16 << 20),
        name="place",
    )(frame, head, info)
    return out.reshape(VARS, 64, E_NEW), out_jac.reshape(E_NEW)


def solution(mesh):
    axis = P("curve")
    wide = P(None, None, "curve")
    return jax.shard_map(
        shards,
        mesh=mesh,
        in_specs=(wide, axis, P(), axis, axis, P(None, "curve")),
        out_specs=(wide, axis),
        check_vma=False,
    )
```

```python
import functools
import math

import jax
import jax.numpy as jnp
import numpy as np
from jax import lax
from jax.experimental import pallas as pl
from jax.experimental.pallas import tpu as pltpu
from jax.sharding import PartitionSpec as P

TIME_STEP = 0.02
VARS = 5
E_DEV = 512
E_NEW = 960
SLOTS = 96
ROWS = 64 * VARS
LANES = 128
GROUPS = E_DEV // LANES
ROW_OF = 8
COL_OF = 16
F32 = jnp.float32
BF16 = jnp.bfloat16
MESH = pl.DeviceIdType.MESH


def lagrange_at(points, targets):
    values_at = np.ones((len(targets), 4))
    for basis_id in range(4):
        for partner in range(4):
            if partner != basis_id:
                values_at[:, basis_id] *= (targets - points[partner]) / (
                    points[basis_id] - points[partner]
                )
    return values_at


def tables():
    root = 1.0 / math.sqrt(5.0)
    points = np.array([-1.0, -root, root, 1.0])
    weights = np.array([1.0, 5.0, 5.0, 1.0]) / 6.0
    bary = np.ones(4)
    for a in range(4):
        for b in range(4):
            if a != b:
                bary[a] /= points[a] - points[b]
    deriv = np.zeros((4, 4))
    for a in range(4):
        for b in range(4):
            if a != b:
                deriv[a, b] = bary[b] / bary[a] / (points[a] - points[b])
        deriv[a, a] = -np.sum(deriv[a])
    skew = weights[:, None] * deriv
    legendre = np.stack(
        [points**0, points, 0.5 * (3 * points**2 - 1), 0.5 * (5 * points**3 - 3 * points)], axis=1
    )
    to_modes = np.linalg.inv(legendre)
    sides = [lagrange_at(points, (points - 1.0) / 2.0), lagrange_at(points, (points + 1.0) / 2.0)]
    return skew, np.kron(to_modes, np.kron(to_modes, to_modes)), sides


SKEW, MODES, SIDES = tables()
Q01, Q02, Q03, Q12 = (float(SKEW[0, 1]), float(SKEW[0, 2]), float(SKEW[0, 3]), float(SKEW[1, 2]))
END, MID = 6.0, 1.2


def split2(x):
    high = x.astype(BF16)
    return high, (x - high.astype(F32)).astype(BF16)


def low_half(shape):
    return (lax.broadcasted_iota(jnp.int32, shape, 0) & 7) < 4


def turn(x):
    return pltpu.roll(x, 4, 0)


def fetch_state(x_ref, tile_ref, sems):
    copies = []
    for g in range(GROUPS):
        copy = pltpu.make_async_copy(
            x_ref.at[:, g * LANES : (g + 1) * LANES], tile_ref.at[g], sems.at[g]
        )
        copy.start()
        copies.append(copy)
    return copies


def build_traces(tile_ref, trace_ref, g):
    low = low_half((8, LANES))
    cols = slice(g * LANES, (g + 1) * LANES)
    for v in range(VARS):
        base = 64 * v
        tiles = [tile_ref[g, base + 8 * t : base + 8 * t + 8, :] for t in range(8)]
        first, last = tiles[0::2], tiles[1::2]
        sets = {
            0: [tile_ref[g, pl.ds(base + 32 * h, 8, stride=4), :] for h in range(2)],
            1: [tile_ref[g, pl.ds(base + 32 * h + 3, 8, stride=4), :] for h in range(2)],
            2: [jnp.where(low, first[k], turn(first[k + 1])) for k in (0, 2)],
            3: [jnp.where(low, turn(last[k]), last[k + 1]) for k in (0, 2)],
            4: tiles[0:2],
            5: tiles[6:8],
        }
        for f, rows in sets.items():
            high, rest = split2(jnp.concatenate(rows, axis=0))
            trace_ref[f, 16 * v : 16 * v + 16, cols] = high
            trace_ref[f, 80 + 16 * v : 96 + 16 * v, cols] = rest


def one_hot(index, size, width):
    rows = lax.broadcasted_iota(jnp.int32, (size, width), 0).astype(jnp.int16)
    index = jnp.broadcast_to(index, (16, width)).astype(jnp.int16)
    index = jnp.concatenate([index] * (size // 16), axis=0)
    return jnp.where(
        rows == index, jnp.ones((size, width), BF16), jnp.zeros((size, width), BF16)
    )


def gather_sends(send_ref, trace_ref, out_ref):
    packed = jnp.broadcast_to(send_ref[...].reshape(1, 4 * SLOTS), (8, 4 * SLOTS))
    for pair in range(2):
        moved = [
            packed if block == 0 else pltpu.roll(packed, 4 * SLOTS - SLOTS * block, 1)
            for block in (2 * pair, 2 * pair + 1)
        ]
        index = jnp.concatenate([m[0:1, 0:LANES] for m in moved], axis=1)
        total = jnp.zeros((160, 2 * LANES), F32)
        for f in range(6):
            total = total + jnp.dot(
                trace_ref[f],
                one_hot(index - f * E_DEV, E_DEV, 2 * LANES),
                preferred_element_type=F32,
            )
        total = total[0:80] + total[80:160]
        for half in range(2):
            out_ref[2 * pair + half] = total[:, half * LANES : (half + 1) * LANES]


def pair_sum(ui, um, si, sm):
    return (si + sm) + ui * um


def line_update(u, coef):
    ca, cb, c02, c03, cd = coef
    s = [x * x for x in u]
    m = [jnp.abs(x) for x in u]
    e = []
    for n, c in ((0, ca), (1, cb), (2, ca)):
        g = pair_sum(u[n], u[n + 1], s[n], s[n + 1])
        e.append(c * g - cd * (jnp.maximum(m[n], m[n + 1]) * (u[n + 1] - u[n])))
    r02 = c02 * pair_sum(u[0], u[2], s[0], s[2])
    r13 = c02 * pair_sum(u[1], u[3], s[1], s[3])
    r03 = c03 * pair_sum(u[0], u[3], s[0], s[3])
    t0 = -(e[0] + r02 + r03)
    t1 = e[0] - e[1] - r13
    t2 = e[1] - e[2] + r02
    t3 = e[2] + r13 + r03
    return t0, t1, t2, t3


def edge(u, o, cg, cd):
    g = pair_sum(u, o, u * u, o * o)
    return cg * g - cd * (jnp.maximum(jnp.abs(u), jnp.abs(o)) * (u - o))


def rows8(x):
    return jnp.broadcast_to(x, (8, LANES))


def blend_rates(tile_ref, modes_ref, jac_ref, rate_ref):
    n = lax.broadcasted_iota(jnp.int32, (64, LANES), 0)
    top = ((n & 3) == 3) | ((n & 12) == 12) | (n >= 48)
    for g in range(GROUPS):
        cols = slice(g * LANES, (g + 1) * LANES)
        modal = jnp.dot(
            modes_ref[...], tile_ref[g, 0:64, :], precision=lax.Precision.HIGHEST,
            preferred_element_type=F32,
        )
        energy = modal * modal
        high = jnp.sum(jnp.where(top, energy, 0.0), axis=0, keepdims=True)
        full = jnp.sum(energy, axis=0, keepdims=True)
        ratio = high / (full + 1e-06)
        blend = 0.5 * ratio / (ratio + 0.1)
        step = TIME_STEP * jac_ref[0:1, cols]
        rate_ref[0:1, cols] = step * (1.0 - blend)
        rate_ref[1:2, cols] = step * blend
        rate_ref[2:3, cols] = step


def outside_near(source_ref, trace_ref, far_ref, outside_ref):
    for f in range(6):
        index = source_ref[f : f + 1, :]
        total = jnp.dot(
            trace_ref[f ^ 1],
            one_hot(index - (f ^ 1) * E_DEV, E_DEV, E_DEV),
            preferred_element_type=F32,
        )
        outside_ref[f] = total[0:80] + total[80:160]
        far = index - 6 * E_DEV
        slot = (
            (far >= SLOTS).astype(jnp.int32)
            + (far >= 2 * SLOTS).astype(jnp.int32)
            + (far >= 3 * SLOTS).astype(jnp.int32)
        )
        far_ref[f] = one_hot(
            jnp.where(far >= 0, far + (LANES - SLOTS) * slot, -1), E_DEV, E_DEV
        )


def split_ghost(ghost_ref, ghost_bf):
    for slot in range(4):
        high, rest = split2(ghost_ref[slot])
        ghost_bf[0:80, slot * LANES : (slot + 1) * LANES] = high
        ghost_bf[80:160, slot * LANES : (slot + 1) * LANES] = rest


def outside_far(half, far_ref, ghost_bf, outside_ref):
    cols = pl.ds(pl.multiple_of(2 * LANES * half, 2 * LANES), 2 * LANES)
    for f in range(6):
        total = jnp.dot(ghost_bf[...], far_ref[f, :, cols], preferred_element_type=F32)
        outside_ref[f, :, cols] += total[0:80] + total[80:160]


def coefs_of(d, v, speed_ref, hi, lo):
    a = speed_ref[d, v]
    third = (a / 3.0) * hi
    sixth = (a / 6.0) * lo
    return [
        rows8(c)
        for c in (
            Q01 * third + sixth, Q12 * third + sixth, Q02 * third, Q03 * third,
            (0.5 * jnp.abs(a)) * lo,
        )
    ]


def interior_block(v, g, tile_ref, speed_ref, rate_ref, state_ref):
    base = pl.multiple_of(64 * v, 64)
    cols = pl.ds(pl.multiple_of(g * LANES, LANES), LANES)
    hi = rate_ref[0:1, cols]
    lo = rate_ref[1:2, cols]
    low = low_half((8, LANES))
    coef = coefs_of(0, v, speed_ref, hi, lo)
    for h in range(2):
        u = [tile_ref[g, pl.ds(base + 32 * h + i, 8, stride=4), :] for i in range(4)]
        t = line_update(u, coef)
        for i, w in enumerate((END, MID, MID, END)):
            state_ref[g, pl.ds(base + 32 * h + i, 8, stride=4), :] = u[i] + w * t[i]
    tiles = [tile_ref[g, pl.ds(base + 8 * t, 8), :] for t in range(8)]
    coef = coefs_of(2, v, speed_ref, hi, lo)
    total = [None] * 8
    for h in range(2):
        t = line_update([tiles[2 * k + h] for k in range(4)], coef)
        for k, w in enumerate((END, MID, MID, END)):
            total[2 * k + h] = w * t[k]
    ca, cb, c02, c03, cd = coefs_of(1, v, speed_ref, hi, lo)
    signed = jnp.where(low, -ca, ca)
    cross = jnp.where(low, -c03, -cb)
    cross_d = jnp.where(low, 0.0, cd)
    wa = jnp.where(low, END, MID)
    wb = jnp.where(low, MID, END)
    for k in range(4):
        a, b = tiles[2 * k], tiles[2 * k + 1]
        at, bt = turn(a), turn(b)
        sa, sb, sat, sbt = a * a, b * b, at * at, bt * bt
        ma, mb, mat, mbt = jnp.abs(a), jnp.abs(b), jnp.abs(at), jnp.abs(bt)
        x1 = signed * pair_sum(a, at, sa, sat) + cd * (jnp.maximum(ma, mat) * (at - a))
        x2 = signed * pair_sum(b, bt, sb, sbt) + cd * (jnp.maximum(mb, mbt) * (bt - b))
        x3 = c02 * pair_sum(a, b, sa, sb)
        x4 = cross * pair_sum(a, bt, sa, sbt) + cross_d * (jnp.maximum(ma, mbt) * (bt - a))
        total[2 * k] += wa * (x1 - x3 + x4)
        total[2 * k + 1] += wb * (x2 + x3 - turn(x4))
    for t in range(8):
        state_ref[g, pl.ds(base + 8 * t, 8), :] += total[t]


def edge_block(v, g, tile_ref, speed_ref, rate_ref, outside_ref, state_ref, up_ref):
    base = pl.multiple_of(64 * v, 64)
    face = pl.multiple_of(16 * v, 16)
    cols = pl.ds(pl.multiple_of(g * LANES, LANES), LANES)
    step = rate_ref[2:3, cols]
    low = low_half((8, LANES))

    def coefs(d):
        a = speed_ref[d, v]
        return rows8((a * (END / 6.0)) * step), rows8((0.5 * END) * jnp.abs(a) * step)

    bg, bd = coefs(0)
    for h in range(2):
        for f, i, sign in ((0, 0, bg), (1, 3, -bg)):
            rows = pl.ds(base + 32 * h + i, 8, stride=4)
            outer = outside_ref[f, pl.ds(face + 8 * h, 8), cols]
            state_ref[g, rows, :] += edge(tile_ref[g, rows, :], outer, sign, bd)
    tiles = [tile_ref[g, pl.ds(base + 8 * t, 8), :] for t in range(8)]
    total = [state_ref[g, pl.ds(base + 8 * t, 8), :] for t in range(8)]
    bg, bd = coefs(2)
    for h in range(2):
        for f, k, sign in ((4, 0, bg), (5, 3, -bg)):
            outer = outside_ref[f, pl.ds(face + 8 * h, 8), cols]
            total[2 * k + h] += edge(tiles[2 * k + h], outer, sign, bd)
    bg, bd = coefs(1)
    bgs = jnp.where(low, bg, -bg)
    outer_l = [outside_ref[2, pl.ds(face + 8 * h, 8), cols] for h in range(2)]
    outer_r = [outside_ref[3, pl.ds(face + 8 * h, 8), cols] for h in range(2)]
    for k in range(4):
        ol = outer_l[k // 2]
        orr = outer_r[k // 2]
        outer = jnp.where(low, ol, turn(orr)) if k % 2 == 0 else jnp.where(low, turn(ol), orr)
        bound = edge(jnp.where(low, tiles[2 * k], tiles[2 * k + 1]), outer, bgs, bd)
        total[2 * k] += jnp.where(low, bound, 0.0)
        total[2 * k + 1] += jnp.where(low, 0.0, bound)
    for t in range(4):
        high, rest = split2(jnp.concatenate(total[2 * t : 2 * t + 2], axis=0))
        up_ref[pl.ds(pl.multiple_of(base + 16 * t, 16), 16), cols] = high
        up_ref[pl.ds(pl.multiple_of(ROWS + base + 16 * t, 16), 16), cols] = rest


def refine_tables(flag_ref, jac_ref, start_ref, aux_ref):
    flags = flag_ref[...].astype(F32)
    wide = jnp.broadcast_to(flags, (LANES, E_DEV)).astype(BF16)
    row = lax.broadcasted_iota(jnp.int32, (E_DEV, E_DEV), 0)
    col = lax.broadcasted_iota(jnp.int32, (E_DEV, E_DEV), 1)
    ahead = jnp.where(col < row, 1.0, 0.0).astype(BF16)
    within = jnp.where(col <= row, 1.0, 0.0).astype(BF16)
    dims = (((1,), (1,)), ((), ()))
    place = lax.broadcasted_iota(jnp.int32, (E_DEV, LANES), 0).astype(F32)
    start_ref[0] = place + 7.0 * lax.dot_general(ahead, wide, dims, preferred_element_type=F32)
    start_ref[1] = (
        place + 1.0 + 7.0 * lax.dot_general(within, wide, dims, preferred_element_type=F32)
    )
    count = lax.dot_general(wide[0:16], ahead, dims, preferred_element_type=F32)[0:1]
    at = lax.broadcasted_iota(jnp.int32, (1, E_DEV), 1).astype(F32) + 7.0 * count
    at_high = jnp.floor(at * (1.0 / 16.0))
    jac = jac_ref[...]
    j0, rest = split2(jac)
    rest = jac - j0.astype(F32)
    j1 = rest.astype(BF16)
    j2 = (rest - j1.astype(F32)).astype(BF16)
    zero = jnp.zeros((10, E_DEV), F32)
    aux_ref[...] = jnp.concatenate(
        [
            at_high, at - 16.0 * at_high, flags, j0.astype(F32), j1.astype(F32), j2.astype(F32),
            zero,
        ],
        axis=0,
    ).astype(BF16)


def column_tables(tile, first, start_ref, aux_ref, coef_ref, hot_ref):
    place = lax.broadcasted_iota(jnp.int32, (1, LANES), 1).astype(F32) + first
    inside = (place >= start_ref[0]) & (place < start_ref[1])
    hot = jnp.where(inside, 1.0, 0.0).astype(BF16)
    cols = pl.ds(pl.multiple_of((tile % 2) * LANES, LANES), LANES)
    hot_ref[tile // 2, :, cols] = hot
    aux = jnp.dot(aux_ref[...], hot, preferred_element_type=F32)
    child = place - (16.0 * aux[0:1] + aux[1:2])
    refined = aux[2:3] > 0.5
    z = child >= 4.0
    child = child - jnp.where(z, 4.0, 0.0)
    y = child >= 2.0
    child = child - jnp.where(y, 2.0, 0.0)
    x = child >= 1.0
    jac = (aux[3:4] + aux[4:5] + aux[5:6]) * jnp.where(refined, 2.0, 1.0)

    def table(bit):
        return [
            [
                rows8(
                    jnp.where(
                        refined,
                        jnp.where(bit, float(SIDES[1][i, m]), float(SIDES[0][i, m])),
                        1.0 if i == m else 0.0,
                    )
                )
                for m in range(4)
            ]
            for i in range(4)
        ]

    cx, cy, cz = table(x), table(y), table(z)
    low = low_half((8, LANES))
    n = 0
    for i in range(4):
        for m in range(4):
            coef_ref[tile, n] = cx[i][m]
            coef_ref[tile, 16 + n] = cz[i][m]
            n += 1
    order = [(0, 1), (1, 0), (2, 3), (3, 2)]
    for at, (first_j, last_j) in enumerate(((0, 1), (2, 3))):
        for k, (lo_m, hi_m) in enumerate(order):
            coef_ref[tile, 32 + 4 * at + k] = jnp.where(low, cy[first_j][lo_m], cy[last_j][hi_m])
    return jac


def combine4(c, u):
    return (c[0] * u[0] + c[1] * u[1]) + (c[2] * u[2] + c[3] * u[3])


def interpolate(v, tile, half, pick_ref, coef_ref, line_ref, put):
    base = 64 * v
    cols = slice(half * LANES, half * LANES + LANES)
    tiles = [
        pick_ref[base + 8 * t : base + 8 * t + 8, cols]
        + pick_ref[ROWS + base + 8 * t : ROWS + base + 8 * t + 8, cols]
        for t in range(8)
    ]
    mid = [None] * 8
    for h in range(2):
        u = [tiles[2 * k + h] for k in range(4)]
        for k in range(4):
            mid[2 * k + h] = combine4([coef_ref[tile, 16 + 4 * k + m] for m in range(4)], u)
    for k in range(4):
        a, b = mid[2 * k], mid[2 * k + 1]
        u = [a, turn(a), b, turn(b)]
        for at in range(2):
            line_ref[v, 16 * k + 8 * at : 16 * k + 8 * at + 8, :] = combine4(
                [coef_ref[tile, 32 + 4 * at + m] for m in range(4)], u
            )
    for h in range(2):
        u = [line_ref[v, pl.ds(32 * h + i, 8, stride=4), :] for i in range(4)]
        for i in range(4):
            put(base + 32 * h + i, combine4([coef_ref[tile, 4 * i + m] for m in range(4)], u))


TILES = 13
FRAME = ROWS + 8


def kernel(
    x_hbm, jac_hbm, speed_hbm, flag_hbm, send_hbm, source_hbm, modes_hbm,
    frame_ref, head_ref, info_ref,
    jac_ref, speed_ref, flag_ref, send_ref, source_ref, modes_ref,
    tile_ref, trace_ref, out_buf, ghost_ref, ghost_bf, outside_ref, rate_ref, state_ref, up_ref,
    start_ref, aux_ref, coef_ref, hot_ref, pick_a, pick_b, line_ref, far_ref,
    row_buf, col_buf, mine, group,
    small_sems, fetch_sems, send_sems, recv_sems, row_send, row_recv, col_send, col_recv,
    head_send, head_recv, tail_send, tail_recv,
):
    me = lax.axis_index("curve")
    devices = ROW_OF * COL_OF
    row_at = me % ROW_OF
    col_at = me // ROW_OF
    near = [(me + devices + o) % devices for o in (-2, -1, 1, 2)]
    row_mates = [col_at * ROW_OF + (row_at + k) % ROW_OF for k in range(1, ROW_OF)]
    barrier = pltpu.get_barrier_semaphore()
    for partner in near + row_mates:
        pl.semaphore_signal(barrier, inc=1, device_id=(partner,), device_id_type=MESH)
    for k in range(1, COL_OF):

        @pl.when(col_at >= k)
        def _(k=k):
            pl.semaphore_signal(
                barrier, inc=1, device_id=(me - k * ROW_OF,), device_id_type=MESH
            )

    fetches = fetch_state(x_hbm, tile_ref, fetch_sems)
    small = []
    for at, (src, dst) in enumerate(
        (
            (send_hbm, send_ref), (flag_hbm, flag_ref), (source_hbm, source_ref),
            (jac_hbm, jac_ref), (modes_hbm, modes_ref), (speed_hbm, speed_ref),
        )
    ):
        copy = pltpu.make_async_copy(src, dst, small_sems.at[at])
        copy.start()
        small.append(copy)

    def send(src, dst, send_sem, recv_sem, mate):
        copy = remote(src, dst, send_sem, recv_sem, mate)
        copy.start()
        return copy

    def remote(src, dst, send_sem, recv_sem, mate):
        return pltpu.make_async_remote_copy(
            src_ref=src, dst_ref=dst, send_sem=send_sem, recv_sem=recv_sem,
            device_id=(mate,), device_id_type=MESH,
        )

    for g in range(GROUPS):
        fetches[g].wait()
        build_traces(tile_ref, trace_ref, g)
    for copy in small:
        copy.wait()
    gather_sends(send_ref, trace_ref, out_buf)
    count = jnp.sum(flag_ref[...].astype(F32), axis=1, keepdims=True)
    mine[...] = jnp.broadcast_to(count, (1, LANES)).astype(jnp.int32) - 64
    pl.semaphore_wait(barrier, 4 + ROW_OF - 1 + COL_OF - 1 - col_at)
    halo = [
        send(out_buf.at[b], ghost_ref.at[3 - b], send_sems.at[b], recv_sems.at[3 - b], mate)
        for b, mate in enumerate(near)
    ]
    row_copies = [
        send(mine, row_buf.at[k], row_send.at[k], row_recv.at[k], mate)
        for k, mate in enumerate(row_mates)
    ]
    outside_near(source_ref, trace_ref, far_ref, outside_ref)
    blend_rates(tile_ref, modes_ref, jac_ref, rate_ref)

    def interior_step(n, carry):
        interior_block(n // GROUPS, n % GROUPS, tile_ref, speed_ref, rate_ref, state_ref)
        return carry

    lax.fori_loop(0, VARS * GROUPS, interior_step, 0)
    refine_tables(flag_ref, jac_ref, start_ref, aux_ref)
    total_new = 7.0 * jnp.broadcast_to(count, (1, LANES)) + float(E_DEV)

    def table_step(tile, carry):
        shift = (jnp.full((1, LANES), tile, jnp.int32) * LANES).astype(F32)
        first = shift - 2.0 * LANES + jnp.where(tile < 2, total_new, 0.0)
        jac_row = rows8(column_tables(tile, first, start_ref, aux_ref, coef_ref, hot_ref))
        frame_ref[jnp.where(tile < 2, TILES + tile, tile), ROWS:FRAME, :] = jac_row
        return carry

    lax.fori_loop(0, TILES, table_step, 0)

    for copy in row_copies:
        copy.wait()
    total = mine[...]
    behind = jnp.zeros((1, LANES), jnp.int32)
    for k in range(ROW_OF - 1):
        value = row_buf[k]
        total = total + value
        behind = behind + jnp.where(row_at >= k + 1, value, 0)
    group[...] = total
    col_copies = [
        remote(
            group, col_buf.at[k - 1], col_send.at[k - 1], col_recv.at[k - 1],
            (me + k * ROW_OF) % devices,
        )
        for k in range(1, COL_OF)
    ]
    for k in range(1, COL_OF):

        @pl.when(col_at + k < COL_OF)
        def _(k=k):
            col_copies[k - 1].start()

    for b in range(4):
        halo[b].wait_send()
        halo[3 - b].wait_recv()
    split_ghost(ghost_ref, ghost_bf)
    first, last = me == 0, me == devices - 1
    tails = [
        remote(
            frame_ref.at[TILES + h], frame_ref.at[h], tail_send.at[h], tail_recv.at[h], near[2]
        )
        for h in range(2)
    ]
    heads = [
        remote(frame_ref.at[2 + h], head_ref.at[h], head_send.at[h], head_recv.at[h], near[1])
        for h in range(2)
    ]

    def fill(dst, tile, half, pick_ref):
        for v in range(VARS):

            def put(row, value):
                frame_ref[dst, pl.ds(row, 8, stride=4), :] = value

            interpolate(v, tile, half, pick_ref, coef_ref, line_ref, put)

    for order in range(2):
        part = me % 2 if order == 0 else 1 - me % 2
        outside_far(part, far_ref, ghost_bf, outside_ref)

        def edge_step(n, carry, part=part):
            edge_block(
                n // 2, 2 * part + n % 2, tile_ref, speed_ref, rate_ref, outside_ref, state_ref,
                up_ref,
            )
            return carry

        lax.fori_loop(0, 2 * VARS, edge_step, 0)
        within = pl.ds(pl.multiple_of(2 * LANES * part, 2 * LANES), 2 * LANES)
        pick_a[...] = jnp.dot(
            up_ref[:, within], hot_ref[1 - part, within, :], preferred_element_type=F32
        )
        for half in range(2):
            fill(
                jnp.where(part == 1, TILES, 2) + half, 2 * (1 - part) + half, half, pick_a
            )
            pl.when((part == 1) & jnp.logical_not(last))(tails[half].start)
            pl.when((part == 0) & jnp.logical_not(first))(heads[half].start)

    picks = [pick_a, pick_b]
    pick_a[...] = jnp.dot(up_ref[...], hot_ref[2], preferred_element_type=F32)
    for pair in range(2, 7):
        now, later = picks[pair % 2], picks[(pair + 1) % 2]
        if pair < 5:
            later[...] = jnp.dot(up_ref[...], hot_ref[pair + 1], preferred_element_type=F32)
        if pair == 5:
            later[:, 0:LANES] = jnp.dot(
                up_ref[...], hot_ref[6, :, 0:LANES], preferred_element_type=F32
            )
        for half in range(2 if pair < 6 else 1):
            fill(2 * pair + half, 2 * pair + half, half, now)

    for k in range(1, COL_OF):

        @pl.when(col_at + k < COL_OF)
        def _(k=k):
            col_copies[k - 1].wait_send()

        @pl.when(col_at >= k)
        def _(k=k):
            col_copies[k - 1].wait_recv()

    for k in range(1, COL_OF):
        behind = behind + jnp.where(col_at >= k, col_buf[k - 1], 0)
    info_ref[0:1, :] = behind
    info_ref[1:2, :] = total_new.astype(jnp.int32)
    for half in range(2):

        @pl.when(jnp.logical_not(last))
        def _(half=half):
            tails[half].wait_send()
            heads[half].wait_recv()

        @pl.when(jnp.logical_not(first))
        def _(half=half):
            heads[half].wait_send()
            tails[half].wait_recv()


CHUNK = 64


def place_kernel(frame_ref, head_ref, info_ref, out_hbm, jac_hbm, out_ref, jac_ref, sems):
    shift = 7 * jnp.max(info_ref[0:1, :])
    size = jnp.max(info_ref[1:2, :])
    begin = 2 * LANES - shift
    tile = begin // LANES
    turn_by = begin - tile * LANES
    over = -(size + shift)
    head_tile = over // LANES
    head_turn = over - head_tile * LANES
    lane = lax.broadcasted_iota(jnp.int32, (8, LANES), 1)
    kept = lane < LANES - turn_by
    head_kept = lane < LANES - head_turn
    back = (LANES - turn_by) % LANES
    head_back = (LANES - head_turn) % LANES

    def row_tile(rows):
        parts = [pltpu.roll(frame_ref[tile + c, rows, :], back, 1) for c in range(9)]
        out = [jnp.where(kept, parts[c], parts[c + 1]) for c in range(8)]
        ends = []
        for c in range(4):
            at = head_tile + 5 + c
            part = pltpu.roll(head_ref[jnp.clip(at, 0, 1), rows, :], head_back, 1)
            ends.append(jnp.where((at >= 0) & (at < 2), part, 0.0))
        for c in range(3):
            out[5 + c] = out[5 + c] + jnp.where(head_kept, ends[c], ends[c + 1])
        return out

    out = row_tile(pl.ds(ROWS, 8))
    for c in range(8):
        width = min(LANES, E_NEW - c * LANES)
        jac_ref[0:1, c * LANES : c * LANES + width] = out[c][0:1, :width]
    copies = [pltpu.make_async_copy(jac_ref, jac_hbm, sems.at[ROWS // CHUNK])]
    copies[0].start()
    for chunk in range(ROWS // CHUNK):
        for n in range(CHUNK // 8):
            row = chunk * CHUNK + 8 * n
            out = row_tile(pl.ds(row, 8))
            for c in range(7):
                out_ref[row : row + 8, c * LANES : (c + 1) * LANES] = out[c]
            out_ref[row : row + 8, 7 * LANES : E_NEW] = out[7][:, : E_NEW - 7 * LANES]
        rows = pl.ds(chunk * CHUNK, CHUNK)
        copy = pltpu.make_async_copy(out_ref.at[rows], out_hbm.at[rows], sems.at[chunk])
        copy.start()
        copies.append(copy)
    for copy in copies:
        copy.wait()


def vmem(count):
    return [pl.BlockSpec(memory_space=pltpu.VMEM)] * count


def shards(nodal_state, inverse_jacobian, speeds, refine_flags, send_index, face_source):
    x = nodal_state.reshape(ROWS, E_DEV)
    jac = inverse_jacobian.reshape(1, E_DEV)
    flags = refine_flags.reshape(1, E_DEV)
    dma = pltpu.SemaphoreType.DMA
    frame, head, info = pl.pallas_call(
        kernel,
        out_shape=(
            jax.ShapeDtypeStruct((TILES + 2, FRAME, LANES), F32),
            jax.ShapeDtypeStruct((2, FRAME, LANES), F32),
            jax.ShapeDtypeStruct((2, LANES), jnp.int32),
        ),
        in_specs=[pl.BlockSpec(memory_space=pltpu.HBM)] * 7,
        out_specs=tuple(vmem(3)),
        scratch_shapes=[
            pltpu.VMEM((1, E_DEV), F32),
            pltpu.SMEM((3, VARS), F32),
            pltpu.VMEM((1, E_DEV), jnp.int32),
            pltpu.VMEM((4 * SLOTS,), jnp.int32),
            pltpu.VMEM((6, E_DEV), jnp.int32),
            pltpu.VMEM((64, 64), F32),
            pltpu.VMEM((GROUPS, ROWS, LANES), F32),
            pltpu.VMEM((6, 160, E_DEV), BF16),
            pltpu.VMEM((4, 80, LANES), F32),
            pltpu.VMEM((4, 80, LANES), F32),
            pltpu.VMEM((160, E_DEV), BF16),
            pltpu.VMEM((6, 80, E_DEV), F32),
            pltpu.VMEM((8, E_DEV), F32),
            pltpu.VMEM((GROUPS, ROWS, LANES), F32),
            pltpu.VMEM((2 * ROWS, E_DEV), BF16),
            pltpu.VMEM((2, E_DEV, LANES), F32),
            pltpu.VMEM((16, E_DEV), BF16),
            pltpu.VMEM((TILES, 40, 8, LANES), F32),
            pltpu.VMEM((7, E_DEV, 2 * LANES), BF16),
            pltpu.VMEM((2 * ROWS, 2 * LANES), F32),
            pltpu.VMEM((2 * ROWS, 2 * LANES), F32),
            pltpu.VMEM((VARS, 64, LANES), F32),
            pltpu.VMEM((6, E_DEV, E_DEV), BF16),
            pltpu.VMEM((ROW_OF - 1, 1, LANES), jnp.int32),
            pltpu.VMEM((COL_OF - 1, 1, LANES), jnp.int32),
            pltpu.VMEM((1, LANES), jnp.int32),
            pltpu.VMEM((1, LANES), jnp.int32),
            dma((6,)), dma((GROUPS,)), dma((4,)), dma((4,)), dma((ROW_OF - 1,)),
            dma((ROW_OF - 1,)), dma((COL_OF - 1,)), dma((COL_OF - 1,)),
            dma((2,)), dma((2,)), dma((2,)), dma((2,)),
        ],
        compiler_params=pltpu.CompilerParams(
            collective_id=0, has_side_effects=True, vmem_limit_bytes=28 << 20
        ),
        name="step",
    )(*[
        pltpu.with_memory_space_constraint(a, pltpu.HBM)
        for a in (x, jac, speeds, flags, send_index, face_source, jnp.asarray(MODES, F32))
    ])
    out, out_jac = pl.pallas_call(
        place_kernel,
        out_shape=(
            jax.ShapeDtypeStruct((ROWS, E_NEW), F32),
            jax.ShapeDtypeStruct((1, E_NEW), F32),
        ),
        in_specs=vmem(3),
        out_specs=(
            pl.BlockSpec(memory_space=pltpu.HBM), pl.BlockSpec(memory_space=pltpu.HBM)
        ),
        scratch_shapes=[
            pltpu.VMEM((ROWS, E_NEW), F32), pltpu.VMEM((1, E_NEW), F32), dma((ROWS // CHUNK + 1,))
        ],
        compiler_params=pltpu.CompilerParams(vmem_limit_bytes=16 << 20),
        name="place",
    )(frame, head, info)
    return out.reshape(VARS, 64, E_NEW), out_jac.reshape(E_NEW)


def solution(mesh):
    axis = P("curve")
    wide = P(None, None, "curve")
    return jax.shard_map(
        shards,
        mesh=mesh,
        in_specs=(wide, axis, P(), axis, axis, P(None, "curve")),
        out_specs=(wide, axis),
        check_vma=False,
    )
```

```python
import functools
import math

import jax
import jax.numpy as jnp
import numpy as np
from jax import lax
from jax.experimental import pallas as pl
from jax.experimental.pallas import tpu as pltpu
from jax.sharding import PartitionSpec as P

TIME_STEP = 0.02
VARS = 5
E_DEV = 512
E_NEW = 960
SLOTS = 96
ROWS = 64 * VARS
LANES = 128
GROUPS = E_DEV // LANES
ROW_OF = 8
SIDE = 4
F32 = jnp.float32
BF16 = jnp.bfloat16
MESH = pl.DeviceIdType.MESH


def lagrange_at(points, targets):
    values_at = np.ones((len(targets), 4))
    for basis_id in range(4):
        for partner in range(4):
            if partner != basis_id:
                values_at[:, basis_id] *= (targets - points[partner]) / (
                    points[basis_id] - points[partner]
                )
    return values_at


def tables():
    root = 1.0 / math.sqrt(5.0)
    points = np.array([-1.0, -root, root, 1.0])
    weights = np.array([1.0, 5.0, 5.0, 1.0]) / 6.0
    bary = np.ones(4)
    for a in range(4):
        for b in range(4):
            if a != b:
                bary[a] /= points[a] - points[b]
    deriv = np.zeros((4, 4))
    for a in range(4):
        for b in range(4):
            if a != b:
                deriv[a, b] = bary[b] / bary[a] / (points[a] - points[b])
        deriv[a, a] = -np.sum(deriv[a])
    skew = weights[:, None] * deriv
    legendre = np.stack(
        [points**0, points, 0.5 * (3 * points**2 - 1), 0.5 * (5 * points**3 - 3 * points)], axis=1
    )
    to_modes = np.linalg.inv(legendre)
    sides = [lagrange_at(points, (points - 1.0) / 2.0), lagrange_at(points, (points + 1.0) / 2.0)]
    return skew, np.kron(to_modes, np.kron(to_modes, to_modes)), sides


SKEW, MODES, SIDES = tables()
Q01, Q02, Q03, Q12 = (float(SKEW[0, 1]), float(SKEW[0, 2]), float(SKEW[0, 3]), float(SKEW[1, 2]))
END, MID = 6.0, 1.2


def split2(x):
    high = x.astype(BF16)
    return high, (x - high.astype(F32)).astype(BF16)


def low_half(shape):
    return (lax.broadcasted_iota(jnp.int32, shape, 0) & 7) < 4


def turn(x):
    return pltpu.roll(x, 4, 0)


def fetch_state(x_ref, tile_ref, sems):
    copies = []
    for g in range(GROUPS):
        copy = pltpu.make_async_copy(
            x_ref.at[:, g * LANES : (g + 1) * LANES], tile_ref.at[g], sems.at[g]
        )
        copy.start()
        copies.append(copy)
    return copies


def build_traces(tile_ref, trace_ref, g):
    low = low_half((8, LANES))
    cols = slice(g * LANES, (g + 1) * LANES)
    for v in range(VARS):
        base = 64 * v
        tiles = [tile_ref[g, base + 8 * t : base + 8 * t + 8, :] for t in range(8)]
        first, last = tiles[0::2], tiles[1::2]
        sets = {
            0: [tile_ref[g, pl.ds(base + 32 * h, 8, stride=4), :] for h in range(2)],
            1: [tile_ref[g, pl.ds(base + 32 * h + 3, 8, stride=4), :] for h in range(2)],
            2: [jnp.where(low, first[k], turn(first[k + 1])) for k in (0, 2)],
            3: [jnp.where(low, turn(last[k]), last[k + 1]) for k in (0, 2)],
            4: tiles[0:2],
            5: tiles[6:8],
        }
        for f, rows in sets.items():
            high, rest = split2(jnp.concatenate(rows, axis=0))
            trace_ref[f, 16 * v : 16 * v + 16, cols] = high
            trace_ref[f, 80 + 16 * v : 96 + 16 * v, cols] = rest


def one_hot(index, size, width):
    rows = lax.broadcasted_iota(jnp.int32, (size, width), 0).astype(jnp.int16)
    index = jnp.broadcast_to(index, (16, width)).astype(jnp.int16)
    index = jnp.concatenate([index] * (size // 16), axis=0)
    return jnp.where(
        rows == index, jnp.ones((size, width), BF16), jnp.zeros((size, width), BF16)
    )


def gather_sends(send_ref, trace_ref, out_ref):
    packed = jnp.broadcast_to(send_ref[...].reshape(1, 4 * SLOTS), (8, 4 * SLOTS))
    for pair in range(2):
        moved = [
            packed if block == 0 else pltpu.roll(packed, 4 * SLOTS - SLOTS * block, 1)
            for block in (2 * pair, 2 * pair + 1)
        ]
        index = jnp.concatenate([m[0:1, 0:LANES] for m in moved], axis=1)
        total = jnp.zeros((160, 2 * LANES), F32)
        for f in range(6):
            total = total + jnp.dot(
                trace_ref[f],
                one_hot(index - f * E_DEV, E_DEV, 2 * LANES),
                preferred_element_type=F32,
            )
        total = total[0:80] + total[80:160]
        for half in range(2):
            out_ref[2 * pair + half] = total[:, half * LANES : (half + 1) * LANES]


def pair_sum(ui, um, si, sm):
    return (si + sm) + ui * um


def line_update(u, coef):
    ca, cb, c02, c03, cd = coef
    s = [x * x for x in u]
    m = [jnp.abs(x) for x in u]
    e = []
    for n, c in ((0, ca), (1, cb), (2, ca)):
        g = pair_sum(u[n], u[n + 1], s[n], s[n + 1])
        e.append(c * g - cd * (jnp.maximum(m[n], m[n + 1]) * (u[n + 1] - u[n])))
    r02 = c02 * pair_sum(u[0], u[2], s[0], s[2])
    r13 = c02 * pair_sum(u[1], u[3], s[1], s[3])
    r03 = c03 * pair_sum(u[0], u[3], s[0], s[3])
    t0 = -(e[0] + r02 + r03)
    t1 = e[0] - e[1] - r13
    t2 = e[1] - e[2] + r02
    t3 = e[2] + r13 + r03
    return t0, t1, t2, t3


def edge(u, o, cg, cd):
    g = pair_sum(u, o, u * u, o * o)
    return cg * g - cd * (jnp.maximum(jnp.abs(u), jnp.abs(o)) * (u - o))


def rows8(x):
    return jnp.broadcast_to(x, (8, LANES))


def blend_rates(tile_ref, modes_ref, jac_ref, rate_ref):
    n = lax.broadcasted_iota(jnp.int32, (64, LANES), 0)
    top = ((n & 3) == 3) | ((n & 12) == 12) | (n >= 48)
    for g in range(GROUPS):
        cols = slice(g * LANES, (g + 1) * LANES)
        modal = jnp.dot(
            modes_ref[...], tile_ref[g, 0:64, :], precision=lax.Precision.HIGHEST,
            preferred_element_type=F32,
        )
        energy = modal * modal
        high = jnp.sum(jnp.where(top, energy, 0.0), axis=0, keepdims=True)
        full = jnp.sum(energy, axis=0, keepdims=True)
        ratio = high / (full + 1e-06)
        blend = 0.5 * ratio / (ratio + 0.1)
        step = TIME_STEP * jac_ref[0:1, cols]
        rate_ref[0:1, cols] = step * (1.0 - blend)
        rate_ref[1:2, cols] = step * blend
        rate_ref[2:3, cols] = step


def outside_near(source_ref, trace_ref, far_ref, outside_ref):
    for f in range(6):
        index = source_ref[f : f + 1, :]
        total = jnp.dot(
            trace_ref[f ^ 1],
            one_hot(index - (f ^ 1) * E_DEV, E_DEV, E_DEV),
            preferred_element_type=F32,
        )
        outside_ref[f] = total[0:80] + total[80:160]
        far = index - 6 * E_DEV
        slot = (
            (far >= SLOTS).astype(jnp.int32)
            + (far >= 2 * SLOTS).astype(jnp.int32)
            + (far >= 3 * SLOTS).astype(jnp.int32)
        )
        far_ref[f] = one_hot(
            jnp.where(far >= 0, far + (LANES - SLOTS) * slot, -1), E_DEV, E_DEV
        )


def split_ghost(ghost_ref, ghost_bf):
    for slot in range(4):
        high, rest = split2(ghost_ref[slot])
        ghost_bf[0:80, slot * LANES : (slot + 1) * LANES] = high
        ghost_bf[80:160, slot * LANES : (slot + 1) * LANES] = rest


def outside_far(half, far_ref, ghost_bf, outside_ref):
    cols = pl.ds(pl.multiple_of(2 * LANES * half, 2 * LANES), 2 * LANES)
    for f in range(6):
        total = jnp.dot(ghost_bf[...], far_ref[f, :, cols], preferred_element_type=F32)
        outside_ref[f, :, cols] += total[0:80] + total[80:160]


def coefs_of(d, v, speed_ref, hi, lo):
    a = speed_ref[d, v]
    third = (a / 3.0) * hi
    sixth = (a / 6.0) * lo
    return [
        rows8(c)
        for c in (
            Q01 * third + sixth, Q12 * third + sixth, Q02 * third, Q03 * third,
            (0.5 * jnp.abs(a)) * lo,
        )
    ]


def interior_block(v, g, tile_ref, speed_ref, rate_ref, state_ref):
    base = pl.multiple_of(64 * v, 64)
    cols = pl.ds(pl.multiple_of(g * LANES, LANES), LANES)
    hi = rate_ref[0:1, cols]
    lo = rate_ref[1:2, cols]
    low = low_half((8, LANES))
    coef = coefs_of(0, v, speed_ref, hi, lo)
    for h in range(2):
        u = [tile_ref[g, pl.ds(base + 32 * h + i, 8, stride=4), :] for i in range(4)]
        t = line_update(u, coef)
        for i, w in enumerate((END, MID, MID, END)):
            state_ref[g, pl.ds(base + 32 * h + i, 8, stride=4), :] = u[i] + w * t[i]
    tiles = [tile_ref[g, pl.ds(base + 8 * t, 8), :] for t in range(8)]
    coef = coefs_of(2, v, speed_ref, hi, lo)
    total = [None] * 8
    for h in range(2):
        t = line_update([tiles[2 * k + h] for k in range(4)], coef)
        for k, w in enumerate((END, MID, MID, END)):
            total[2 * k + h] = w * t[k]
    ca, cb, c02, c03, cd = coefs_of(1, v, speed_ref, hi, lo)
    signed = jnp.where(low, -ca, ca)
    cross = jnp.where(low, -c03, -cb)
    cross_d = jnp.where(low, 0.0, cd)
    wa = jnp.where(low, END, MID)
    wb = jnp.where(low, MID, END)
    for k in range(4):
        a, b = tiles[2 * k], tiles[2 * k + 1]
        at, bt = turn(a), turn(b)
        sa, sb, sat, sbt = a * a, b * b, at * at, bt * bt
        ma, mb, mat, mbt = jnp.abs(a), jnp.abs(b), jnp.abs(at), jnp.abs(bt)
        x1 = signed * pair_sum(a, at, sa, sat) + cd * (jnp.maximum(ma, mat) * (at - a))
        x2 = signed * pair_sum(b, bt, sb, sbt) + cd * (jnp.maximum(mb, mbt) * (bt - b))
        x3 = c02 * pair_sum(a, b, sa, sb)
        x4 = cross * pair_sum(a, bt, sa, sbt) + cross_d * (jnp.maximum(ma, mbt) * (bt - a))
        total[2 * k] += wa * (x1 - x3 + x4)
        total[2 * k + 1] += wb * (x2 + x3 - turn(x4))
    for t in range(8):
        state_ref[g, pl.ds(base + 8 * t, 8), :] += total[t]


def edge_block(v, g, tile_ref, speed_ref, rate_ref, outside_ref, state_ref, up_ref):
    base = pl.multiple_of(64 * v, 64)
    face = pl.multiple_of(16 * v, 16)
    cols = pl.ds(pl.multiple_of(g * LANES, LANES), LANES)
    step = rate_ref[2:3, cols]
    low = low_half((8, LANES))

    def coefs(d):
        a = speed_ref[d, v]
        return rows8((a * (END / 6.0)) * step), rows8((0.5 * END) * jnp.abs(a) * step)

    bg, bd = coefs(0)
    for h in range(2):
        for f, i, sign in ((0, 0, bg), (1, 3, -bg)):
            rows = pl.ds(base + 32 * h + i, 8, stride=4)
            outer = outside_ref[f, pl.ds(face + 8 * h, 8), cols]
            state_ref[g, rows, :] += edge(tile_ref[g, rows, :], outer, sign, bd)
    tiles = [tile_ref[g, pl.ds(base + 8 * t, 8), :] for t in range(8)]
    total = [state_ref[g, pl.ds(base + 8 * t, 8), :] for t in range(8)]
    bg, bd = coefs(2)
    for h in range(2):
        for f, k, sign in ((4, 0, bg), (5, 3, -bg)):
            outer = outside_ref[f, pl.ds(face + 8 * h, 8), cols]
            total[2 * k + h] += edge(tiles[2 * k + h], outer, sign, bd)
    bg, bd = coefs(1)
    bgs = jnp.where(low, bg, -bg)
    outer_l = [outside_ref[2, pl.ds(face + 8 * h, 8), cols] for h in range(2)]
    outer_r = [outside_ref[3, pl.ds(face + 8 * h, 8), cols] for h in range(2)]
    for k in range(4):
        ol = outer_l[k // 2]
        orr = outer_r[k // 2]
        outer = jnp.where(low, ol, turn(orr)) if k % 2 == 0 else jnp.where(low, turn(ol), orr)
        bound = edge(jnp.where(low, tiles[2 * k], tiles[2 * k + 1]), outer, bgs, bd)
        total[2 * k] += jnp.where(low, bound, 0.0)
        total[2 * k + 1] += jnp.where(low, 0.0, bound)
    for t in range(4):
        high, rest = split2(jnp.concatenate(total[2 * t : 2 * t + 2], axis=0))
        up_ref[pl.ds(pl.multiple_of(base + 16 * t, 16), 16), cols] = high
        up_ref[pl.ds(pl.multiple_of(ROWS + base + 16 * t, 16), 16), cols] = rest


def refine_tables(flag_ref, jac_ref, start_ref, aux_ref):
    flags = flag_ref[...].astype(F32)
    wide = jnp.broadcast_to(flags, (LANES, E_DEV)).astype(BF16)
    row = lax.broadcasted_iota(jnp.int32, (E_DEV, E_DEV), 0)
    col = lax.broadcasted_iota(jnp.int32, (E_DEV, E_DEV), 1)
    ahead = jnp.where(col < row, 1.0, 0.0).astype(BF16)
    within = jnp.where(col <= row, 1.0, 0.0).astype(BF16)
    dims = (((1,), (1,)), ((), ()))
    place = lax.broadcasted_iota(jnp.int32, (E_DEV, LANES), 0).astype(F32)
    start_ref[0] = place + 7.0 * lax.dot_general(ahead, wide, dims, preferred_element_type=F32)
    start_ref[1] = (
        place + 1.0 + 7.0 * lax.dot_general(within, wide, dims, preferred_element_type=F32)
    )
    count = lax.dot_general(wide[0:16], ahead, dims, preferred_element_type=F32)[0:1]
    at = lax.broadcasted_iota(jnp.int32, (1, E_DEV), 1).astype(F32) + 7.0 * count
    at_high = jnp.floor(at * (1.0 / 16.0))
    jac = jac_ref[...]
    j0, rest = split2(jac)
    rest = jac - j0.astype(F32)
    j1 = rest.astype(BF16)
    j2 = (rest - j1.astype(F32)).astype(BF16)
    zero = jnp.zeros((10, E_DEV), F32)
    aux_ref[...] = jnp.concatenate(
        [
            at_high, at - 16.0 * at_high, flags, j0.astype(F32), j1.astype(F32), j2.astype(F32),
            zero,
        ],
        axis=0,
    ).astype(BF16)


def column_tables(tile, first, start_ref, aux_ref, coef_ref, hot_ref):
    place = lax.broadcasted_iota(jnp.int32, (1, LANES), 1).astype(F32) + first
    inside = (place >= start_ref[0]) & (place < start_ref[1])
    hot = jnp.where(inside, 1.0, 0.0).astype(BF16)
    cols = pl.ds(pl.multiple_of((tile % 2) * LANES, LANES), LANES)
    hot_ref[tile // 2, :, cols] = hot
    aux = jnp.dot(aux_ref[...], hot, preferred_element_type=F32)
    child = place - (16.0 * aux[0:1] + aux[1:2])
    refined = aux[2:3] > 0.5
    z = child >= 4.0
    child = child - jnp.where(z, 4.0, 0.0)
    y = child >= 2.0
    child = child - jnp.where(y, 2.0, 0.0)
    x = child >= 1.0
    jac = (aux[3:4] + aux[4:5] + aux[5:6]) * jnp.where(refined, 2.0, 1.0)

    def table(bit):
        return [
            [
                rows8(
                    jnp.where(
                        refined,
                        jnp.where(bit, float(SIDES[1][i, m]), float(SIDES[0][i, m])),
                        1.0 if i == m else 0.0,
                    )
                )
                for m in range(4)
            ]
            for i in range(4)
        ]

    cx, cy, cz = table(x), table(y), table(z)
    low = low_half((8, LANES))
    n = 0
    for i in range(4):
        for m in range(4):
            coef_ref[tile, n] = cx[i][m]
            coef_ref[tile, 16 + n] = cz[i][m]
            n += 1
    order = [(0, 1), (1, 0), (2, 3), (3, 2)]
    for at, (first_j, last_j) in enumerate(((0, 1), (2, 3))):
        for k, (lo_m, hi_m) in enumerate(order):
            coef_ref[tile, 32 + 4 * at + k] = jnp.where(low, cy[first_j][lo_m], cy[last_j][hi_m])
    return jac


def combine4(c, u):
    return (c[0] * u[0] + c[1] * u[1]) + (c[2] * u[2] + c[3] * u[3])


def interpolate(v, tile, half, pick_ref, coef_ref, line_ref, put):
    base = 64 * v
    cols = slice(half * LANES, half * LANES + LANES)
    tiles = [
        pick_ref[base + 8 * t : base + 8 * t + 8, cols]
        + pick_ref[ROWS + base + 8 * t : ROWS + base + 8 * t + 8, cols]
        for t in range(8)
    ]
    mid = [None] * 8
    for h in range(2):
        u = [tiles[2 * k + h] for k in range(4)]
        for k in range(4):
            mid[2 * k + h] = combine4([coef_ref[tile, 16 + 4 * k + m] for m in range(4)], u)
    for k in range(4):
        a, b = mid[2 * k], mid[2 * k + 1]
        u = [a, turn(a), b, turn(b)]
        for at in range(2):
            line_ref[v, 16 * k + 8 * at : 16 * k + 8 * at + 8, :] = combine4(
                [coef_ref[tile, 32 + 4 * at + m] for m in range(4)], u
            )
    for h in range(2):
        u = [line_ref[v, pl.ds(32 * h + i, 8, stride=4), :] for i in range(4)]
        for i in range(4):
            put(base + 32 * h + i, combine4([coef_ref[tile, 4 * i + m] for m in range(4)], u))


TILES = 13
FRAME = ROWS + 8


def kernel(
    x_hbm, jac_hbm, speed_hbm, flag_hbm, send_hbm, source_hbm, modes_hbm,
    frame_ref, head_ref, info_ref,
    jac_ref, speed_ref, flag_ref, send_ref, source_ref, modes_ref,
    tile_ref, trace_ref, out_buf, ghost_ref, ghost_bf, outside_ref, rate_ref, state_ref, up_ref,
    start_ref, aux_ref, coef_ref, hot_ref, pick_a, pick_b, line_ref, far_ref,
    row_buf, z_buf, y_buf, mine, row_sum, plane_sum,
    small_sems, fetch_sems, send_sems, recv_sems, row_send, row_recv, z_send, z_recv,
    y_send, y_recv,
    head_send, head_recv, tail_send, tail_recv,
):
    me = lax.axis_index("curve")
    devices = ROW_OF * SIDE * SIDE
    row_at = me % ROW_OF
    z_at = me // ROW_OF % SIDE
    y_at = me // (ROW_OF * SIDE)
    near = [(me + devices + o) % devices for o in (-2, -1, 1, 2)]
    row_mates = [me - row_at + (row_at + k) % ROW_OF for k in range(1, ROW_OF)]
    z_mates = [me + ROW_OF * ((z_at + k) % SIDE - z_at) for k in range(1, SIDE)]
    early = me < 2
    barrier = pltpu.get_barrier_semaphore()
    for partner in near:
        pl.semaphore_signal(barrier, inc=1, device_id=(partner,), device_id_type=MESH)
    fetches = fetch_state(x_hbm, tile_ref, fetch_sems)
    for partner in row_mates + z_mates:
        pl.semaphore_signal(barrier, inc=1, device_id=(partner,), device_id_type=MESH)
    for k in range(1, SIDE):

        @pl.when(y_at >= k)
        def _(k=k):
            pl.semaphore_signal(
                barrier, inc=1, device_id=(me - k * ROW_OF * SIDE,), device_id_type=MESH
            )

    small = []
    for at, (src, dst) in enumerate(
        (
            (send_hbm, send_ref), (flag_hbm, flag_ref), (source_hbm, source_ref),
            (jac_hbm, jac_ref), (modes_hbm, modes_ref), (speed_hbm, speed_ref),
        )
    ):
        copy = pltpu.make_async_copy(src, dst, small_sems.at[at])
        copy.start()
        small.append(copy)

    def send(src, dst, send_sem, recv_sem, mate):
        copy = remote(src, dst, send_sem, recv_sem, mate)
        copy.start()
        return copy

    def remote(src, dst, send_sem, recv_sem, mate):
        return pltpu.make_async_remote_copy(
            src_ref=src, dst_ref=dst, send_sem=send_sem, recv_sem=recv_sem,
            device_id=(mate,), device_id_type=MESH,
        )

    for g in range(GROUPS):
        fetches[g].wait()
        build_traces(tile_ref, trace_ref, g)
    for copy in small:
        copy.wait()
    gather_sends(send_ref, trace_ref, out_buf)
    count = jnp.sum(flag_ref[...].astype(F32), axis=1, keepdims=True)
    mine[...] = jnp.broadcast_to(count, (1, LANES)).astype(jnp.int32) - 64
    total_new = 7.0 * jnp.broadcast_to(count, (1, LANES)) + float(E_DEV)

    def local_work():
        outside_near(source_ref, trace_ref, far_ref, outside_ref)
        blend_rates(tile_ref, modes_ref, jac_ref, rate_ref)

        def interior_step(n, carry):
            interior_block(n // GROUPS, n % GROUPS, tile_ref, speed_ref, rate_ref, state_ref)
            return carry

        lax.fori_loop(0, VARS * GROUPS, interior_step, 0)
        refine_tables(flag_ref, jac_ref, start_ref, aux_ref)

        def table_step(tile, carry):
            shift = (jnp.full((1, LANES), tile, jnp.int32) * LANES).astype(F32)
            first = shift - 2.0 * LANES + jnp.where(tile < 2, total_new, 0.0)
            jac_row = rows8(column_tables(tile, first, start_ref, aux_ref, coef_ref, hot_ref))
            frame_ref[jnp.where(tile < 2, TILES + tile, tile), ROWS:FRAME, :] = jac_row
            return carry

        lax.fori_loop(0, TILES, table_step, 0)

    pl.when(early)(local_work)
    pl.semaphore_wait(barrier, 4 + ROW_OF - 1 + SIDE - 1 + SIDE - 1 - y_at)
    halo = [
        send(out_buf.at[b], ghost_ref.at[3 - b], send_sems.at[b], recv_sems.at[3 - b], mate)
        for b, mate in enumerate(near)
    ]
    row_copies = [
        send(mine, row_buf.at[k], row_send.at[k], row_recv.at[k], mate)
        for k, mate in enumerate(row_mates)
    ]
    pl.when(jnp.logical_not(early))(local_work)

    def gathered(copies, own_ref, buf_ref, at, behind):
        for copy in copies:
            copy.wait()
        total = own_ref[...]
        for k in range(len(copies)):
            value = buf_ref[k]
            total = total + value
            behind = behind + jnp.where(at >= k + 1, value, 0)
        return total, behind

    total, behind = gathered(
        row_copies, mine, row_buf, row_at, jnp.zeros((1, LANES), jnp.int32)
    )
    row_sum[...] = total
    z_copies = [
        send(row_sum, z_buf.at[k], z_send.at[k], z_recv.at[k], mate)
        for k, mate in enumerate(z_mates)
    ]
    for b in range(4):
        halo[b].wait_send()
        halo[3 - b].wait_recv()
    split_ghost(ghost_ref, ghost_bf)
    first, last = me == 0, me == devices - 1
    tails = [
        remote(
            frame_ref.at[TILES + h], frame_ref.at[h], tail_send.at[h], tail_recv.at[h], near[2]
        )
        for h in range(2)
    ]
    heads = [
        remote(frame_ref.at[2 + h], head_ref.at[h], head_send.at[h], head_recv.at[h], near[1])
        for h in range(2)
    ]

    def fill(dst, tile, half, pick_ref):
        for v in range(VARS):

            def put(row, value):
                frame_ref[dst, pl.ds(row, 8, stride=4), :] = value

            interpolate(v, tile, half, pick_ref, coef_ref, line_ref, put)

    for order in range(2):
        part = me % 2 if order == 0 else 1 - me % 2
        outside_far(part, far_ref, ghost_bf, outside_ref)

        def edge_step(n, carry, part=part):
            edge_block(
                n // 2, 2 * part + n % 2, tile_ref, speed_ref, rate_ref, outside_ref, state_ref,
                up_ref,
            )
            return carry

        lax.fori_loop(0, 2 * VARS, edge_step, 0)
        within = pl.ds(pl.multiple_of(2 * LANES * part, 2 * LANES), 2 * LANES)
        pick_a[...] = jnp.dot(
            up_ref[:, within], hot_ref[1 - part, within, :], preferred_element_type=F32
        )
        for half in range(2):
            fill(
                jnp.where(part == 1, TILES, 2) + half, 2 * (1 - part) + half, half, pick_a
            )
            pl.when((part == 1) & jnp.logical_not(last))(tails[half].start)
            pl.when((part == 0) & jnp.logical_not(first))(heads[half].start)

    total, behind = gathered(z_copies, row_sum, z_buf, z_at, behind)
    plane_sum[...] = total
    y_copies = [
        remote(
            plane_sum, y_buf.at[k - 1], y_send.at[k - 1], y_recv.at[k - 1],
            (me + k * ROW_OF * SIDE) % devices,
        )
        for k in range(1, SIDE)
    ]
    for k in range(1, SIDE):
        pl.when(y_at + k < SIDE)(y_copies[k - 1].start)

    picks = [pick_a, pick_b]
    pick_a[...] = jnp.dot(up_ref[...], hot_ref[2], preferred_element_type=F32)
    for pair in range(2, 7):
        now, later = picks[pair % 2], picks[(pair + 1) % 2]
        if pair < 5:
            later[...] = jnp.dot(up_ref[...], hot_ref[pair + 1], preferred_element_type=F32)
        if pair == 5:
            later[:, 0:LANES] = jnp.dot(
                up_ref[...], hot_ref[6, :, 0:LANES], preferred_element_type=F32
            )
        for half in range(2 if pair < 6 else 1):
            fill(2 * pair + half, 2 * pair + half, half, now)

    for k in range(1, SIDE):
        pl.when(y_at + k < SIDE)(y_copies[k - 1].wait_send)
        pl.when(y_at >= k)(y_copies[k - 1].wait_recv)
        behind = behind + jnp.where(y_at >= k, y_buf[k - 1], 0)
    info_ref[0:1, :] = behind
    info_ref[1:2, :] = total_new.astype(jnp.int32)
    for half in range(2):

        @pl.when(jnp.logical_not(last))
        def _(half=half):
            tails[half].wait_send()
            heads[half].wait_recv()

        @pl.when(jnp.logical_not(first))
        def _(half=half):
            heads[half].wait_send()
            tails[half].wait_recv()


CHUNK = 64


def place_kernel(frame_ref, head_ref, info_ref, out_hbm, jac_hbm, out_ref, jac_ref, sems):
    shift = 7 * jnp.max(info_ref[0:1, :])
    size = jnp.max(info_ref[1:2, :])
    begin = 2 * LANES - shift
    tile = begin // LANES
    turn_by = begin - tile * LANES
    over = -(size + shift)
    head_tile = over // LANES
    head_turn = over - head_tile * LANES
    lane = lax.broadcasted_iota(jnp.int32, (8, LANES), 1)
    kept = lane < LANES - turn_by
    head_kept = lane < LANES - head_turn
    back = (LANES - turn_by) % LANES
    head_back = (LANES - head_turn) % LANES

    def row_tile(rows):
        parts = [pltpu.roll(frame_ref[tile + c, rows, :], back, 1) for c in range(9)]
        out = [jnp.where(kept, parts[c], parts[c + 1]) for c in range(8)]
        ends = []
        for c in range(4):
            at = head_tile + 5 + c
            part = pltpu.roll(head_ref[jnp.clip(at, 0, 1), rows, :], head_back, 1)
            ends.append(jnp.where((at >= 0) & (at < 2), part, 0.0))
        for c in range(3):
            out[5 + c] = out[5 + c] + jnp.where(head_kept, ends[c], ends[c + 1])
        return out

    out = row_tile(pl.ds(ROWS, 8))
    for c in range(8):
        width = min(LANES, E_NEW - c * LANES)
        jac_ref[0:1, c * LANES : c * LANES + width] = out[c][0:1, :width]
    copies = [pltpu.make_async_copy(jac_ref, jac_hbm, sems.at[ROWS // CHUNK])]
    copies[0].start()
    for chunk in range(ROWS // CHUNK):
        for n in range(CHUNK // 8):
            row = chunk * CHUNK + 8 * n
            out = row_tile(pl.ds(row, 8))
            for c in range(7):
                out_ref[row : row + 8, c * LANES : (c + 1) * LANES] = out[c]
            out_ref[row : row + 8, 7 * LANES : E_NEW] = out[7][:, : E_NEW - 7 * LANES]
        rows = pl.ds(chunk * CHUNK, CHUNK)
        copy = pltpu.make_async_copy(out_ref.at[rows], out_hbm.at[rows], sems.at[chunk])
        copy.start()
        copies.append(copy)
    for copy in copies:
        copy.wait()


def vmem(count):
    return [pl.BlockSpec(memory_space=pltpu.VMEM)] * count


def shards(nodal_state, inverse_jacobian, speeds, refine_flags, send_index, face_source):
    x = nodal_state.reshape(ROWS, E_DEV)
    jac = inverse_jacobian.reshape(1, E_DEV)
    flags = refine_flags.reshape(1, E_DEV)
    dma = pltpu.SemaphoreType.DMA
    frame, head, info = pl.pallas_call(
        kernel,
        out_shape=(
            jax.ShapeDtypeStruct((TILES + 2, FRAME, LANES), F32),
            jax.ShapeDtypeStruct((2, FRAME, LANES), F32),
            jax.ShapeDtypeStruct((2, LANES), jnp.int32),
        ),
        in_specs=[pl.BlockSpec(memory_space=pltpu.HBM)] * 7,
        out_specs=tuple(vmem(3)),
        scratch_shapes=[
            pltpu.VMEM((1, E_DEV), F32),
            pltpu.SMEM((3, VARS), F32),
            pltpu.VMEM((1, E_DEV), jnp.int32),
            pltpu.VMEM((4 * SLOTS,), jnp.int32),
            pltpu.VMEM((6, E_DEV), jnp.int32),
            pltpu.VMEM((64, 64), F32),
            pltpu.VMEM((GROUPS, ROWS, LANES), F32),
            pltpu.VMEM((6, 160, E_DEV), BF16),
            pltpu.VMEM((4, 80, LANES), F32),
            pltpu.VMEM((4, 80, LANES), F32),
            pltpu.VMEM((160, E_DEV), BF16),
            pltpu.VMEM((6, 80, E_DEV), F32),
            pltpu.VMEM((8, E_DEV), F32),
            pltpu.VMEM((GROUPS, ROWS, LANES), F32),
            pltpu.VMEM((2 * ROWS, E_DEV), BF16),
            pltpu.VMEM((2, E_DEV, LANES), F32),
            pltpu.VMEM((16, E_DEV), BF16),
            pltpu.VMEM((TILES, 40, 8, LANES), F32),
            pltpu.VMEM((7, E_DEV, 2 * LANES), BF16),
            pltpu.VMEM((2 * ROWS, 2 * LANES), F32),
            pltpu.VMEM((2 * ROWS, 2 * LANES), F32),
            pltpu.VMEM((VARS, 64, LANES), F32),
            pltpu.VMEM((6, E_DEV, E_DEV), BF16),
            pltpu.VMEM((ROW_OF - 1, 1, LANES), jnp.int32),
            pltpu.VMEM((SIDE - 1, 1, LANES), jnp.int32),
            pltpu.VMEM((SIDE - 1, 1, LANES), jnp.int32),
            pltpu.VMEM((1, LANES), jnp.int32),
            pltpu.VMEM((1, LANES), jnp.int32),
            pltpu.VMEM((1, LANES), jnp.int32),
            dma((6,)), dma((GROUPS,)), dma((4,)), dma((4,)), dma((ROW_OF - 1,)),
            dma((ROW_OF - 1,)), dma((SIDE - 1,)), dma((SIDE - 1,)), dma((SIDE - 1,)),
            dma((SIDE - 1,)),
            dma((2,)), dma((2,)), dma((2,)), dma((2,)),
        ],
        compiler_params=pltpu.CompilerParams(
            collective_id=0, has_side_effects=True, vmem_limit_bytes=28 << 20
        ),
        name="step",
    )(*[
        pltpu.with_memory_space_constraint(a, pltpu.HBM)
        for a in (x, jac, speeds, flags, send_index, face_source, jnp.asarray(MODES, F32))
    ])
    out, out_jac = pl.pallas_call(
        place_kernel,
        out_shape=(
            jax.ShapeDtypeStruct((ROWS, E_NEW), F32),
            jax.ShapeDtypeStruct((1, E_NEW), F32),
        ),
        in_specs=vmem(3),
        out_specs=(
            pl.BlockSpec(memory_space=pltpu.HBM), pl.BlockSpec(memory_space=pltpu.HBM)
        ),
        scratch_shapes=[
            pltpu.VMEM((ROWS, E_NEW), F32), pltpu.VMEM((1, E_NEW), F32), dma((ROWS // CHUNK + 1,))
        ],
        compiler_params=pltpu.CompilerParams(vmem_limit_bytes=16 << 20),
        name="place",
    )(frame, head, info)
    return out.reshape(VARS, 64, E_NEW), out_jac.reshape(E_NEW)


def solution(mesh):
    axis = P("curve")
    wide = P(None, None, "curve")
    return jax.shard_map(
        shards,
        mesh=mesh,
        in_specs=(wide, axis, P(), axis, axis, P(None, "curve")),
        out_specs=(wide, axis),
        check_vma=False,
    )
```

```python
import functools
import math

import jax
import jax.numpy as jnp
import numpy as np
from jax import lax
from jax.experimental import pallas as pl
from jax.experimental.pallas import tpu as pltpu
from jax.sharding import PartitionSpec as P

TIME_STEP = 0.02
VARS = 5
E_DEV = 512
E_NEW = 960
SLOTS = 96
ROWS = 64 * VARS
LANES = 128
GROUPS = E_DEV // LANES
ROW_OF = 8
SIDE = 4
F32 = jnp.float32
BF16 = jnp.bfloat16
MESH = pl.DeviceIdType.MESH


def lagrange_at(points, targets):
    values_at = np.ones((len(targets), 4))
    for basis_id in range(4):
        for partner in range(4):
            if partner != basis_id:
                values_at[:, basis_id] *= (targets - points[partner]) / (
                    points[basis_id] - points[partner]
                )
    return values_at


def tables():
    root = 1.0 / math.sqrt(5.0)
    points = np.array([-1.0, -root, root, 1.0])
    weights = np.array([1.0, 5.0, 5.0, 1.0]) / 6.0
    bary = np.ones(4)
    for a in range(4):
        for b in range(4):
            if a != b:
                bary[a] /= points[a] - points[b]
    deriv = np.zeros((4, 4))
    for a in range(4):
        for b in range(4):
            if a != b:
                deriv[a, b] = bary[b] / bary[a] / (points[a] - points[b])
        deriv[a, a] = -np.sum(deriv[a])
    skew = weights[:, None] * deriv
    legendre = np.stack(
        [points**0, points, 0.5 * (3 * points**2 - 1), 0.5 * (5 * points**3 - 3 * points)], axis=1
    )
    to_modes = np.linalg.inv(legendre)
    sides = [lagrange_at(points, (points - 1.0) / 2.0), lagrange_at(points, (points + 1.0) / 2.0)]
    return skew, np.kron(to_modes, np.kron(to_modes, to_modes)), sides


SKEW, MODES, SIDES = tables()
Q01, Q02, Q03, Q12 = (float(SKEW[0, 1]), float(SKEW[0, 2]), float(SKEW[0, 3]), float(SKEW[1, 2]))
END, MID = 6.0, 1.2


def split2(x):
    high = x.astype(BF16)
    return high, (x - high.astype(F32)).astype(BF16)


def low_half(shape):
    return (lax.broadcasted_iota(jnp.int32, shape, 0) & 7) < 4


def turn(x):
    return pltpu.roll(x, 4, 0)


def fetch_state(x_ref, tile_ref, sems):
    copies = []
    for g in range(GROUPS):
        copy = pltpu.make_async_copy(
            x_ref.at[:, g * LANES : (g + 1) * LANES], tile_ref.at[g], sems.at[g]
        )
        copy.start()
        copies.append(copy)
    return copies


def build_traces(tile_ref, trace_ref, g):
    low = low_half((8, LANES))
    cols = slice(g * LANES, (g + 1) * LANES)
    for v in range(VARS):
        base = 64 * v
        tiles = [tile_ref[g, base + 8 * t : base + 8 * t + 8, :] for t in range(8)]
        first, last = tiles[0::2], tiles[1::2]
        sets = {
            0: [tile_ref[g, pl.ds(base + 32 * h, 8, stride=4), :] for h in range(2)],
            1: [tile_ref[g, pl.ds(base + 32 * h + 3, 8, stride=4), :] for h in range(2)],
            2: [jnp.where(low, first[k], turn(first[k + 1])) for k in (0, 2)],
            3: [jnp.where(low, turn(last[k]), last[k + 1]) for k in (0, 2)],
            4: tiles[0:2],
            5: tiles[6:8],
        }
        for f, rows in sets.items():
            high, rest = split2(jnp.concatenate(rows, axis=0))
            trace_ref[f, 16 * v : 16 * v + 16, cols] = high
            trace_ref[f, 80 + 16 * v : 96 + 16 * v, cols] = rest


def one_hot(index, size, width):
    rows = lax.broadcasted_iota(jnp.int32, (size, width), 0).astype(jnp.int16)
    index = jnp.broadcast_to(index, (16, width)).astype(jnp.int16)
    index = jnp.concatenate([index] * (size // 16), axis=0)
    return jnp.where(
        rows == index, jnp.ones((size, width), BF16), jnp.zeros((size, width), BF16)
    )


def gather_sends(send_ref, trace_ref, out_ref):
    packed = jnp.broadcast_to(send_ref[...].reshape(1, 4 * SLOTS), (8, 4 * SLOTS))
    for pair in range(2):
        moved = [
            packed if block == 0 else pltpu.roll(packed, 4 * SLOTS - SLOTS * block, 1)
            for block in (2 * pair, 2 * pair + 1)
        ]
        index = jnp.concatenate([m[0:1, 0:LANES] for m in moved], axis=1)
        total = jnp.zeros((160, 2 * LANES), F32)
        for f in range(6):
            total = total + jnp.dot(
                trace_ref[f],
                one_hot(index - f * E_DEV, E_DEV, 2 * LANES),
                preferred_element_type=F32,
            )
        total = total[0:80] + total[80:160]
        for half in range(2):
            out_ref[2 * pair + half] = total[:, half * LANES : (half + 1) * LANES]


def pair_sum(ui, um, si, sm):
    return (si + sm) + ui * um


def line_update(u, coef):
    ca, cb, c02, c03, cd = coef
    s = [x * x for x in u]
    m = [jnp.abs(x) for x in u]
    e = []
    for n, c in ((0, ca), (1, cb), (2, ca)):
        g = pair_sum(u[n], u[n + 1], s[n], s[n + 1])
        e.append(c * g - cd * (jnp.maximum(m[n], m[n + 1]) * (u[n + 1] - u[n])))
    r02 = c02 * pair_sum(u[0], u[2], s[0], s[2])
    r13 = c02 * pair_sum(u[1], u[3], s[1], s[3])
    r03 = c03 * pair_sum(u[0], u[3], s[0], s[3])
    t0 = -(e[0] + r02 + r03)
    t1 = e[0] - e[1] - r13
    t2 = e[1] - e[2] + r02
    t3 = e[2] + r13 + r03
    return t0, t1, t2, t3


def edge(u, o, cg, cd):
    g = pair_sum(u, o, u * u, o * o)
    return cg * g - cd * (jnp.maximum(jnp.abs(u), jnp.abs(o)) * (u - o))


def rows8(x):
    return jnp.broadcast_to(x, (8, LANES))


def blend_rates(tile_ref, modes_ref, jac_ref, rate_ref):
    n = lax.broadcasted_iota(jnp.int32, (64, LANES), 0)
    top = ((n & 3) == 3) | ((n & 12) == 12) | (n >= 48)
    for g in range(GROUPS):
        cols = slice(g * LANES, (g + 1) * LANES)
        modal = jnp.dot(
            modes_ref[...], tile_ref[g, 0:64, :], precision=lax.Precision.HIGHEST,
            preferred_element_type=F32,
        )
        energy = modal * modal
        high = jnp.sum(jnp.where(top, energy, 0.0), axis=0, keepdims=True)
        full = jnp.sum(energy, axis=0, keepdims=True)
        ratio = high / (full + 1e-06)
        blend = 0.5 * ratio / (ratio + 0.1)
        step = TIME_STEP * jac_ref[0:1, cols]
        rate_ref[0:1, cols] = step * (1.0 - blend)
        rate_ref[1:2, cols] = step * blend
        rate_ref[2:3, cols] = step


def outside_near(source_ref, trace_ref, far_ref, outside_ref):
    for f in range(6):
        index = source_ref[f : f + 1, :]
        total = jnp.dot(
            trace_ref[f ^ 1],
            one_hot(index - (f ^ 1) * E_DEV, E_DEV, E_DEV),
            preferred_element_type=F32,
        )
        outside_ref[f] = total[0:80] + total[80:160]
        far = index - 6 * E_DEV
        slot = (
            (far >= SLOTS).astype(jnp.int32)
            + (far >= 2 * SLOTS).astype(jnp.int32)
            + (far >= 3 * SLOTS).astype(jnp.int32)
        )
        far_ref[f] = one_hot(
            jnp.where(far >= 0, far + (LANES - SLOTS) * slot, -1), E_DEV, E_DEV
        )


def split_ghost(ghost_ref, ghost_bf):
    for slot in range(4):
        high, rest = split2(ghost_ref[slot])
        ghost_bf[0:80, slot * LANES : (slot + 1) * LANES] = high
        ghost_bf[80:160, slot * LANES : (slot + 1) * LANES] = rest


def outside_far(half, far_ref, ghost_bf, outside_ref):
    cols = pl.ds(pl.multiple_of(2 * LANES * half, 2 * LANES), 2 * LANES)
    for f in range(6):
        total = jnp.dot(ghost_bf[...], far_ref[f, :, cols], preferred_element_type=F32)
        outside_ref[f, :, cols] += total[0:80] + total[80:160]


def coefs_of(d, v, speed_ref, hi, lo):
    a = speed_ref[d, v]
    third = (a / 3.0) * hi
    sixth = (a / 6.0) * lo
    return [
        rows8(c)
        for c in (
            Q01 * third + sixth, Q12 * third + sixth, Q02 * third, Q03 * third,
            (0.5 * jnp.abs(a)) * lo,
        )
    ]


def interior_block(v, g, tile_ref, speed_ref, rate_ref, state_ref):
    base = pl.multiple_of(64 * v, 64)
    cols = pl.ds(pl.multiple_of(g * LANES, LANES), LANES)
    hi = rate_ref[0:1, cols]
    lo = rate_ref[1:2, cols]
    low = low_half((8, LANES))
    coef = coefs_of(0, v, speed_ref, hi, lo)
    for h in range(2):
        u = [tile_ref[g, pl.ds(base + 32 * h + i, 8, stride=4), :] for i in range(4)]
        t = line_update(u, coef)
        for i, w in enumerate((END, MID, MID, END)):
            state_ref[g, pl.ds(base + 32 * h + i, 8, stride=4), :] = u[i] + w * t[i]
    tiles = [tile_ref[g, pl.ds(base + 8 * t, 8), :] for t in range(8)]
    coef = coefs_of(2, v, speed_ref, hi, lo)
    total = [None] * 8
    for h in range(2):
        t = line_update([tiles[2 * k + h] for k in range(4)], coef)
        for k, w in enumerate((END, MID, MID, END)):
            total[2 * k + h] = w * t[k]
    ca, cb, c02, c03, cd = coefs_of(1, v, speed_ref, hi, lo)
    signed = jnp.where(low, -ca, ca)
    cross = jnp.where(low, -c03, -cb)
    cross_d = jnp.where(low, 0.0, cd)
    wa = jnp.where(low, END, MID)
    wb = jnp.where(low, MID, END)
    for k in range(4):
        a, b = tiles[2 * k], tiles[2 * k + 1]
        at, bt = turn(a), turn(b)
        sa, sb, sat, sbt = a * a, b * b, at * at, bt * bt
        ma, mb, mat, mbt = jnp.abs(a), jnp.abs(b), jnp.abs(at), jnp.abs(bt)
        x1 = signed * pair_sum(a, at, sa, sat) + cd * (jnp.maximum(ma, mat) * (at - a))
        x2 = signed * pair_sum(b, bt, sb, sbt) + cd * (jnp.maximum(mb, mbt) * (bt - b))
        x3 = c02 * pair_sum(a, b, sa, sb)
        x4 = cross * pair_sum(a, bt, sa, sbt) + cross_d * (jnp.maximum(ma, mbt) * (bt - a))
        total[2 * k] += wa * (x1 - x3 + x4)
        total[2 * k + 1] += wb * (x2 + x3 - turn(x4))
    for t in range(8):
        state_ref[g, pl.ds(base + 8 * t, 8), :] += total[t]


def edge_block(v, g, tile_ref, speed_ref, rate_ref, outside_ref, state_ref, up_ref):
    base = pl.multiple_of(64 * v, 64)
    face = pl.multiple_of(16 * v, 16)
    cols = pl.ds(pl.multiple_of(g * LANES, LANES), LANES)
    step = rate_ref[2:3, cols]
    low = low_half((8, LANES))

    def coefs(d):
        a = speed_ref[d, v]
        return rows8((a * (END / 6.0)) * step), rows8((0.5 * END) * jnp.abs(a) * step)

    bg, bd = coefs(0)
    for h in range(2):
        for f, i, sign in ((0, 0, bg), (1, 3, -bg)):
            rows = pl.ds(base + 32 * h + i, 8, stride=4)
            outer = outside_ref[f, pl.ds(face + 8 * h, 8), cols]
            state_ref[g, rows, :] += edge(tile_ref[g, rows, :], outer, sign, bd)
    tiles = [tile_ref[g, pl.ds(base + 8 * t, 8), :] for t in range(8)]
    total = [state_ref[g, pl.ds(base + 8 * t, 8), :] for t in range(8)]
    bg, bd = coefs(2)
    for h in range(2):
        for f, k, sign in ((4, 0, bg), (5, 3, -bg)):
            outer = outside_ref[f, pl.ds(face + 8 * h, 8), cols]
            total[2 * k + h] += edge(tiles[2 * k + h], outer, sign, bd)
    bg, bd = coefs(1)
    bgs = jnp.where(low, bg, -bg)
    outer_l = [outside_ref[2, pl.ds(face + 8 * h, 8), cols] for h in range(2)]
    outer_r = [outside_ref[3, pl.ds(face + 8 * h, 8), cols] for h in range(2)]
    for k in range(4):
        ol = outer_l[k // 2]
        orr = outer_r[k // 2]
        outer = jnp.where(low, ol, turn(orr)) if k % 2 == 0 else jnp.where(low, turn(ol), orr)
        bound = edge(jnp.where(low, tiles[2 * k], tiles[2 * k + 1]), outer, bgs, bd)
        total[2 * k] += jnp.where(low, bound, 0.0)
        total[2 * k + 1] += jnp.where(low, 0.0, bound)
    for t in range(4):
        high, rest = split2(jnp.concatenate(total[2 * t : 2 * t + 2], axis=0))
        up_ref[pl.ds(pl.multiple_of(base + 16 * t, 16), 16), cols] = high
        up_ref[pl.ds(pl.multiple_of(ROWS + base + 16 * t, 16), 16), cols] = rest


def refine_tables(flag_ref, jac_ref, start_ref, aux_ref):
    flags = flag_ref[...].astype(F32)
    wide = jnp.broadcast_to(flags, (LANES, E_DEV)).astype(BF16)
    row = lax.broadcasted_iota(jnp.int32, (E_DEV, E_DEV), 0)
    col = lax.broadcasted_iota(jnp.int32, (E_DEV, E_DEV), 1)
    ahead = jnp.where(col < row, 1.0, 0.0).astype(BF16)
    within = jnp.where(col <= row, 1.0, 0.0).astype(BF16)
    dims = (((1,), (1,)), ((), ()))
    place = lax.broadcasted_iota(jnp.int32, (E_DEV, LANES), 0).astype(F32)
    start_ref[0] = place + 7.0 * lax.dot_general(ahead, wide, dims, preferred_element_type=F32)
    start_ref[1] = (
        place + 1.0 + 7.0 * lax.dot_general(within, wide, dims, preferred_element_type=F32)
    )
    count = lax.dot_general(wide[0:16], ahead, dims, preferred_element_type=F32)[0:1]
    at = lax.broadcasted_iota(jnp.int32, (1, E_DEV), 1).astype(F32) + 7.0 * count
    at_high = jnp.floor(at * (1.0 / 16.0))
    jac = jac_ref[...]
    j0, rest = split2(jac)
    rest = jac - j0.astype(F32)
    j1 = rest.astype(BF16)
    j2 = (rest - j1.astype(F32)).astype(BF16)
    zero = jnp.zeros((10, E_DEV), F32)
    aux_ref[...] = jnp.concatenate(
        [
            at_high, at - 16.0 * at_high, flags, j0.astype(F32), j1.astype(F32), j2.astype(F32),
            zero,
        ],
        axis=0,
    ).astype(BF16)


def column_tables(tile, first, start_ref, aux_ref, coef_ref, hot_ref):
    place = lax.broadcasted_iota(jnp.int32, (1, LANES), 1).astype(F32) + first
    inside = (place >= start_ref[0]) & (place < start_ref[1])
    hot = jnp.where(inside, 1.0, 0.0).astype(BF16)
    cols = pl.ds(pl.multiple_of((tile % 2) * LANES, LANES), LANES)
    hot_ref[tile // 2, :, cols] = hot
    aux = jnp.dot(aux_ref[...], hot, preferred_element_type=F32)
    child = place - (16.0 * aux[0:1] + aux[1:2])
    refined = aux[2:3] > 0.5
    z = child >= 4.0
    child = child - jnp.where(z, 4.0, 0.0)
    y = child >= 2.0
    child = child - jnp.where(y, 2.0, 0.0)
    x = child >= 1.0
    jac = (aux[3:4] + aux[4:5] + aux[5:6]) * jnp.where(refined, 2.0, 1.0)

    def table(bit):
        return [
            [
                rows8(
                    jnp.where(
                        refined,
                        jnp.where(bit, float(SIDES[1][i, m]), float(SIDES[0][i, m])),
                        1.0 if i == m else 0.0,
                    )
                )
                for m in range(4)
            ]
            for i in range(4)
        ]

    cx, cy, cz = table(x), table(y), table(z)
    low = low_half((8, LANES))
    n = 0
    for i in range(4):
        for m in range(4):
            coef_ref[tile, n] = cx[i][m]
            coef_ref[tile, 16 + n] = cz[i][m]
            n += 1
    order = [(0, 1), (1, 0), (2, 3), (3, 2)]
    for at, (first_j, last_j) in enumerate(((0, 1), (2, 3))):
        for k, (lo_m, hi_m) in enumerate(order):
            coef_ref[tile, 32 + 4 * at + k] = jnp.where(low, cy[first_j][lo_m], cy[last_j][hi_m])
    return jac


def combine4(c, u):
    return (c[0] * u[0] + c[1] * u[1]) + (c[2] * u[2] + c[3] * u[3])


def interpolate(v, tile, half, pick_ref, coef_ref, line_ref, put):
    base = 64 * v
    cols = slice(half * LANES, half * LANES + LANES)
    tiles = [
        pick_ref[base + 8 * t : base + 8 * t + 8, cols]
        + pick_ref[ROWS + base + 8 * t : ROWS + base + 8 * t + 8, cols]
        for t in range(8)
    ]
    mid = [None] * 8
    for h in range(2):
        u = [tiles[2 * k + h] for k in range(4)]
        for k in range(4):
            mid[2 * k + h] = combine4([coef_ref[tile, 16 + 4 * k + m] for m in range(4)], u)
    for k in range(4):
        a, b = mid[2 * k], mid[2 * k + 1]
        u = [a, turn(a), b, turn(b)]
        for at in range(2):
            line_ref[v, 16 * k + 8 * at : 16 * k + 8 * at + 8, :] = combine4(
                [coef_ref[tile, 32 + 4 * at + m] for m in range(4)], u
            )
    for h in range(2):
        u = [line_ref[v, pl.ds(32 * h + i, 8, stride=4), :] for i in range(4)]
        for i in range(4):
            put(base + 32 * h + i, combine4([coef_ref[tile, 4 * i + m] for m in range(4)], u))


TILES = 13
FRAME = ROWS + 8


def kernel(
    x_hbm, jac_hbm, speed_hbm, flag_hbm, send_hbm, source_hbm, modes_hbm,
    frame_ref, head_ref, info_ref,
    jac_ref, speed_ref, flag_ref, send_ref, source_ref, modes_ref,
    tile_ref, trace_ref, out_buf, ghost_ref, ghost_bf, outside_ref, rate_ref, state_ref, up_ref,
    start_ref, aux_ref, coef_ref, hot_ref, pick_a, pick_b, line_ref, far_ref,
    row_buf, z_buf, y_buf, mine, row_sum, plane_sum, behind_ref,
    small_sems, fetch_sems, send_sems, recv_sems, row_send, row_recv, z_send, z_recv,
    y_send, y_recv,
    head_send, head_recv, tail_send, tail_recv, reply,
):
    me = lax.axis_index("curve")
    devices = ROW_OF * SIDE * SIDE
    row_at = me % ROW_OF
    z_at = me // ROW_OF % SIDE
    y_at = me // (ROW_OF * SIDE)
    near = [(me + devices + o) % devices for o in (-2, -1, 1, 2)]
    row_mates = [me - row_at + (row_at + k) % ROW_OF for k in range(1, ROW_OF)]
    z_mates = [me + ROW_OF * ((z_at + k) % SIDE - z_at) for k in range(1, SIDE)]
    early = me % (ROW_OF * SIDE) < 2
    awaited = me >= devices - 4
    barrier = pltpu.get_barrier_semaphore()
    for b, partner in enumerate(near):

        @pl.when(me + (-2, -1, 1, 2)[b] < devices)
        def _(partner=partner):
            pl.semaphore_signal(barrier, inc=1, device_id=(partner,), device_id_type=MESH)

    fetches = fetch_state(x_hbm, tile_ref, fetch_sems)
    for partner in row_mates + z_mates:
        pl.semaphore_signal(barrier, inc=1, device_id=(partner,), device_id_type=MESH)
    for k in range(1, SIDE):

        @pl.when(y_at >= k)
        def _(k=k):
            pl.semaphore_signal(
                barrier, inc=1, device_id=(me - k * ROW_OF * SIDE,), device_id_type=MESH
            )

    small = []
    for at, (src, dst) in enumerate(
        (
            (send_hbm, send_ref), (flag_hbm, flag_ref), (source_hbm, source_ref),
            (jac_hbm, jac_ref), (modes_hbm, modes_ref), (speed_hbm, speed_ref),
        )
    ):
        copy = pltpu.make_async_copy(src, dst, small_sems.at[at])
        copy.start()
        small.append(copy)

    def send(src, dst, send_sem, recv_sem, mate):
        copy = remote(src, dst, send_sem, recv_sem, mate)
        copy.start()
        return copy

    def remote(src, dst, send_sem, recv_sem, mate):
        return pltpu.make_async_remote_copy(
            src_ref=src, dst_ref=dst, send_sem=send_sem, recv_sem=recv_sem,
            device_id=(mate,), device_id_type=MESH,
        )

    for g in range(GROUPS):
        fetches[g].wait()
        build_traces(tile_ref, trace_ref, g)
    small[0].wait()
    gather_sends(send_ref, trace_ref, out_buf)
    for copy in small[1:]:
        copy.wait()
    count = jnp.sum(flag_ref[...].astype(F32), axis=1, keepdims=True)
    mine[...] = jnp.broadcast_to(count, (1, LANES)).astype(jnp.int32) - 64
    total_new = 7.0 * jnp.broadcast_to(count, (1, LANES)) + float(E_DEV)

    def near_work():
        outside_near(source_ref, trace_ref, far_ref, outside_ref)
        blend_rates(tile_ref, modes_ref, jac_ref, rate_ref)

    def table_step(tile, carry):
        shift = (jnp.full((1, LANES), tile, jnp.int32) * LANES).astype(F32)
        first = shift - 2.0 * LANES + jnp.where(tile < 2, total_new, 0.0)
        jac_row = rows8(column_tables(tile, first, start_ref, aux_ref, coef_ref, hot_ref))
        frame_ref[jnp.where(tile < 2, TILES + tile, tile), ROWS:FRAME, :] = jac_row
        return carry

    def inner_work():
        def interior_step(n, carry):
            interior_block(n // GROUPS, n % GROUPS, tile_ref, speed_ref, rate_ref, state_ref)
            return carry

        lax.fori_loop(0, VARS * GROUPS, interior_step, 0)
        refine_tables(flag_ref, jac_ref, start_ref, aux_ref)
        lax.fori_loop(0, 4, table_step, 0)

    def own_tables():
        lax.fori_loop(4, TILES, table_step, 0)

    pl.when(jnp.logical_not(awaited))(near_work)
    pl.when(early)(inner_work)
    pl.semaphore_wait(
        barrier, 4 - jnp.maximum(2 - me, 0) + ROW_OF - 1 + SIDE - 1 + SIDE - 1 - y_at
    )
    for b in (2, 3):

        @pl.when(me + b - 1 >= devices)
        def _(b=b):
            pl.semaphore_signal(reply, inc=1, device_id=(near[b],), device_id_type=MESH)

    halo = {
        b: remote(
            out_buf.at[b], ghost_ref.at[3 - b], send_sems.at[b], recv_sems.at[3 - b], near[b]
        )
        for b in (1, 3, 0, 2)
    }
    for b in (1, 3, 0, 2):
        pl.when(me >= 2 - b)(halo[b].start)
    row_copies = [
        send(mine, row_buf.at[k], row_send.at[k], row_recv.at[k], mate)
        for k, mate in enumerate(row_mates)
    ]
    pl.when(awaited)(near_work)
    pl.when(jnp.logical_not(early))(inner_work)
    pl.when(early)(own_tables)

    @pl.when(me < 2)
    def _():
        pl.semaphore_wait(reply, 2 - me)
        for b in range(2):
            pl.when(me < 2 - b)(halo[b].start)

    def gathered(copies, own_ref, buf_ref, at, sum_ref):
        for copy in copies:
            copy.wait()
        total = own_ref[...]
        behind = behind_ref[...]
        for k in range(len(copies)):
            value = buf_ref[k]
            total = total + value
            behind = behind + jnp.where(at >= k + 1, value, 0)
        sum_ref[...] = total
        behind_ref[...] = behind

    behind_ref[...] = jnp.zeros((1, LANES), jnp.int32)
    z_copies = [
        remote(row_sum, z_buf.at[k], z_send.at[k], z_recv.at[k], mate)
        for k, mate in enumerate(z_mates)
    ]
    y_copies = [
        remote(
            plane_sum, y_buf.at[k - 1], y_send.at[k - 1], y_recv.at[k - 1],
            (me + k * ROW_OF * SIDE) % devices,
        )
        for k in range(1, SIDE)
    ]

    def row_stage():
        gathered(row_copies, mine, row_buf, row_at, row_sum)
        for copy in z_copies:
            copy.start()

    row_stage()
    for b in range(4):
        halo[b].wait_send()
        halo[3 - b].wait_recv()
    split_ghost(ghost_ref, ghost_bf)
    first, last = me == 0, me == devices - 1

    def tail(h):
        return remote(
            frame_ref.at[TILES + h], frame_ref.at[h], tail_send.at[h], tail_recv.at[h], near[2]
        )

    def head(h):
        return remote(
            frame_ref.at[2 + h], head_ref.at[h], head_send.at[h], head_recv.at[h], near[1]
        )

    def fill(dst, tile, half, pick_ref):
        for v in range(VARS):

            def put(row, value):
                frame_ref[dst, pl.ds(row, 8, stride=4), :] = value

            interpolate(v, tile, half, pick_ref, coef_ref, line_ref, put)

    for order in range(2):
        part = me % 2 if order == 0 else 1 - me % 2
        outside_far(part, far_ref, ghost_bf, outside_ref)

        for step in range(2):
            half = jnp.where(part == 1, 1 - step, step)
            group = 2 * part + half

            def edge_step(v, carry, group=group):
                edge_block(
                    v, group, tile_ref, speed_ref, rate_ref, outside_ref, state_ref, up_ref
                )
                return carry

            lax.fori_loop(0, VARS, edge_step, 0)
            within = (
                pl.ds(pl.multiple_of(LANES * group, LANES), LANES)
                if step == 0
                else pl.ds(pl.multiple_of(2 * LANES * part, 2 * LANES), 2 * LANES)
            )
            cols = pl.ds(pl.multiple_of(LANES * half, LANES), LANES)
            pick_a[:, 0:LANES] = jnp.dot(
                up_ref[:, within], hot_ref[1 - part, within, cols], preferred_element_type=F32
            )
            fill(jnp.where(part == 1, TILES, 2) + half, 2 * (1 - part) + half, 0, pick_a)
            pl.when((part == 1) & jnp.logical_not(last))(tail(half).start)
            pl.when((part == 0) & jnp.logical_not(first))(head(half).start)

    pl.when(jnp.logical_not(early))(own_tables)
    gathered(z_copies, row_sum, z_buf, z_at, plane_sum)
    for k in range(1, SIDE):
        pl.when(y_at + k < SIDE)(y_copies[k - 1].start)

    picks = [pick_a, pick_b]
    pick_a[...] = jnp.dot(up_ref[...], hot_ref[2], preferred_element_type=F32)
    for pair in range(2, 7):
        now, later = picks[pair % 2], picks[(pair + 1) % 2]
        if pair < 5:
            later[...] = jnp.dot(up_ref[...], hot_ref[pair + 1], preferred_element_type=F32)
        if pair == 5:
            later[:, 0:LANES] = jnp.dot(
                up_ref[...], hot_ref[6, :, 0:LANES], preferred_element_type=F32
            )
        for half in range(2 if pair < 6 else 1):
            fill(2 * pair + half, 2 * pair + half, half, now)

    behind = behind_ref[...]
    for k in range(1, SIDE):
        pl.when(y_at + k < SIDE)(y_copies[k - 1].wait_send)
        pl.when(y_at >= k)(y_copies[k - 1].wait_recv)
        behind = behind + jnp.where(y_at >= k, y_buf[k - 1], 0)
    info_ref[0:1, :] = behind
    info_ref[1:2, :] = total_new.astype(jnp.int32)
    for half in range(2):

        @pl.when(jnp.logical_not(last))
        def _(half=half):
            tail(half).wait_send()
            head(half).wait_recv()

        @pl.when(jnp.logical_not(first))
        def _(half=half):
            head(half).wait_send()
            tail(half).wait_recv()


CHUNK = 64


def place_kernel(frame_ref, head_ref, info_ref, out_hbm, jac_hbm, out_ref, jac_ref, sems):
    shift = 7 * jnp.max(info_ref[0:1, :])
    size = jnp.max(info_ref[1:2, :])
    begin = 2 * LANES - shift
    tile = begin // LANES
    turn_by = begin - tile * LANES
    over = -(size + shift)
    head_tile = over // LANES
    head_turn = over - head_tile * LANES
    lane = lax.broadcasted_iota(jnp.int32, (8, LANES), 1)
    kept = lane < LANES - turn_by
    head_kept = lane < LANES - head_turn
    back = (LANES - turn_by) % LANES
    head_back = (LANES - head_turn) % LANES

    def row_tile(rows):
        parts = [pltpu.roll(frame_ref[tile + c, rows, :], back, 1) for c in range(9)]
        out = [jnp.where(kept, parts[c], parts[c + 1]) for c in range(8)]
        heads = [pltpu.roll(head_ref[c, rows, :], head_back, 1) for c in range(2)]
        ends = [
            jnp.where(head_tile + 5 + c == 0, heads[0], jnp.where(head_tile + 5 + c == 1, heads[1], 0.0))
            for c in range(4)
        ]
        for c in range(3):
            out[5 + c] = out[5 + c] + jnp.where(head_kept, ends[c], ends[c + 1])
        return out

    copies = []
    for chunk in range(ROWS // CHUNK):
        for n in range(CHUNK // 8):
            row = chunk * CHUNK + 8 * n
            out = row_tile(pl.ds(row, 8))
            for c in range(7):
                out_ref[row : row + 8, c * LANES : (c + 1) * LANES] = out[c]
            out_ref[row : row + 8, 7 * LANES : E_NEW] = out[7][:, : E_NEW - 7 * LANES]
        rows = pl.ds(chunk * CHUNK, CHUNK)
        copy = pltpu.make_async_copy(out_ref.at[rows], out_hbm.at[rows], sems.at[chunk])
        copy.start()
        copies.append(copy)
    out = row_tile(pl.ds(ROWS, 8))
    for c in range(8):
        width = min(LANES, E_NEW - c * LANES)
        jac_ref[0:1, c * LANES : c * LANES + width] = out[c][0:1, :width]
    copies.append(pltpu.make_async_copy(jac_ref, jac_hbm, sems.at[ROWS // CHUNK]))
    copies[-1].start()
    for copy in copies:
        copy.wait()


def vmem(count):
    return [pl.BlockSpec(memory_space=pltpu.VMEM)] * count


def shards(nodal_state, inverse_jacobian, speeds, refine_flags, send_index, face_source):
    x = nodal_state.reshape(ROWS, E_DEV)
    jac = inverse_jacobian.reshape(1, E_DEV)
    flags = refine_flags.reshape(1, E_DEV)
    dma = pltpu.SemaphoreType.DMA
    frame, head, info = pl.pallas_call(
        kernel,
        out_shape=(
            jax.ShapeDtypeStruct((TILES + 2, FRAME, LANES), F32),
            jax.ShapeDtypeStruct((2, FRAME, LANES), F32),
            jax.ShapeDtypeStruct((2, LANES), jnp.int32),
        ),
        in_specs=[pl.BlockSpec(memory_space=pltpu.HBM)] * 7,
        out_specs=tuple(vmem(3)),
        scratch_shapes=[
            pltpu.VMEM((1, E_DEV), F32),
            pltpu.SMEM((3, VARS), F32),
            pltpu.VMEM((1, E_DEV), jnp.int32),
            pltpu.VMEM((4 * SLOTS,), jnp.int32),
            pltpu.VMEM((6, E_DEV), jnp.int32),
            pltpu.VMEM((64, 64), F32),
            pltpu.VMEM((GROUPS, ROWS, LANES), F32),
            pltpu.VMEM((6, 160, E_DEV), BF16),
            pltpu.VMEM((4, 80, LANES), F32),
            pltpu.VMEM((4, 80, LANES), F32),
            pltpu.VMEM((160, E_DEV), BF16),
            pltpu.VMEM((6, 80, E_DEV), F32),
            pltpu.VMEM((8, E_DEV), F32),
            pltpu.VMEM((GROUPS, ROWS, LANES), F32),
            pltpu.VMEM((2 * ROWS, E_DEV), BF16),
            pltpu.VMEM((2, E_DEV, LANES), F32),
            pltpu.VMEM((16, E_DEV), BF16),
            pltpu.VMEM((TILES, 40, 8, LANES), F32),
            pltpu.VMEM((7, E_DEV, 2 * LANES), BF16),
            pltpu.VMEM((2 * ROWS, 2 * LANES), F32),
            pltpu.VMEM((2 * ROWS, 2 * LANES), F32),
            pltpu.VMEM((VARS, 64, LANES), F32),
            pltpu.VMEM((6, E_DEV, E_DEV), BF16),
            pltpu.VMEM((ROW_OF - 1, 1, LANES), jnp.int32),
            pltpu.VMEM((SIDE - 1, 1, LANES), jnp.int32),
            pltpu.VMEM((SIDE - 1, 1, LANES), jnp.int32),
            pltpu.VMEM((1, LANES), jnp.int32),
            pltpu.VMEM((1, LANES), jnp.int32),
            pltpu.VMEM((1, LANES), jnp.int32),
            pltpu.VMEM((1, LANES), jnp.int32),
            dma((6,)), dma((GROUPS,)), dma((4,)), dma((4,)), dma((ROW_OF - 1,)),
            dma((ROW_OF - 1,)), dma((SIDE - 1,)), dma((SIDE - 1,)), dma((SIDE - 1,)),
            dma((SIDE - 1,)),
            dma((2,)), dma((2,)), dma((2,)), dma((2,)), pltpu.SemaphoreType.REGULAR,
        ],
        compiler_params=pltpu.CompilerParams(
            collective_id=0, has_side_effects=True, vmem_limit_bytes=28 << 20
        ),
        name="step",
    )(*[
        pltpu.with_memory_space_constraint(a, pltpu.HBM)
        for a in (x, jac, speeds, flags, send_index, face_source, jnp.asarray(MODES, F32))
    ])
    out, out_jac = pl.pallas_call(
        place_kernel,
        out_shape=(
            jax.ShapeDtypeStruct((ROWS, E_NEW), F32),
            jax.ShapeDtypeStruct((1, E_NEW), F32),
        ),
        in_specs=vmem(3),
        out_specs=(
            pl.BlockSpec(memory_space=pltpu.HBM), pl.BlockSpec(memory_space=pltpu.HBM)
        ),
        scratch_shapes=[
            pltpu.VMEM((ROWS, E_NEW), F32), pltpu.VMEM((1, E_NEW), F32), dma((ROWS // CHUNK + 1,))
        ],
        compiler_params=pltpu.CompilerParams(vmem_limit_bytes=16 << 20),
        name="place",
    )(frame, head, info)
    return out.reshape(VARS, 64, E_NEW), out_jac.reshape(E_NEW)


def solution(mesh):
    axis = P("curve")
    wide = P(None, None, "curve")
    return jax.shard_map(
        shards,
        mesh=mesh,
        in_specs=(wide, axis, P(), axis, axis, P(None, "curve")),
        out_specs=(wide, axis),
        check_vma=False,
    )
```

```python
import functools
import math

import jax
import jax.numpy as jnp
import numpy as np
from jax import lax
from jax.experimental import pallas as pl
from jax.experimental.pallas import tpu as pltpu
from jax.sharding import PartitionSpec as P

TIME_STEP = 0.02
VARS = 5
E_DEV = 512
E_NEW = 960
SLOTS = 96
ROWS = 64 * VARS
LANES = 128
GROUPS = E_DEV // LANES
ROW_OF = 8
SIDE = 4
F32 = jnp.float32
BF16 = jnp.bfloat16
MESH = pl.DeviceIdType.MESH


def lagrange_at(points, targets):
    values_at = np.ones((len(targets), 4))
    for basis_id in range(4):
        for partner in range(4):
            if partner != basis_id:
                values_at[:, basis_id] *= (targets - points[partner]) / (
                    points[basis_id] - points[partner]
                )
    return values_at


def tables():
    root = 1.0 / math.sqrt(5.0)
    points = np.array([-1.0, -root, root, 1.0])
    weights = np.array([1.0, 5.0, 5.0, 1.0]) / 6.0
    bary = np.ones(4)
    for a in range(4):
        for b in range(4):
            if a != b:
                bary[a] /= points[a] - points[b]
    deriv = np.zeros((4, 4))
    for a in range(4):
        for b in range(4):
            if a != b:
                deriv[a, b] = bary[b] / bary[a] / (points[a] - points[b])
        deriv[a, a] = -np.sum(deriv[a])
    skew = weights[:, None] * deriv
    legendre = np.stack(
        [points**0, points, 0.5 * (3 * points**2 - 1), 0.5 * (5 * points**3 - 3 * points)], axis=1
    )
    to_modes = np.linalg.inv(legendre)
    sides = [lagrange_at(points, (points - 1.0) / 2.0), lagrange_at(points, (points + 1.0) / 2.0)]
    return skew, np.kron(to_modes, np.kron(to_modes, to_modes)), sides


SKEW, MODES, SIDES = tables()
Q01, Q02, Q03, Q12 = (float(SKEW[0, 1]), float(SKEW[0, 2]), float(SKEW[0, 3]), float(SKEW[1, 2]))
END, MID = 6.0, 1.2


def split2(x):
    high = x.astype(BF16)
    return high, (x - high.astype(F32)).astype(BF16)


def low_half(shape):
    return (lax.broadcasted_iota(jnp.int32, shape, 0) & 7) < 4


def turn(x):
    return pltpu.roll(x, 4, 0)


def fetch_state(x_ref, tile_ref, sems):
    copies = []
    for g in range(GROUPS):
        copy = pltpu.make_async_copy(
            x_ref.at[:, g * LANES : (g + 1) * LANES], tile_ref.at[g], sems.at[g]
        )
        copy.start()
        copies.append(copy)
    return copies


def build_traces(tile_ref, trace_ref, g):
    low = low_half((8, LANES))
    cols = slice(g * LANES, (g + 1) * LANES)
    for v in range(VARS):
        base = 64 * v
        tiles = [tile_ref[g, base + 8 * t : base + 8 * t + 8, :] for t in range(8)]
        first, last = tiles[0::2], tiles[1::2]
        sets = {
            0: [tile_ref[g, pl.ds(base + 32 * h, 8, stride=4), :] for h in range(2)],
            1: [tile_ref[g, pl.ds(base + 32 * h + 3, 8, stride=4), :] for h in range(2)],
            2: [jnp.where(low, first[k], turn(first[k + 1])) for k in (0, 2)],
            3: [jnp.where(low, turn(last[k]), last[k + 1]) for k in (0, 2)],
            4: tiles[0:2],
            5: tiles[6:8],
        }
        for f, rows in sets.items():
            high, rest = split2(jnp.concatenate(rows, axis=0))
            trace_ref[f, 16 * v : 16 * v + 16, cols] = high
            trace_ref[f, 80 + 16 * v : 96 + 16 * v, cols] = rest


def one_hot(index, size, width):
    rows = lax.broadcasted_iota(jnp.int32, (size, width), 0).astype(jnp.int16)
    index = jnp.broadcast_to(index, (16, width)).astype(jnp.int16)
    index = jnp.concatenate([index] * (size // 16), axis=0)
    return jnp.where(
        rows == index, jnp.ones((size, width), BF16), jnp.zeros((size, width), BF16)
    )


def gather_sends(send_ref, trace_ref, out_ref):
    packed = jnp.broadcast_to(send_ref[...].reshape(1, 4 * SLOTS), (8, 4 * SLOTS))
    for pair in range(2):
        moved = [
            packed if block == 0 else pltpu.roll(packed, 4 * SLOTS - SLOTS * block, 1)
            for block in (2 * pair, 2 * pair + 1)
        ]
        index = jnp.concatenate([m[0:1, 0:LANES] for m in moved], axis=1)
        total = jnp.zeros((160, 2 * LANES), F32)
        for f in range(6):
            total = total + jnp.dot(
                trace_ref[f],
                one_hot(index - f * E_DEV, E_DEV, 2 * LANES),
                preferred_element_type=F32,
            )
        total = total[0:80] + total[80:160]
        for half in range(2):
            out_ref[2 * pair + half] = total[:, half * LANES : (half + 1) * LANES]


def pair_sum(ui, um, si, sm):
    return (si + sm) + ui * um


def line_update(u, coef):
    ca, cb, c02, c03, cd = coef
    s = [x * x for x in u]
    m = [jnp.abs(x) for x in u]
    e = []
    for n, c in ((0, ca), (1, cb), (2, ca)):
        g = pair_sum(u[n], u[n + 1], s[n], s[n + 1])
        e.append(c * g - cd * (jnp.maximum(m[n], m[n + 1]) * (u[n + 1] - u[n])))
    r02 = c02 * pair_sum(u[0], u[2], s[0], s[2])
    r13 = c02 * pair_sum(u[1], u[3], s[1], s[3])
    r03 = c03 * pair_sum(u[0], u[3], s[0], s[3])
    t0 = -(e[0] + r02 + r03)
    t1 = e[0] - e[1] - r13
    t2 = e[1] - e[2] + r02
    t3 = e[2] + r13 + r03
    return t0, t1, t2, t3


def edge(u, o, cg, cd):
    g = pair_sum(u, o, u * u, o * o)
    return cg * g - cd * (jnp.maximum(jnp.abs(u), jnp.abs(o)) * (u - o))


def rows8(x):
    return jnp.broadcast_to(x, (8, LANES))


def blend_rates(tile_ref, modes_ref, jac_ref, rate_ref):
    n = lax.broadcasted_iota(jnp.int32, (64, LANES), 0)
    top = ((n & 3) == 3) | ((n & 12) == 12) | (n >= 48)
    for g in range(GROUPS):
        cols = slice(g * LANES, (g + 1) * LANES)
        modal = jnp.dot(
            modes_ref[...], tile_ref[g, 0:64, :], precision=lax.Precision.HIGHEST,
            preferred_element_type=F32,
        )
        energy = modal * modal
        high = jnp.sum(jnp.where(top, energy, 0.0), axis=0, keepdims=True)
        full = jnp.sum(energy, axis=0, keepdims=True)
        ratio = high / (full + 1e-06)
        blend = 0.5 * ratio / (ratio + 0.1)
        step = TIME_STEP * jac_ref[0:1, cols]
        rate_ref[0:1, cols] = step * (1.0 - blend)
        rate_ref[1:2, cols] = step * blend
        rate_ref[2:3, cols] = step


def outside_near(source_ref, trace_ref, far_ref, outside_ref):
    for f in range(6):
        index = source_ref[f : f + 1, :]
        total = jnp.dot(
            trace_ref[f ^ 1],
            one_hot(index - (f ^ 1) * E_DEV, E_DEV, E_DEV),
            preferred_element_type=F32,
        )
        outside_ref[f] = total[0:80] + total[80:160]
        far = index - 6 * E_DEV
        slot = (
            (far >= SLOTS).astype(jnp.int32)
            + (far >= 2 * SLOTS).astype(jnp.int32)
            + (far >= 3 * SLOTS).astype(jnp.int32)
        )
        far_ref[f] = one_hot(
            jnp.where(far >= 0, far + (LANES - SLOTS) * slot, -1), E_DEV, E_DEV
        )


def split_ghost(ghost_ref, ghost_bf):
    for slot in range(4):
        high, rest = split2(ghost_ref[slot])
        ghost_bf[0:80, slot * LANES : (slot + 1) * LANES] = high
        ghost_bf[80:160, slot * LANES : (slot + 1) * LANES] = rest


def outside_far(half, far_ref, ghost_bf, outside_ref):
    cols = pl.ds(pl.multiple_of(2 * LANES * half, 2 * LANES), 2 * LANES)
    for f in range(6):
        total = jnp.dot(ghost_bf[...], far_ref[f, :, cols], preferred_element_type=F32)
        outside_ref[f, :, cols] += total[0:80] + total[80:160]


def coefs_of(d, v, speed_ref, hi, lo):
    a = speed_ref[d, v]
    third = (a / 3.0) * hi
    sixth = (a / 6.0) * lo
    return [
        rows8(c)
        for c in (
            Q01 * third + sixth, Q12 * third + sixth, Q02 * third, Q03 * third,
            (0.5 * jnp.abs(a)) * lo,
        )
    ]


def interior_block(v, g, tile_ref, speed_ref, rate_ref, state_ref):
    base = pl.multiple_of(64 * v, 64)
    cols = pl.ds(pl.multiple_of(g * LANES, LANES), LANES)
    hi = rate_ref[0:1, cols]
    lo = rate_ref[1:2, cols]
    low = low_half((8, LANES))
    coef = coefs_of(0, v, speed_ref, hi, lo)
    for h in range(2):
        u = [tile_ref[g, pl.ds(base + 32 * h + i, 8, stride=4), :] for i in range(4)]
        t = line_update(u, coef)
        for i, w in enumerate((END, MID, MID, END)):
            state_ref[g, pl.ds(base + 32 * h + i, 8, stride=4), :] = u[i] + w * t[i]
    tiles = [tile_ref[g, pl.ds(base + 8 * t, 8), :] for t in range(8)]
    coef = coefs_of(2, v, speed_ref, hi, lo)
    total = [None] * 8
    for h in range(2):
        t = line_update([tiles[2 * k + h] for k in range(4)], coef)
        for k, w in enumerate((END, MID, MID, END)):
            total[2 * k + h] = w * t[k]
    ca, cb, c02, c03, cd = coefs_of(1, v, speed_ref, hi, lo)
    signed = jnp.where(low, -ca, ca)
    cross = jnp.where(low, -c03, -cb)
    cross_d = jnp.where(low, 0.0, cd)
    wa = jnp.where(low, END, MID)
    wb = jnp.where(low, MID, END)
    for k in range(4):
        a, b = tiles[2 * k], tiles[2 * k + 1]
        at, bt = turn(a), turn(b)
        sa, sb, sat, sbt = a * a, b * b, at * at, bt * bt
        ma, mb, mat, mbt = jnp.abs(a), jnp.abs(b), jnp.abs(at), jnp.abs(bt)
        x1 = signed * pair_sum(a, at, sa, sat) + cd * (jnp.maximum(ma, mat) * (at - a))
        x2 = signed * pair_sum(b, bt, sb, sbt) + cd * (jnp.maximum(mb, mbt) * (bt - b))
        x3 = c02 * pair_sum(a, b, sa, sb)
        x4 = cross * pair_sum(a, bt, sa, sbt) + cross_d * (jnp.maximum(ma, mbt) * (bt - a))
        total[2 * k] += wa * (x1 - x3 + x4)
        total[2 * k + 1] += wb * (x2 + x3 - turn(x4))
    for t in range(8):
        state_ref[g, pl.ds(base + 8 * t, 8), :] += total[t]


def edge_block(v, g, tile_ref, speed_ref, rate_ref, outside_ref, state_ref, up_ref):
    base = pl.multiple_of(64 * v, 64)
    face = pl.multiple_of(16 * v, 16)
    cols = pl.ds(pl.multiple_of(g * LANES, LANES), LANES)
    step = rate_ref[2:3, cols]
    low = low_half((8, LANES))

    def coefs(d):
        a = speed_ref[d, v]
        return rows8((a * (END / 6.0)) * step), rows8((0.5 * END) * jnp.abs(a) * step)

    bg, bd = coefs(0)
    for h in range(2):
        for f, i, sign in ((0, 0, bg), (1, 3, -bg)):
            rows = pl.ds(base + 32 * h + i, 8, stride=4)
            outer = outside_ref[f, pl.ds(face + 8 * h, 8), cols]
            state_ref[g, rows, :] += edge(tile_ref[g, rows, :], outer, sign, bd)
    tiles = [tile_ref[g, pl.ds(base + 8 * t, 8), :] for t in range(8)]
    total = [state_ref[g, pl.ds(base + 8 * t, 8), :] for t in range(8)]
    bg, bd = coefs(2)
    for h in range(2):
        for f, k, sign in ((4, 0, bg), (5, 3, -bg)):
            outer = outside_ref[f, pl.ds(face + 8 * h, 8), cols]
            total[2 * k + h] += edge(tiles[2 * k + h], outer, sign, bd)
    bg, bd = coefs(1)
    bgs = jnp.where(low, bg, -bg)
    outer_l = [outside_ref[2, pl.ds(face + 8 * h, 8), cols] for h in range(2)]
    outer_r = [outside_ref[3, pl.ds(face + 8 * h, 8), cols] for h in range(2)]
    for k in range(4):
        ol = outer_l[k // 2]
        orr = outer_r[k // 2]
        outer = jnp.where(low, ol, turn(orr)) if k % 2 == 0 else jnp.where(low, turn(ol), orr)
        bound = edge(jnp.where(low, tiles[2 * k], tiles[2 * k + 1]), outer, bgs, bd)
        total[2 * k] += jnp.where(low, bound, 0.0)
        total[2 * k + 1] += jnp.where(low, 0.0, bound)
    for t in range(4):
        high, rest = split2(jnp.concatenate(total[2 * t : 2 * t + 2], axis=0))
        up_ref[pl.ds(pl.multiple_of(base + 16 * t, 16), 16), cols] = high
        up_ref[pl.ds(pl.multiple_of(ROWS + base + 16 * t, 16), 16), cols] = rest


def refine_tables(flag_ref, jac_ref, start_ref, aux_ref):
    flags = flag_ref[...].astype(F32)
    wide = jnp.broadcast_to(flags, (LANES, E_DEV)).astype(BF16)
    row = lax.broadcasted_iota(jnp.int32, (E_DEV, E_DEV), 0)
    col = lax.broadcasted_iota(jnp.int32, (E_DEV, E_DEV), 1)
    ahead = jnp.where(col < row, 1.0, 0.0).astype(BF16)
    within = jnp.where(col <= row, 1.0, 0.0).astype(BF16)
    dims = (((1,), (1,)), ((), ()))
    place = lax.broadcasted_iota(jnp.int32, (E_DEV, LANES), 0).astype(F32)
    start_ref[0] = place + 7.0 * lax.dot_general(ahead, wide, dims, preferred_element_type=F32)
    start_ref[1] = (
        place + 1.0 + 7.0 * lax.dot_general(within, wide, dims, preferred_element_type=F32)
    )
    count = lax.dot_general(wide[0:16], ahead, dims, preferred_element_type=F32)[0:1]
    at = lax.broadcasted_iota(jnp.int32, (1, E_DEV), 1).astype(F32) + 7.0 * count
    at_high = jnp.floor(at * (1.0 / 16.0))
    jac = jac_ref[...]
    j0, rest = split2(jac)
    rest = jac - j0.astype(F32)
    j1 = rest.astype(BF16)
    j2 = (rest - j1.astype(F32)).astype(BF16)
    zero = jnp.zeros((10, E_DEV), F32)
    aux_ref[...] = jnp.concatenate(
        [
            at_high, at - 16.0 * at_high, flags, j0.astype(F32), j1.astype(F32), j2.astype(F32),
            zero,
        ],
        axis=0,
    ).astype(BF16)


def column_tables(tile, first, start_ref, aux_ref, coef_ref, hot_ref):
    place = lax.broadcasted_iota(jnp.int32, (1, LANES), 1).astype(F32) + first
    inside = (place >= start_ref[0]) & (place < start_ref[1])
    hot = jnp.where(inside, 1.0, 0.0).astype(BF16)
    cols = pl.ds(pl.multiple_of((tile % 2) * LANES, LANES), LANES)
    hot_ref[tile // 2, :, cols] = hot
    aux = jnp.dot(aux_ref[...], hot, preferred_element_type=F32)
    child = place - (16.0 * aux[0:1] + aux[1:2])
    refined = aux[2:3] > 0.5
    z = child >= 4.0
    child = child - jnp.where(z, 4.0, 0.0)
    y = child >= 2.0
    child = child - jnp.where(y, 2.0, 0.0)
    x = child >= 1.0
    jac = (aux[3:4] + aux[4:5] + aux[5:6]) * jnp.where(refined, 2.0, 1.0)

    def table(bit):
        return [
            [
                rows8(
                    jnp.where(
                        refined,
                        jnp.where(bit, float(SIDES[1][i, m]), float(SIDES[0][i, m])),
                        1.0 if i == m else 0.0,
                    )
                )
                for m in range(4)
            ]
            for i in range(4)
        ]

    cx, cy, cz = table(x), table(y), table(z)
    low = low_half((8, LANES))
    n = 0
    for i in range(4):
        for m in range(4):
            coef_ref[tile, n] = cx[i][m]
            coef_ref[tile, 16 + n] = cz[i][m]
            n += 1
    order = [(0, 1), (1, 0), (2, 3), (3, 2)]
    for at, (first_j, last_j) in enumerate(((0, 1), (2, 3))):
        for k, (lo_m, hi_m) in enumerate(order):
            coef_ref[tile, 32 + 4 * at + k] = jnp.where(low, cy[first_j][lo_m], cy[last_j][hi_m])
    return jac


def combine4(c, u):
    return (c[0] * u[0] + c[1] * u[1]) + (c[2] * u[2] + c[3] * u[3])


def interpolate(v, tile, half, pick_ref, coef_ref, line_ref, put):
    base = 64 * v
    cols = slice(half * LANES, half * LANES + LANES)
    tiles = [
        pick_ref[base + 8 * t : base + 8 * t + 8, cols]
        + pick_ref[ROWS + base + 8 * t : ROWS + base + 8 * t + 8, cols]
        for t in range(8)
    ]
    mid = [None] * 8
    for h in range(2):
        u = [tiles[2 * k + h] for k in range(4)]
        for k in range(4):
            mid[2 * k + h] = combine4([coef_ref[tile, 16 + 4 * k + m] for m in range(4)], u)
    for k in range(4):
        a, b = mid[2 * k], mid[2 * k + 1]
        u = [a, turn(a), b, turn(b)]
        for at in range(2):
            line_ref[v, 16 * k + 8 * at : 16 * k + 8 * at + 8, :] = combine4(
                [coef_ref[tile, 32 + 4 * at + m] for m in range(4)], u
            )
    for h in range(2):
        u = [line_ref[v, pl.ds(32 * h + i, 8, stride=4), :] for i in range(4)]
        for i in range(4):
            put(base + 32 * h + i, combine4([coef_ref[tile, 4 * i + m] for m in range(4)], u))


TILES = 13
FRAME = ROWS + 8
PACKED = ROWS // 4 * 3 + 8


def pack(frame_ref, tile, pack_ref, part):
    lane = lax.broadcasted_iota(jnp.int32, (8, LANES), 1)
    unused = jnp.where(part == 1, lane, LANES - 1 - lane) < 32
    for n in range(ROWS // 32):
        fourth = frame_ref[tile, 32 * n + 24 : 32 * n + 32, :]
        for j in range(3):
            rows = frame_ref[tile, 32 * n + 8 * j : 32 * n + 8 * j + 8, :]
            pack_ref[part, 24 * n + 8 * j : 24 * n + 8 * j + 8, :] = jnp.where(
                unused, pltpu.roll(fourth, 96 - 32 * j, 1), rows
            )
    pack_ref[part, PACKED - 8 : PACKED, :] = frame_ref[tile, ROWS:FRAME, :]


def unpack(land_ref, part, dst_ref, tile):
    lane = lax.broadcasted_iota(jnp.int32, (8, LANES), 1)
    for n in range(ROWS // 32):
        rows = [land_ref[part, 24 * n + 8 * j : 24 * n + 8 * j + 8, :] for j in range(3)]
        turned = [pltpu.roll(rows[j], 32 + 32 * j, 1) for j in range(3)]
        for j in range(3):
            dst_ref[tile, 32 * n + 8 * j : 32 * n + 8 * j + 8, :] = rows[j]
        dst_ref[tile, 32 * n + 24 : 32 * n + 32, :] = jnp.where(
            lane < 32 + 32 * part, turned[0],
            jnp.where(lane < 64 + 32 * part, turned[1], turned[2]),
        )
    dst_ref[tile, ROWS:FRAME, :] = land_ref[part, PACKED - 8 : PACKED, :]


def kernel(
    x_hbm, jac_hbm, speed_hbm, flag_hbm, send_hbm, source_hbm, modes_hbm,
    frame_ref, head_ref, info_ref,
    jac_ref, speed_ref, flag_ref, send_ref, source_ref, modes_ref,
    tile_ref, trace_ref, out_buf, ghost_ref, ghost_bf, outside_ref, rate_ref, state_ref, up_ref,
    start_ref, aux_ref, coef_ref, hot_ref, pick_a, pick_b, line_ref, far_ref, pack_ref, land_ref,
    row_buf, z_buf, y_buf, mine, row_sum, plane_sum, behind_ref,
    small_sems, fetch_sems, send_sems, recv_sems, row_send, row_recv, z_send, z_recv,
    y_send, y_recv,
    head_send, head_recv, tail_send, tail_recv, reply,
):
    me = lax.axis_index("curve")
    devices = ROW_OF * SIDE * SIDE
    row_at = me % ROW_OF
    z_at = me // ROW_OF % SIDE
    y_at = me // (ROW_OF * SIDE)
    near = [(me + devices + o) % devices for o in (-2, -1, 1, 2)]
    row_mates = [me - row_at + (row_at + k) % ROW_OF for k in range(1, ROW_OF)]
    z_mates = [me + ROW_OF * ((z_at + k) % SIDE - z_at) for k in range(1, SIDE)]
    early = me % (ROW_OF * SIDE) < 2
    awaited = me >= devices - 4
    barrier = pltpu.get_barrier_semaphore()
    for b, partner in enumerate(near):

        @pl.when(me + (-2, -1, 1, 2)[b] < devices)
        def _(partner=partner):
            pl.semaphore_signal(barrier, inc=1, device_id=(partner,), device_id_type=MESH)

    fetches = fetch_state(x_hbm, tile_ref, fetch_sems)
    for partner in row_mates + z_mates:
        pl.semaphore_signal(barrier, inc=1, device_id=(partner,), device_id_type=MESH)
    for k in range(1, SIDE):

        @pl.when(y_at >= k)
        def _(k=k):
            pl.semaphore_signal(
                barrier, inc=1, device_id=(me - k * ROW_OF * SIDE,), device_id_type=MESH
            )

    small = []
    for at, (src, dst) in enumerate(
        (
            (send_hbm, send_ref), (flag_hbm, flag_ref), (source_hbm, source_ref),
            (jac_hbm, jac_ref), (modes_hbm, modes_ref), (speed_hbm, speed_ref),
        )
    ):
        copy = pltpu.make_async_copy(src, dst, small_sems.at[at])
        copy.start()
        small.append(copy)

    def send(src, dst, send_sem, recv_sem, mate):
        copy = remote(src, dst, send_sem, recv_sem, mate)
        copy.start()
        return copy

    def remote(src, dst, send_sem, recv_sem, mate):
        return pltpu.make_async_remote_copy(
            src_ref=src, dst_ref=dst, send_sem=send_sem, recv_sem=recv_sem,
            device_id=(mate,), device_id_type=MESH,
        )

    for g in range(GROUPS):
        fetches[g].wait()
        build_traces(tile_ref, trace_ref, g)
    small[0].wait()
    gather_sends(send_ref, trace_ref, out_buf)
    for copy in small[1:]:
        copy.wait()
    count = jnp.sum(flag_ref[...].astype(F32), axis=1, keepdims=True)
    mine[...] = jnp.broadcast_to(count, (1, LANES)).astype(jnp.int32) - 64
    total_new = 7.0 * jnp.broadcast_to(count, (1, LANES)) + float(E_DEV)

    def near_work():
        outside_near(source_ref, trace_ref, far_ref, outside_ref)
        blend_rates(tile_ref, modes_ref, jac_ref, rate_ref)

    def table_step(tile, carry):
        shift = (jnp.full((1, LANES), tile, jnp.int32) * LANES).astype(F32)
        first = shift - 2.0 * LANES + jnp.where(tile < 2, total_new, 0.0)
        jac_row = rows8(column_tables(tile, first, start_ref, aux_ref, coef_ref, hot_ref))
        frame_ref[jnp.where(tile < 2, TILES + tile, tile), ROWS:FRAME, :] = jac_row
        return carry

    def inner_work():
        def interior_step(n, carry):
            interior_block(n // GROUPS, n % GROUPS, tile_ref, speed_ref, rate_ref, state_ref)
            return carry

        lax.fori_loop(0, VARS * GROUPS, interior_step, 0)
        refine_tables(flag_ref, jac_ref, start_ref, aux_ref)
        lax.fori_loop(0, 4, table_step, 0)

    def own_tables():
        lax.fori_loop(4, TILES, table_step, 0)

    pl.when(jnp.logical_not(awaited))(near_work)
    pl.when(early)(inner_work)
    pl.semaphore_wait(
        barrier, 4 - jnp.maximum(2 - me, 0) + ROW_OF - 1 + SIDE - 1 + SIDE - 1 - y_at
    )
    for b in (2, 3):

        @pl.when(me + b - 1 >= devices)
        def _(b=b):
            pl.semaphore_signal(reply, inc=1, device_id=(near[b],), device_id_type=MESH)

    halo = {
        b: remote(
            out_buf.at[b], ghost_ref.at[3 - b], send_sems.at[b], recv_sems.at[3 - b], near[b]
        )
        for b in (1, 3, 0, 2)
    }
    for b in (1, 3, 0, 2):
        pl.when(me >= 2 - b)(halo[b].start)
    row_copies = [
        send(mine, row_buf.at[k], row_send.at[k], row_recv.at[k], mate)
        for k, mate in enumerate(row_mates)
    ]
    pl.when(awaited)(near_work)
    pl.when(jnp.logical_not(early))(inner_work)
    pl.when(early)(own_tables)

    @pl.when(me < 2)
    def _():
        pl.semaphore_wait(reply, 2 - me)
        for b in range(2):
            pl.when(me < 2 - b)(halo[b].start)

    def gathered(copies, own_ref, buf_ref, at, sum_ref):
        for copy in copies:
            copy.wait()
        total = own_ref[...]
        behind = behind_ref[...]
        for k in range(len(copies)):
            value = buf_ref[k]
            total = total + value
            behind = behind + jnp.where(at >= k + 1, value, 0)
        sum_ref[...] = total
        behind_ref[...] = behind

    behind_ref[...] = jnp.zeros((1, LANES), jnp.int32)
    z_copies = [
        remote(row_sum, z_buf.at[k], z_send.at[k], z_recv.at[k], mate)
        for k, mate in enumerate(z_mates)
    ]
    y_copies = [
        remote(
            plane_sum, y_buf.at[k - 1], y_send.at[k - 1], y_recv.at[k - 1],
            (me + k * ROW_OF * SIDE) % devices,
        )
        for k in range(1, SIDE)
    ]

    def row_stage():
        gathered(row_copies, mine, row_buf, row_at, row_sum)
        for copy in z_copies:
            copy.start()

    row_stage()
    for b in range(4):
        halo[b].wait_send()
        halo[3 - b].wait_recv()
    split_ghost(ghost_ref, ghost_bf)
    first, last = me == 0, me == devices - 1

    outer_tail = remote(
        frame_ref.at[TILES + 1], frame_ref.at[1], tail_send.at[1], tail_recv.at[1], near[2]
    )
    outer_head = remote(
        frame_ref.at[2], head_ref.at[0], head_send.at[0], head_recv.at[0], near[1]
    )
    inner_tail = remote(
        pack_ref.at[1], land_ref.at[1], tail_send.at[0], tail_recv.at[0], near[2]
    )
    inner_head = remote(
        pack_ref.at[0], land_ref.at[0], head_send.at[1], head_recv.at[1], near[1]
    )

    def fill(dst, tile, half, pick_ref):
        for v in range(VARS):

            def put(row, value):
                frame_ref[dst, pl.ds(row, 8, stride=4), :] = value

            interpolate(v, tile, half, pick_ref, coef_ref, line_ref, put)

    for order in range(2):
        part = me % 2 if order == 0 else 1 - me % 2
        outside_far(part, far_ref, ghost_bf, outside_ref)

        for step in range(2):
            half = jnp.where(part == 1, 1 - step, step)
            group = 2 * part + half

            def edge_step(v, carry, group=group):
                edge_block(
                    v, group, tile_ref, speed_ref, rate_ref, outside_ref, state_ref, up_ref
                )
                return carry

            lax.fori_loop(0, VARS, edge_step, 0)
            within = (
                pl.ds(pl.multiple_of(LANES * group, LANES), LANES)
                if step == 0
                else pl.ds(pl.multiple_of(2 * LANES * part, 2 * LANES), 2 * LANES)
            )
            cols = pl.ds(pl.multiple_of(LANES * half, LANES), LANES)
            pick_a[:, 0:LANES] = jnp.dot(
                up_ref[:, within], hot_ref[1 - part, within, cols], preferred_element_type=F32
            )
            fill(jnp.where(part == 1, TILES, 2) + half, 2 * (1 - part) + half, 0, pick_a)
            if step == 0:
                pl.when((part == 1) & jnp.logical_not(last))(outer_tail.start)
                pl.when((part == 0) & jnp.logical_not(first))(outer_head.start)
            else:
                pack(frame_ref, jnp.where(part == 1, TILES, 3), pack_ref, part)
                pl.when((part == 1) & jnp.logical_not(last))(inner_tail.start)
                pl.when((part == 0) & jnp.logical_not(first))(inner_head.start)

    pl.when(jnp.logical_not(early))(own_tables)
    gathered(z_copies, row_sum, z_buf, z_at, plane_sum)
    for k in range(1, SIDE):
        pl.when(y_at + k < SIDE)(y_copies[k - 1].start)

    picks = [pick_a, pick_b]
    pick_a[...] = jnp.dot(up_ref[...], hot_ref[2], preferred_element_type=F32)
    for pair in range(2, 7):
        now, later = picks[pair % 2], picks[(pair + 1) % 2]
        if pair < 5:
            later[...] = jnp.dot(up_ref[...], hot_ref[pair + 1], preferred_element_type=F32)
        if pair == 5:
            later[:, 0:LANES] = jnp.dot(
                up_ref[...], hot_ref[6, :, 0:LANES], preferred_element_type=F32
            )
        for half in range(2 if pair < 6 else 1):
            fill(2 * pair + half, 2 * pair + half, half, now)

    behind = behind_ref[...]
    for k in range(1, SIDE):
        pl.when(y_at + k < SIDE)(y_copies[k - 1].wait_send)
        pl.when(y_at >= k)(y_copies[k - 1].wait_recv)
        behind = behind + jnp.where(y_at >= k, y_buf[k - 1], 0)
    info_ref[0:1, :] = behind
    info_ref[1:2, :] = total_new.astype(jnp.int32)

    @pl.when(jnp.logical_not(last))
    def _():
        outer_tail.wait_send()
        inner_tail.wait_send()
        outer_head.wait_recv()
        inner_head.wait_recv()
        unpack(land_ref, 0, head_ref, 1)

    @pl.when(jnp.logical_not(first))
    def _():
        outer_head.wait_send()
        inner_head.wait_send()
        outer_tail.wait_recv()
        inner_tail.wait_recv()
        unpack(land_ref, 1, frame_ref, 0)


CHUNK = 64


def place_kernel(frame_ref, head_ref, info_ref, out_hbm, jac_hbm, out_ref, jac_ref, sems):
    shift = 7 * info_ref[0, 0]
    size = info_ref[1, 0]
    begin = 2 * LANES - shift
    tile = begin // LANES
    turn_by = begin - tile * LANES
    over = -(size + shift)
    head_tile = over // LANES
    head_turn = over - head_tile * LANES
    lane = lax.broadcasted_iota(jnp.int32, (8, LANES), 1)
    kept = lane < LANES - turn_by
    head_kept = lane < LANES - head_turn
    back = (LANES - turn_by) % LANES
    head_back = (LANES - head_turn) % LANES

    def row_tile(rows):
        parts = [pltpu.roll(frame_ref[tile + c, rows, :], back, 1) for c in range(9)]
        out = [jnp.where(kept, parts[c], parts[c + 1]) for c in range(8)]
        heads = [pltpu.roll(head_ref[c, rows, :], head_back, 1) for c in range(2)]
        ends = [
            jnp.where(head_tile + 5 + c == 0, heads[0], jnp.where(head_tile + 5 + c == 1, heads[1], 0.0))
            for c in range(4)
        ]
        for c in range(3):
            out[5 + c] = out[5 + c] + jnp.where(head_kept, ends[c], ends[c + 1])
        return out

    copies = []
    for chunk in range(ROWS // CHUNK):
        for n in range(CHUNK // 8):
            row = chunk * CHUNK + 8 * n
            out = row_tile(pl.ds(row, 8))
            for c in range(7):
                out_ref[row : row + 8, c * LANES : (c + 1) * LANES] = out[c]
            out_ref[row : row + 8, 7 * LANES : E_NEW] = out[7][:, : E_NEW - 7 * LANES]
        rows = pl.ds(chunk * CHUNK, CHUNK)
        copy = pltpu.make_async_copy(out_ref.at[rows], out_hbm.at[rows], sems.at[chunk])
        copy.start()
        copies.append(copy)
    out = row_tile(pl.ds(ROWS, 8))
    for c in range(8):
        width = min(LANES, E_NEW - c * LANES)
        jac_ref[0:1, c * LANES : c * LANES + width] = out[c][0:1, :width]
    copies.append(pltpu.make_async_copy(jac_ref, jac_hbm, sems.at[ROWS // CHUNK]))
    copies[-1].start()
    for copy in copies:
        copy.wait()


def vmem(count):
    return [pl.BlockSpec(memory_space=pltpu.VMEM)] * count


def shards(nodal_state, inverse_jacobian, speeds, refine_flags, send_index, face_source):
    x = nodal_state.reshape(ROWS, E_DEV)
    jac = inverse_jacobian.reshape(1, E_DEV)
    flags = refine_flags.reshape(1, E_DEV)
    dma = pltpu.SemaphoreType.DMA
    frame, head, info = pl.pallas_call(
        kernel,
        out_shape=(
            jax.ShapeDtypeStruct((TILES + 2, FRAME, LANES), F32),
            jax.ShapeDtypeStruct((2, FRAME, LANES), F32),
            jax.ShapeDtypeStruct((2, LANES), jnp.int32),
        ),
        in_specs=[pl.BlockSpec(memory_space=pltpu.HBM)] * 7,
        out_specs=tuple(vmem(3)),
        scratch_shapes=[
            pltpu.VMEM((1, E_DEV), F32),
            pltpu.SMEM((3, VARS), F32),
            pltpu.VMEM((1, E_DEV), jnp.int32),
            pltpu.VMEM((4 * SLOTS,), jnp.int32),
            pltpu.VMEM((6, E_DEV), jnp.int32),
            pltpu.VMEM((64, 64), F32),
            pltpu.VMEM((GROUPS, ROWS, LANES), F32),
            pltpu.VMEM((6, 160, E_DEV), BF16),
            pltpu.VMEM((4, 80, LANES), F32),
            pltpu.VMEM((4, 80, LANES), F32),
            pltpu.VMEM((160, E_DEV), BF16),
            pltpu.VMEM((6, 80, E_DEV), F32),
            pltpu.VMEM((8, E_DEV), F32),
            pltpu.VMEM((GROUPS, ROWS, LANES), F32),
            pltpu.VMEM((2 * ROWS, E_DEV), BF16),
            pltpu.VMEM((2, E_DEV, LANES), F32),
            pltpu.VMEM((16, E_DEV), BF16),
            pltpu.VMEM((TILES, 40, 8, LANES), F32),
            pltpu.VMEM((7, E_DEV, 2 * LANES), BF16),
            pltpu.VMEM((2 * ROWS, 2 * LANES), F32),
            pltpu.VMEM((2 * ROWS, 2 * LANES), F32),
            pltpu.VMEM((VARS, 64, LANES), F32),
            pltpu.VMEM((6, E_DEV, E_DEV), BF16),
            pltpu.VMEM((2, PACKED, LANES), F32),
            pltpu.VMEM((2, PACKED, LANES), F32),
            pltpu.VMEM((ROW_OF - 1, 1, LANES), jnp.int32),
            pltpu.VMEM((SIDE - 1, 1, LANES), jnp.int32),
            pltpu.VMEM((SIDE - 1, 1, LANES), jnp.int32),
            pltpu.VMEM((1, LANES), jnp.int32),
            pltpu.VMEM((1, LANES), jnp.int32),
            pltpu.VMEM((1, LANES), jnp.int32),
            pltpu.VMEM((1, LANES), jnp.int32),
            dma((6,)), dma((GROUPS,)), dma((4,)), dma((4,)), dma((ROW_OF - 1,)),
            dma((ROW_OF - 1,)), dma((SIDE - 1,)), dma((SIDE - 1,)), dma((SIDE - 1,)),
            dma((SIDE - 1,)),
            dma((2,)), dma((2,)), dma((2,)), dma((2,)), pltpu.SemaphoreType.REGULAR,
        ],
        compiler_params=pltpu.CompilerParams(
            collective_id=0, has_side_effects=True, vmem_limit_bytes=28 << 20
        ),
        name="step",
    )(*[
        pltpu.with_memory_space_constraint(a, pltpu.HBM)
        for a in (x, jac, speeds, flags, send_index, face_source, jnp.asarray(MODES, F32))
    ])
    out, out_jac = pl.pallas_call(
        place_kernel,
        out_shape=(
            jax.ShapeDtypeStruct((ROWS, E_NEW), F32),
            jax.ShapeDtypeStruct((1, E_NEW), F32),
        ),
        in_specs=vmem(3),
        out_specs=(
            pl.BlockSpec(memory_space=pltpu.HBM), pl.BlockSpec(memory_space=pltpu.HBM)
        ),
        scratch_shapes=[
            pltpu.VMEM((ROWS, E_NEW), F32), pltpu.VMEM((1, E_NEW), F32), dma((ROWS // CHUNK + 1,))
        ],
        compiler_params=pltpu.CompilerParams(vmem_limit_bytes=16 << 20),
        name="place",
    )(frame, head, info)
    return out.reshape(VARS, 64, E_NEW), out_jac.reshape(E_NEW)


def solution(mesh):
    axis = P("curve")
    wide = P(None, None, "curve")
    return jax.shard_map(
        shards,
        mesh=mesh,
        in_specs=(wide, axis, P(), axis, axis, P(None, "curve")),
        out_specs=(wide, axis),
        check_vma=False,
    )
```

```python
import functools
import math

import jax
import jax.numpy as jnp
import numpy as np
from jax import lax
from jax.experimental import pallas as pl
from jax.experimental.pallas import tpu as pltpu
from jax.sharding import PartitionSpec as P

TIME_STEP = 0.02
VARS = 5
E_DEV = 512
E_NEW = 960
SLOTS = 96
ROWS = 64 * VARS
LANES = 128
GROUPS = E_DEV // LANES
ROW_OF = 8
SIDE = 4
F32 = jnp.float32
BF16 = jnp.bfloat16
MESH = pl.DeviceIdType.MESH


def lagrange_at(points, targets):
    values_at = np.ones((len(targets), 4))
    for basis_id in range(4):
        for partner in range(4):
            if partner != basis_id:
                values_at[:, basis_id] *= (targets - points[partner]) / (
                    points[basis_id] - points[partner]
                )
    return values_at


def tables():
    root = 1.0 / math.sqrt(5.0)
    points = np.array([-1.0, -root, root, 1.0])
    weights = np.array([1.0, 5.0, 5.0, 1.0]) / 6.0
    bary = np.ones(4)
    for a in range(4):
        for b in range(4):
            if a != b:
                bary[a] /= points[a] - points[b]
    deriv = np.zeros((4, 4))
    for a in range(4):
        for b in range(4):
            if a != b:
                deriv[a, b] = bary[b] / bary[a] / (points[a] - points[b])
        deriv[a, a] = -np.sum(deriv[a])
    skew = weights[:, None] * deriv
    legendre = np.stack(
        [points**0, points, 0.5 * (3 * points**2 - 1), 0.5 * (5 * points**3 - 3 * points)], axis=1
    )
    to_modes = np.linalg.inv(legendre)
    sides = [lagrange_at(points, (points - 1.0) / 2.0), lagrange_at(points, (points + 1.0) / 2.0)]
    return skew, np.kron(to_modes, np.kron(to_modes, to_modes)), sides


SKEW, MODES, SIDES = tables()
Q01, Q02, Q03, Q12 = (float(SKEW[0, 1]), float(SKEW[0, 2]), float(SKEW[0, 3]), float(SKEW[1, 2]))
END, MID = 6.0, 1.2


def split2(x):
    high = x.astype(BF16)
    return high, (x - high.astype(F32)).astype(BF16)


def low_half(shape):
    return (lax.broadcasted_iota(jnp.int32, shape, 0) & 7) < 4


def turn(x):
    return pltpu.roll(x, 4, 0)


def fetch_state(x_ref, tile_ref, sems):
    copies = []
    for g in range(GROUPS):
        copy = pltpu.make_async_copy(
            x_ref.at[:, g * LANES : (g + 1) * LANES], tile_ref.at[g], sems.at[g]
        )
        copy.start()
        copies.append(copy)
    return copies


def build_traces(tile_ref, trace_ref, g):
    low = low_half((8, LANES))
    cols = slice(g * LANES, (g + 1) * LANES)
    for v in range(VARS):
        base = 64 * v
        tiles = [tile_ref[g, base + 8 * t : base + 8 * t + 8, :] for t in range(8)]
        first, last = tiles[0::2], tiles[1::2]
        sets = {
            0: [tile_ref[g, pl.ds(base + 32 * h, 8, stride=4), :] for h in range(2)],
            1: [tile_ref[g, pl.ds(base + 32 * h + 3, 8, stride=4), :] for h in range(2)],
            2: [jnp.where(low, first[k], turn(first[k + 1])) for k in (0, 2)],
            3: [jnp.where(low, turn(last[k]), last[k + 1]) for k in (0, 2)],
            4: tiles[0:2],
            5: tiles[6:8],
        }
        for f, rows in sets.items():
            high, rest = split2(jnp.concatenate(rows, axis=0))
            trace_ref[f, 16 * v : 16 * v + 16, cols] = high
            trace_ref[f, 80 + 16 * v : 96 + 16 * v, cols] = rest


def one_hot(index, size, width):
    rows = lax.broadcasted_iota(jnp.int32, (size, width), 0).astype(jnp.int16)
    index = jnp.broadcast_to(index, (16, width)).astype(jnp.int16)
    index = jnp.concatenate([index] * (size // 16), axis=0)
    return jnp.where(
        rows == index, jnp.ones((size, width), BF16), jnp.zeros((size, width), BF16)
    )


def gather_sends(send_ref, trace_ref, out_ref):
    packed = jnp.broadcast_to(send_ref[...].reshape(1, 4 * SLOTS), (8, 4 * SLOTS))
    for pair in range(2):
        moved = [
            packed if block == 0 else pltpu.roll(packed, 4 * SLOTS - SLOTS * block, 1)
            for block in (2 * pair, 2 * pair + 1)
        ]
        index = jnp.concatenate([m[0:1, 0:LANES] for m in moved], axis=1)
        total = jnp.zeros((160, 2 * LANES), F32)
        for f in range(6):
            total = total + jnp.dot(
                trace_ref[f],
                one_hot(index - f * E_DEV, E_DEV, 2 * LANES),
                preferred_element_type=F32,
            )
        total = total[0:80] + total[80:160]
        for half in range(2):
            out_ref[2 * pair + half] = total[:, half * LANES : (half + 1) * LANES]


def pair_sum(ui, um, si, sm):
    return (si + sm) + ui * um


def line_update(u, coef):
    ca, cb, c02, c03, cd = coef
    s = [x * x for x in u]
    m = [jnp.abs(x) for x in u]
    e = []
    for n, c in ((0, ca), (1, cb), (2, ca)):
        g = pair_sum(u[n], u[n + 1], s[n], s[n + 1])
        e.append(c * g - cd * (jnp.maximum(m[n], m[n + 1]) * (u[n + 1] - u[n])))
    r02 = c02 * pair_sum(u[0], u[2], s[0], s[2])
    r13 = c02 * pair_sum(u[1], u[3], s[1], s[3])
    r03 = c03 * pair_sum(u[0], u[3], s[0], s[3])
    t0 = -(e[0] + r02 + r03)
    t1 = e[0] - e[1] - r13
    t2 = e[1] - e[2] + r02
    t3 = e[2] + r13 + r03
    return t0, t1, t2, t3


def edge(u, o, cg, cd):
    g = pair_sum(u, o, u * u, o * o)
    return cg * g - cd * (jnp.maximum(jnp.abs(u), jnp.abs(o)) * (u - o))


def rows8(x):
    return jnp.broadcast_to(x, (8, LANES))


def blend_rates(tile_ref, modes_ref, jac_ref, rate_ref):
    n = lax.broadcasted_iota(jnp.int32, (64, LANES), 0)
    top = ((n & 3) == 3) | ((n & 12) == 12) | (n >= 48)
    for g in range(GROUPS):
        cols = slice(g * LANES, (g + 1) * LANES)
        modal = jnp.dot(
            modes_ref[...], tile_ref[g, 0:64, :], precision=lax.Precision.HIGHEST,
            preferred_element_type=F32,
        )
        energy = modal * modal
        high = jnp.sum(jnp.where(top, energy, 0.0), axis=0, keepdims=True)
        full = jnp.sum(energy, axis=0, keepdims=True)
        ratio = high / (full + 1e-06)
        blend = 0.5 * ratio / (ratio + 0.1)
        step = TIME_STEP * jac_ref[0:1, cols]
        rate_ref[0:1, cols] = step * (1.0 - blend)
        rate_ref[1:2, cols] = step * blend
        rate_ref[2:3, cols] = step


def outside_near(source_ref, trace_ref, far_ref, outside_ref):
    for f in range(6):
        index = source_ref[f : f + 1, :]
        total = jnp.dot(
            trace_ref[f ^ 1],
            one_hot(index - (f ^ 1) * E_DEV, E_DEV, E_DEV),
            preferred_element_type=F32,
        )
        outside_ref[f] = total[0:80] + total[80:160]
        far = index - 6 * E_DEV
        slot = (
            (far >= SLOTS).astype(jnp.int32)
            + (far >= 2 * SLOTS).astype(jnp.int32)
            + (far >= 3 * SLOTS).astype(jnp.int32)
        )
        hot = one_hot(jnp.where(far >= 0, far + (LANES - SLOTS) * slot, -1), E_DEV, E_DEV)
        for g in range(GROUPS):
            far_ref[g, :, f * LANES : (f + 1) * LANES] = hot[:, g * LANES : (g + 1) * LANES]


def split_ghost(ghost_ref, ghost_bf):
    for slot in range(4):
        high, rest = split2(ghost_ref[slot])
        ghost_bf[0:80, slot * LANES : (slot + 1) * LANES] = high
        ghost_bf[80:160, slot * LANES : (slot + 1) * LANES] = rest


def outside_far(group, far_ref, ghost_bf, outside_ref):
    cols = pl.ds(pl.multiple_of(LANES * group, LANES), LANES)
    total = jnp.dot(ghost_bf[...], far_ref[group], preferred_element_type=F32)
    for f in range(6):
        part = slice(f * LANES, (f + 1) * LANES)
        outside_ref[f, :, cols] += total[0:80, part] + total[80:160, part]


def coefs_of(d, v, speed_ref, hi, lo):
    a = speed_ref[d, v]
    third = (a / 3.0) * hi
    sixth = (a / 6.0) * lo
    return [
        rows8(c)
        for c in (
            Q01 * third + sixth, Q12 * third + sixth, Q02 * third, Q03 * third,
            (0.5 * jnp.abs(a)) * lo,
        )
    ]


def interior_block(v, g, tile_ref, speed_ref, rate_ref, state_ref):
    base = pl.multiple_of(64 * v, 64)
    cols = pl.ds(pl.multiple_of(g * LANES, LANES), LANES)
    hi = rate_ref[0:1, cols]
    lo = rate_ref[1:2, cols]
    low = low_half((8, LANES))
    coef = coefs_of(0, v, speed_ref, hi, lo)
    for h in range(2):
        u = [tile_ref[g, pl.ds(base + 32 * h + i, 8, stride=4), :] for i in range(4)]
        t = line_update(u, coef)
        for i, w in enumerate((END, MID, MID, END)):
            state_ref[g, pl.ds(base + 32 * h + i, 8, stride=4), :] = u[i] + w * t[i]
    tiles = [tile_ref[g, pl.ds(base + 8 * t, 8), :] for t in range(8)]
    coef = coefs_of(2, v, speed_ref, hi, lo)
    total = [None] * 8
    for h in range(2):
        t = line_update([tiles[2 * k + h] for k in range(4)], coef)
        for k, w in enumerate((END, MID, MID, END)):
            total[2 * k + h] = w * t[k]
    ca, cb, c02, c03, cd = coefs_of(1, v, speed_ref, hi, lo)
    signed = jnp.where(low, -ca, ca)
    cross = jnp.where(low, -c03, -cb)
    cross_d = jnp.where(low, 0.0, cd)
    wa = jnp.where(low, END, MID)
    wb = jnp.where(low, MID, END)
    for k in range(4):
        a, b = tiles[2 * k], tiles[2 * k + 1]
        at, bt = turn(a), turn(b)
        sa, sb, sat, sbt = a * a, b * b, at * at, bt * bt
        ma, mb, mat, mbt = jnp.abs(a), jnp.abs(b), jnp.abs(at), jnp.abs(bt)
        x1 = signed * pair_sum(a, at, sa, sat) + cd * (jnp.maximum(ma, mat) * (at - a))
        x2 = signed * pair_sum(b, bt, sb, sbt) + cd * (jnp.maximum(mb, mbt) * (bt - b))
        x3 = c02 * pair_sum(a, b, sa, sb)
        x4 = cross * pair_sum(a, bt, sa, sbt) + cross_d * (jnp.maximum(ma, mbt) * (bt - a))
        total[2 * k] += wa * (x1 - x3 + x4)
        total[2 * k + 1] += wb * (x2 + x3 - turn(x4))
    for t in range(8):
        state_ref[g, pl.ds(base + 8 * t, 8), :] += total[t]


def edge_block(v, g, tile_ref, speed_ref, rate_ref, outside_ref, state_ref, up_ref):
    base = 64 * v
    face = 16 * v
    cols = pl.ds(pl.multiple_of(g * LANES, LANES), LANES)
    step = rate_ref[2:3, cols]
    low = low_half((8, LANES))

    def coefs(d):
        a = speed_ref[d, v]
        return rows8((a * (END / 6.0)) * step), rows8((0.5 * END) * jnp.abs(a) * step)

    bg, bd = coefs(0)
    for h in range(2):
        for f, i, sign in ((0, 0, bg), (1, 3, -bg)):
            rows = pl.ds(base + 32 * h + i, 8, stride=4)
            outer = outside_ref[f, pl.ds(face + 8 * h, 8), cols]
            state_ref[g, rows, :] += edge(tile_ref[g, rows, :], outer, sign, bd)
    tiles = [tile_ref[g, pl.ds(base + 8 * t, 8), :] for t in range(8)]
    total = [state_ref[g, pl.ds(base + 8 * t, 8), :] for t in range(8)]
    bg, bd = coefs(2)
    for h in range(2):
        for f, k, sign in ((4, 0, bg), (5, 3, -bg)):
            outer = outside_ref[f, pl.ds(face + 8 * h, 8), cols]
            total[2 * k + h] += edge(tiles[2 * k + h], outer, sign, bd)
    bg, bd = coefs(1)
    bgs = jnp.where(low, bg, -bg)
    outer_l = [outside_ref[2, pl.ds(face + 8 * h, 8), cols] for h in range(2)]
    outer_r = [outside_ref[3, pl.ds(face + 8 * h, 8), cols] for h in range(2)]
    for k in range(4):
        ol = outer_l[k // 2]
        orr = outer_r[k // 2]
        outer = jnp.where(low, ol, turn(orr)) if k % 2 == 0 else jnp.where(low, turn(ol), orr)
        bound = edge(jnp.where(low, tiles[2 * k], tiles[2 * k + 1]), outer, bgs, bd)
        total[2 * k] += jnp.where(low, bound, 0.0)
        total[2 * k + 1] += jnp.where(low, 0.0, bound)
    for t in range(4):
        high, rest = split2(jnp.concatenate(total[2 * t : 2 * t + 2], axis=0))
        up_ref[base + 16 * t : base + 16 * t + 16, cols] = high
        up_ref[ROWS + base + 16 * t : ROWS + base + 16 * t + 16, cols] = rest


def refine_tables(flag_ref, jac_ref, start_ref, aux_ref):
    flags = flag_ref[...].astype(F32)
    wide = jnp.broadcast_to(flags, (LANES, E_DEV)).astype(BF16)
    row = lax.broadcasted_iota(jnp.int32, (E_DEV, E_DEV), 0)
    col = lax.broadcasted_iota(jnp.int32, (E_DEV, E_DEV), 1)
    ahead = jnp.where(col < row, 1.0, 0.0).astype(BF16)
    within = jnp.where(col <= row, 1.0, 0.0).astype(BF16)
    dims = (((1,), (1,)), ((), ()))
    place = lax.broadcasted_iota(jnp.int32, (E_DEV, LANES), 0).astype(F32)
    start_ref[0] = place + 7.0 * lax.dot_general(ahead, wide, dims, preferred_element_type=F32)
    start_ref[1] = (
        place + 1.0 + 7.0 * lax.dot_general(within, wide, dims, preferred_element_type=F32)
    )
    count = lax.dot_general(wide[0:16], ahead, dims, preferred_element_type=F32)[0:1]
    at = lax.broadcasted_iota(jnp.int32, (1, E_DEV), 1).astype(F32) + 7.0 * count
    at_high = jnp.floor(at * (1.0 / 16.0))
    jac = jac_ref[...]
    j0, rest = split2(jac)
    rest = jac - j0.astype(F32)
    j1 = rest.astype(BF16)
    j2 = (rest - j1.astype(F32)).astype(BF16)
    zero = jnp.zeros((10, E_DEV), F32)
    aux_ref[...] = jnp.concatenate(
        [
            at_high, at - 16.0 * at_high, flags, j0.astype(F32), j1.astype(F32), j2.astype(F32),
            zero,
        ],
        axis=0,
    ).astype(BF16)


def column_tables(tile, first, start_ref, aux_ref, coef_ref, hot_ref):
    place = lax.broadcasted_iota(jnp.int32, (1, LANES), 1).astype(F32) + first
    inside = (place >= start_ref[0]) & (place < start_ref[1])
    hot = jnp.where(inside, 1.0, 0.0).astype(BF16)
    cols = pl.ds(pl.multiple_of((tile % 2) * LANES, LANES), LANES)
    hot_ref[tile // 2, :, cols] = hot
    aux = jnp.dot(aux_ref[...], hot, preferred_element_type=F32)
    child = place - (16.0 * aux[0:1] + aux[1:2])
    refined = aux[2:3] > 0.5
    z = child >= 4.0
    child = child - jnp.where(z, 4.0, 0.0)
    y = child >= 2.0
    child = child - jnp.where(y, 2.0, 0.0)
    x = child >= 1.0
    jac = (aux[3:4] + aux[4:5] + aux[5:6]) * jnp.where(refined, 2.0, 1.0)

    def table(bit):
        return [
            [
                rows8(
                    jnp.where(
                        refined,
                        jnp.where(bit, float(SIDES[1][i, m]), float(SIDES[0][i, m])),
                        1.0 if i == m else 0.0,
                    )
                )
                for m in range(4)
            ]
            for i in range(4)
        ]

    cx, cy, cz = table(x), table(y), table(z)
    low = low_half((8, LANES))
    n = 0
    for i in range(4):
        for m in range(4):
            coef_ref[tile, n] = cx[i][m]
            coef_ref[tile, 16 + n] = cz[i][m]
            n += 1
    order = [(0, 1), (1, 0), (2, 3), (3, 2)]
    for at, (first_j, last_j) in enumerate(((0, 1), (2, 3))):
        for k, (lo_m, hi_m) in enumerate(order):
            coef_ref[tile, 32 + 4 * at + k] = jnp.where(low, cy[first_j][lo_m], cy[last_j][hi_m])
    return jac


def combine4(c, u):
    return (c[0] * u[0] + c[1] * u[1]) + (c[2] * u[2] + c[3] * u[3])


def interpolate(v, tile, half, pick_ref, coef_ref, line_ref, put):
    base = 64 * v
    cols = slice(half * LANES, half * LANES + LANES)
    tiles = [
        pick_ref[base + 8 * t : base + 8 * t + 8, cols]
        + pick_ref[ROWS + base + 8 * t : ROWS + base + 8 * t + 8, cols]
        for t in range(8)
    ]
    mid = [None] * 8
    for h in range(2):
        u = [tiles[2 * k + h] for k in range(4)]
        for k in range(4):
            mid[2 * k + h] = combine4([coef_ref[tile, 16 + 4 * k + m] for m in range(4)], u)
    for k in range(4):
        a, b = mid[2 * k], mid[2 * k + 1]
        u = [a, turn(a), b, turn(b)]
        for at in range(2):
            line_ref[v, 16 * k + 8 * at : 16 * k + 8 * at + 8, :] = combine4(
                [coef_ref[tile, 32 + 4 * at + m] for m in range(4)], u
            )
    for h in range(2):
        u = [line_ref[v, pl.ds(32 * h + i, 8, stride=4), :] for i in range(4)]
        for i in range(4):
            put(base + 32 * h + i, combine4([coef_ref[tile, 4 * i + m] for m in range(4)], u))


TILES = 13
FRAME = ROWS + 8
PACKED = ROWS // 4 * 3 + 8


def pack(frame_ref, tile, pack_ref, part):
    lane = lax.broadcasted_iota(jnp.int32, (8, LANES), 1)
    unused = jnp.where(part == 1, lane, LANES - 1 - lane) < 32
    for n in range(ROWS // 32):
        fourth = frame_ref[tile, 32 * n + 24 : 32 * n + 32, :]
        for j in range(3):
            rows = frame_ref[tile, 32 * n + 8 * j : 32 * n + 8 * j + 8, :]
            pack_ref[part, 24 * n + 8 * j : 24 * n + 8 * j + 8, :] = jnp.where(
                unused, pltpu.roll(fourth, 96 - 32 * j, 1), rows
            )
    pack_ref[part, PACKED - 8 : PACKED, :] = frame_ref[tile, ROWS:FRAME, :]


def unpack(land_ref, part, dst_ref, tile):
    lane = lax.broadcasted_iota(jnp.int32, (8, LANES), 1)
    for n in range(ROWS // 32):
        rows = [land_ref[part, 24 * n + 8 * j : 24 * n + 8 * j + 8, :] for j in range(3)]
        turned = [pltpu.roll(rows[j], 32 + 32 * j, 1) for j in range(3)]
        for j in range(3):
            dst_ref[tile, 32 * n + 8 * j : 32 * n + 8 * j + 8, :] = rows[j]
        dst_ref[tile, 32 * n + 24 : 32 * n + 32, :] = jnp.where(
            lane < 32 + 32 * part, turned[0],
            jnp.where(lane < 64 + 32 * part, turned[1], turned[2]),
        )
    dst_ref[tile, ROWS:FRAME, :] = land_ref[part, PACKED - 8 : PACKED, :]


def kernel(
    x_hbm, jac_hbm, speed_hbm, flag_hbm, send_hbm, source_hbm, modes_hbm,
    frame_ref, head_ref, info_ref,
    jac_ref, speed_ref, flag_ref, send_ref, source_ref, modes_ref,
    tile_ref, trace_ref, out_buf, ghost_ref, ghost_bf, outside_ref, rate_ref, state_ref, up_ref,
    start_ref, aux_ref, coef_ref, hot_ref, pick_a, pick_b, line_ref, far_ref, pack_ref, land_ref,
    row_buf, z_buf, y_buf, mine, row_sum, plane_sum, behind_ref,
    small_sems, fetch_sems, send_sems, recv_sems, row_send, row_recv, z_send, z_recv,
    y_send, y_recv,
    head_send, head_recv, tail_send, tail_recv, reply,
):
    me = lax.axis_index("curve")
    devices = ROW_OF * SIDE * SIDE
    row_at = me % ROW_OF
    z_at = me // ROW_OF % SIDE
    y_at = me // (ROW_OF * SIDE)
    near = [(me + devices + o) % devices for o in (-2, -1, 1, 2)]
    row_mates = [me - row_at + (row_at + k) % ROW_OF for k in range(1, ROW_OF)]
    z_mates = [me + ROW_OF * ((z_at + k) % SIDE - z_at) for k in range(1, SIDE)]
    early = me % (ROW_OF * SIDE) < 2
    idle = early | (me % (ROW_OF * SIDE) >= ROW_OF * SIDE - 2)
    awaited = me >= devices - 4
    barrier = pltpu.get_barrier_semaphore()
    for b, partner in enumerate(near):

        @pl.when(me + (-2, -1, 1, 2)[b] < devices)
        def _(partner=partner):
            pl.semaphore_signal(barrier, inc=1, device_id=(partner,), device_id_type=MESH)

    fetches = fetch_state(x_hbm, tile_ref, fetch_sems)
    for partner in row_mates + z_mates:
        pl.semaphore_signal(barrier, inc=1, device_id=(partner,), device_id_type=MESH)
    for k in range(1, SIDE):

        @pl.when(y_at >= k)
        def _(k=k):
            pl.semaphore_signal(
                barrier, inc=1, device_id=(me - k * ROW_OF * SIDE,), device_id_type=MESH
            )

    small = []
    for at, (src, dst) in enumerate(
        (
            (send_hbm, send_ref), (flag_hbm, flag_ref), (source_hbm, source_ref),
            (jac_hbm, jac_ref), (modes_hbm, modes_ref), (speed_hbm, speed_ref),
        )
    ):
        copy = pltpu.make_async_copy(src, dst, small_sems.at[at])
        copy.start()
        small.append(copy)

    def send(src, dst, send_sem, recv_sem, mate):
        copy = remote(src, dst, send_sem, recv_sem, mate)
        copy.start()
        return copy

    def remote(src, dst, send_sem, recv_sem, mate):
        return pltpu.make_async_remote_copy(
            src_ref=src, dst_ref=dst, send_sem=send_sem, recv_sem=recv_sem,
            device_id=(mate,), device_id_type=MESH,
        )

    for g in range(GROUPS):
        fetches[g].wait()
        build_traces(tile_ref, trace_ref, g)
    small[0].wait()
    gather_sends(send_ref, trace_ref, out_buf)
    for copy in small[1:]:
        copy.wait()
    count = jnp.sum(flag_ref[...].astype(F32), axis=1, keepdims=True)
    mine[...] = jnp.broadcast_to(count, (1, LANES)).astype(jnp.int32) - 64
    total_new = 7.0 * jnp.broadcast_to(count, (1, LANES)) + float(E_DEV)

    def near_work():
        outside_near(source_ref, trace_ref, far_ref, outside_ref)
        blend_rates(tile_ref, modes_ref, jac_ref, rate_ref)

    def table_step(tile, carry):
        shift = (jnp.full((1, LANES), tile, jnp.int32) * LANES).astype(F32)
        first = shift - 2.0 * LANES + jnp.where(tile < 2, total_new, 0.0)
        jac_row = rows8(column_tables(tile, first, start_ref, aux_ref, coef_ref, hot_ref))
        frame_ref[jnp.where(tile < 2, TILES + tile, tile), ROWS:FRAME, :] = jac_row
        return carry

    def inner_work():
        def interior_step(n, carry):
            interior_block(n // GROUPS, n % GROUPS, tile_ref, speed_ref, rate_ref, state_ref)
            return carry

        lax.fori_loop(0, VARS * GROUPS, interior_step, 0)
        refine_tables(flag_ref, jac_ref, start_ref, aux_ref)
        lax.fori_loop(0, 4, table_step, 0)

    def own_tables():
        lax.fori_loop(4, TILES, table_step, 0)

    pl.when(jnp.logical_not(awaited))(near_work)
    pl.when(early)(inner_work)
    pl.semaphore_wait(
        barrier, 4 - jnp.maximum(2 - me, 0) + ROW_OF - 1 + SIDE - 1 + SIDE - 1 - y_at
    )
    for b in (2, 3):

        @pl.when(me + b - 1 >= devices)
        def _(b=b):
            pl.semaphore_signal(reply, inc=1, device_id=(near[b],), device_id_type=MESH)

    halo = {
        b: remote(
            out_buf.at[b], ghost_ref.at[3 - b], send_sems.at[b], recv_sems.at[3 - b], near[b]
        )
        for b in (1, 3, 0, 2)
    }
    for b in (1, 3, 0, 2):
        pl.when(me >= 2 - b)(halo[b].start)
    row_copies = [
        send(mine, row_buf.at[k], row_send.at[k], row_recv.at[k], mate)
        for k, mate in enumerate(row_mates)
    ]
    pl.when(awaited)(near_work)
    pl.when(jnp.logical_not(early))(inner_work)
    pl.when(idle)(own_tables)

    @pl.when(me < 2)
    def _():
        pl.semaphore_wait(reply, 2 - me)
        for b in range(2):
            pl.when(me < 2 - b)(halo[b].start)

    def gathered(copies, own_ref, buf_ref, at, sum_ref):
        for copy in copies:
            copy.wait()
        total = own_ref[...]
        behind = behind_ref[...]
        for k in range(len(copies)):
            value = buf_ref[k]
            total = total + value
            behind = behind + jnp.where(at >= k + 1, value, 0)
        sum_ref[...] = total
        behind_ref[...] = behind

    behind_ref[...] = jnp.zeros((1, LANES), jnp.int32)
    z_copies = [
        remote(row_sum, z_buf.at[k], z_send.at[k], z_recv.at[k], mate)
        for k, mate in enumerate(z_mates)
    ]
    y_copies = [
        remote(
            plane_sum, y_buf.at[k - 1], y_send.at[k - 1], y_recv.at[k - 1],
            (me + k * ROW_OF * SIDE) % devices,
        )
        for k in range(1, SIDE)
    ]

    def row_stage():
        gathered(row_copies, mine, row_buf, row_at, row_sum)
        for copy in z_copies:
            copy.start()

    row_stage()
    for b in range(4):
        halo[b].wait_send()
        halo[3 - b].wait_recv()
    split_ghost(ghost_ref, ghost_bf)
    first, last = me == 0, me == devices - 1

    outer_tail = remote(
        frame_ref.at[TILES + 1], frame_ref.at[1], tail_send.at[1], tail_recv.at[1], near[2]
    )
    outer_head = remote(
        frame_ref.at[2], head_ref.at[0], head_send.at[0], head_recv.at[0], near[1]
    )
    inner_tail = remote(
        pack_ref.at[1], land_ref.at[1], tail_send.at[0], tail_recv.at[0], near[2]
    )
    inner_head = remote(
        pack_ref.at[0], land_ref.at[0], head_send.at[1], head_recv.at[1], near[1]
    )

    def fill(dst, tile, half, pick_ref):
        for v in range(VARS):

            def put(row, value):
                frame_ref[dst, pl.ds(row, 8, stride=4), :] = value

            interpolate(v, tile, half, pick_ref, coef_ref, line_ref, put)

    for order in range(2):
        part = me % 2 if order == 0 else 1 - me % 2

        for step in range(2):
            half = jnp.where(part == 1, 1 - step, step)
            group = 2 * part + half
            outside_far(group, far_ref, ghost_bf, outside_ref)

            for v in range(VARS):
                edge_block(
                    v, group, tile_ref, speed_ref, rate_ref, outside_ref, state_ref, up_ref
                )
            within = (
                pl.ds(pl.multiple_of(LANES * group, LANES), LANES)
                if step == 0
                else pl.ds(pl.multiple_of(2 * LANES * part, 2 * LANES), 2 * LANES)
            )
            cols = pl.ds(pl.multiple_of(LANES * half, LANES), LANES)
            pick_a[:, 0:LANES] = jnp.dot(
                up_ref[:, within], hot_ref[1 - part, within, cols], preferred_element_type=F32
            )
            fill(jnp.where(part == 1, TILES, 2) + half, 2 * (1 - part) + half, 0, pick_a)
            if step == 0:
                pl.when((part == 1) & jnp.logical_not(last))(outer_tail.start)
                pl.when((part == 0) & jnp.logical_not(first))(outer_head.start)
            else:
                pack(frame_ref, jnp.where(part == 1, TILES, 3), pack_ref, part)
                pl.when((part == 1) & jnp.logical_not(last))(inner_tail.start)
                pl.when((part == 0) & jnp.logical_not(first))(inner_head.start)

    pl.when(jnp.logical_not(idle))(own_tables)
    gathered(z_copies, row_sum, z_buf, z_at, plane_sum)
    for k in range(1, SIDE):
        pl.when(y_at + k < SIDE)(y_copies[k - 1].start)

    picks = [pick_a, pick_b]
    pick_a[...] = jnp.dot(up_ref[...], hot_ref[2], preferred_element_type=F32)
    for pair in range(2, 7):
        now, later = picks[pair % 2], picks[(pair + 1) % 2]
        if pair < 5:
            later[...] = jnp.dot(up_ref[...], hot_ref[pair + 1], preferred_element_type=F32)
        if pair == 5:
            later[:, 0:LANES] = jnp.dot(
                up_ref[...], hot_ref[6, :, 0:LANES], preferred_element_type=F32
            )
        for half in range(2 if pair < 6 else 1):
            fill(2 * pair + half, 2 * pair + half, half, now)

    behind = behind_ref[...]
    for k in range(1, SIDE):
        pl.when(y_at + k < SIDE)(y_copies[k - 1].wait_send)
        pl.when(y_at >= k)(y_copies[k - 1].wait_recv)
        behind = behind + jnp.where(y_at >= k, y_buf[k - 1], 0)
    info_ref[0:1, :] = behind
    info_ref[1:2, :] = total_new.astype(jnp.int32)

    @pl.when(jnp.logical_not(last))
    def _():
        outer_tail.wait_send()
        inner_tail.wait_send()
        outer_head.wait_recv()
        inner_head.wait_recv()
        unpack(land_ref, 0, head_ref, 1)

    @pl.when(jnp.logical_not(first))
    def _():
        outer_head.wait_send()
        inner_head.wait_send()
        outer_tail.wait_recv()
        inner_tail.wait_recv()
        unpack(land_ref, 1, frame_ref, 0)


CHUNK = 64


def place_kernel(frame_ref, head_ref, info_ref, out_hbm, jac_hbm, out_ref, jac_ref, sems):
    shift = 7 * info_ref[0, 0]
    size = info_ref[1, 0]
    begin = 2 * LANES - shift
    tile = begin // LANES
    turn_by = begin - tile * LANES
    over = -(size + shift)
    head_tile = over // LANES
    head_turn = over - head_tile * LANES
    lane = lax.broadcasted_iota(jnp.int32, (8, LANES), 1)
    kept = lane < LANES - turn_by
    head_kept = lane < LANES - head_turn
    back = (LANES - turn_by) % LANES
    head_back = (LANES - head_turn) % LANES

    def row_tile(rows):
        parts = [pltpu.roll(frame_ref[tile + c, rows, :], back, 1) for c in range(9)]
        out = [jnp.where(kept, parts[c], parts[c + 1]) for c in range(8)]
        heads = [pltpu.roll(head_ref[c, rows, :], head_back, 1) for c in range(2)]
        ends = [
            jnp.where(head_tile + 5 + c == 0, heads[0], jnp.where(head_tile + 5 + c == 1, heads[1], 0.0))
            for c in range(4)
        ]
        for c in range(3):
            out[5 + c] = out[5 + c] + jnp.where(head_kept, ends[c], ends[c + 1])
        return out

    copies = []
    for chunk in range(ROWS // CHUNK):
        for n in range(CHUNK // 8):
            row = chunk * CHUNK + 8 * n
            out = row_tile(pl.ds(row, 8))
            for c in range(7):
                out_ref[row : row + 8, c * LANES : (c + 1) * LANES] = out[c]
            out_ref[row : row + 8, 7 * LANES : E_NEW] = out[7][:, : E_NEW - 7 * LANES]
        rows = pl.ds(chunk * CHUNK, CHUNK)
        copy = pltpu.make_async_copy(out_ref.at[rows], out_hbm.at[rows], sems.at[chunk])
        copy.start()
        copies.append(copy)
    out = row_tile(pl.ds(ROWS, 8))
    for c in range(8):
        width = min(LANES, E_NEW - c * LANES)
        jac_ref[0:1, c * LANES : c * LANES + width] = out[c][0:1, :width]
    copies.append(pltpu.make_async_copy(jac_ref, jac_hbm, sems.at[ROWS // CHUNK]))
    copies[-1].start()
    for copy in copies:
        copy.wait()


def vmem(count):
    return [pl.BlockSpec(memory_space=pltpu.VMEM)] * count


def shards(nodal_state, inverse_jacobian, speeds, refine_flags, send_index, face_source):
    x = nodal_state.reshape(ROWS, E_DEV)
    jac = inverse_jacobian.reshape(1, E_DEV)
    flags = refine_flags.reshape(1, E_DEV)
    dma = pltpu.SemaphoreType.DMA
    frame, head, info = pl.pallas_call(
        kernel,
        out_shape=(
            jax.ShapeDtypeStruct((TILES + 2, FRAME, LANES), F32),
            jax.ShapeDtypeStruct((2, FRAME, LANES), F32),
            jax.ShapeDtypeStruct((2, LANES), jnp.int32),
        ),
        in_specs=[pl.BlockSpec(memory_space=pltpu.HBM)] * 7,
        out_specs=tuple(vmem(3)),
        scratch_shapes=[
            pltpu.VMEM((1, E_DEV), F32),
            pltpu.SMEM((3, VARS), F32),
            pltpu.VMEM((1, E_DEV), jnp.int32),
            pltpu.VMEM((4 * SLOTS,), jnp.int32),
            pltpu.VMEM((6, E_DEV), jnp.int32),
            pltpu.VMEM((64, 64), F32),
            pltpu.VMEM((GROUPS, ROWS, LANES), F32),
            pltpu.VMEM((6, 160, E_DEV), BF16),
            pltpu.VMEM((4, 80, LANES), F32),
            pltpu.VMEM((4, 80, LANES), F32),
            pltpu.VMEM((160, E_DEV), BF16),
            pltpu.VMEM((6, 80, E_DEV), F32),
            pltpu.VMEM((8, E_DEV), F32),
            pltpu.VMEM((GROUPS, ROWS, LANES), F32),
            pltpu.VMEM((2 * ROWS, E_DEV), BF16),
            pltpu.VMEM((2, E_DEV, LANES), F32),
            pltpu.VMEM((16, E_DEV), BF16),
            pltpu.VMEM((TILES, 40, 8, LANES), F32),
            pltpu.VMEM((7, E_DEV, 2 * LANES), BF16),
            pltpu.VMEM((2 * ROWS, 2 * LANES), F32),
            pltpu.VMEM((2 * ROWS, 2 * LANES), F32),
            pltpu.VMEM((VARS, 64, LANES), F32),
            pltpu.VMEM((GROUPS, E_DEV, 6 * LANES), BF16),
            pltpu.VMEM((2, PACKED, LANES), F32),
            pltpu.VMEM((2, PACKED, LANES), F32),
            pltpu.VMEM((ROW_OF - 1, 1, LANES), jnp.int32),
            pltpu.VMEM((SIDE - 1, 1, LANES), jnp.int32),
            pltpu.VMEM((SIDE - 1, 1, LANES), jnp.int32),
            pltpu.VMEM((1, LANES), jnp.int32),
            pltpu.VMEM((1, LANES), jnp.int32),
            pltpu.VMEM((1, LANES), jnp.int32),
            pltpu.VMEM((1, LANES), jnp.int32),
            dma((6,)), dma((GROUPS,)), dma((4,)), dma((4,)), dma((ROW_OF - 1,)),
            dma((ROW_OF - 1,)), dma((SIDE - 1,)), dma((SIDE - 1,)), dma((SIDE - 1,)),
            dma((SIDE - 1,)),
            dma((2,)), dma((2,)), dma((2,)), dma((2,)), pltpu.SemaphoreType.REGULAR,
        ],
        compiler_params=pltpu.CompilerParams(
            collective_id=0, has_side_effects=True, vmem_limit_bytes=28 << 20
        ),
        name="step",
    )(*[
        pltpu.with_memory_space_constraint(a, pltpu.HBM)
        for a in (x, jac, speeds, flags, send_index, face_source, jnp.asarray(MODES, F32))
    ])
    out, out_jac = pl.pallas_call(
        place_kernel,
        out_shape=(
            jax.ShapeDtypeStruct((ROWS, E_NEW), F32),
            jax.ShapeDtypeStruct((1, E_NEW), F32),
        ),
        in_specs=vmem(3),
        out_specs=(
            pl.BlockSpec(memory_space=pltpu.HBM), pl.BlockSpec(memory_space=pltpu.HBM)
        ),
        scratch_shapes=[
            pltpu.VMEM((ROWS, E_NEW), F32), pltpu.VMEM((1, E_NEW), F32), dma((ROWS // CHUNK + 1,))
        ],
        compiler_params=pltpu.CompilerParams(vmem_limit_bytes=16 << 20),
        name="place",
    )(frame, head, info)
    return out.reshape(VARS, 64, E_NEW), out_jac.reshape(E_NEW)


def solution(mesh):
    axis = P("curve")
    wide = P(None, None, "curve")
    return jax.shard_map(
        shards,
        mesh=mesh,
        in_specs=(wide, axis, P(), axis, axis, P(None, "curve")),
        out_specs=(wide, axis),
        check_vma=False,
    )
```

```python
import functools
import math

import jax
import jax.numpy as jnp
import numpy as np
from jax import lax
from jax.experimental import pallas as pl
from jax.experimental.pallas import tpu as pltpu
from jax.sharding import PartitionSpec as P

TIME_STEP = 0.02
VARS = 5
E_DEV = 512
E_NEW = 960
SLOTS = 96
ROWS = 64 * VARS
LANES = 128
GROUPS = E_DEV // LANES
ROW_OF = 8
SIDE = 4
F32 = jnp.float32
BF16 = jnp.bfloat16
MESH = pl.DeviceIdType.MESH


def lagrange_at(points, targets):
    values_at = np.ones((len(targets), 4))
    for basis_id in range(4):
        for partner in range(4):
            if partner != basis_id:
                values_at[:, basis_id] *= (targets - points[partner]) / (
                    points[basis_id] - points[partner]
                )
    return values_at


def tables():
    root = 1.0 / math.sqrt(5.0)
    points = np.array([-1.0, -root, root, 1.0])
    weights = np.array([1.0, 5.0, 5.0, 1.0]) / 6.0
    bary = np.ones(4)
    for a in range(4):
        for b in range(4):
            if a != b:
                bary[a] /= points[a] - points[b]
    deriv = np.zeros((4, 4))
    for a in range(4):
        for b in range(4):
            if a != b:
                deriv[a, b] = bary[b] / bary[a] / (points[a] - points[b])
        deriv[a, a] = -np.sum(deriv[a])
    skew = weights[:, None] * deriv
    legendre = np.stack(
        [points**0, points, 0.5 * (3 * points**2 - 1), 0.5 * (5 * points**3 - 3 * points)], axis=1
    )
    to_modes = np.linalg.inv(legendre)
    sides = [lagrange_at(points, (points - 1.0) / 2.0), lagrange_at(points, (points + 1.0) / 2.0)]
    return skew, np.kron(to_modes, np.kron(to_modes, to_modes)), sides


SKEW, MODES, SIDES = tables()
Q01, Q02, Q03, Q12 = (float(SKEW[0, 1]), float(SKEW[0, 2]), float(SKEW[0, 3]), float(SKEW[1, 2]))
END, MID = 6.0, 1.2


def split2(x):
    high = x.astype(BF16)
    return high, (x - high.astype(F32)).astype(BF16)


def low_half(shape):
    return (lax.broadcasted_iota(jnp.int32, shape, 0) & 7) < 4


def turn(x):
    return pltpu.roll(x, 4, 0)


def fetch_state(x_ref, tile_ref, sems):
    copies = []
    for g in range(GROUPS):
        copy = pltpu.make_async_copy(
            x_ref.at[:, g * LANES : (g + 1) * LANES], tile_ref.at[g], sems.at[g]
        )
        copy.start()
        copies.append(copy)
    return copies


def build_traces(tile_ref, trace_ref, g):
    low = low_half((8, LANES))
    cols = slice(g * LANES, (g + 1) * LANES)
    for v in range(VARS):
        base = 64 * v
        tiles = [tile_ref[g, base + 8 * t : base + 8 * t + 8, :] for t in range(8)]
        first, last = tiles[0::2], tiles[1::2]
        sets = {
            0: [tile_ref[g, pl.ds(base + 32 * h, 8, stride=4), :] for h in range(2)],
            1: [tile_ref[g, pl.ds(base + 32 * h + 3, 8, stride=4), :] for h in range(2)],
            2: [jnp.where(low, first[k], turn(first[k + 1])) for k in (0, 2)],
            3: [jnp.where(low, turn(last[k]), last[k + 1]) for k in (0, 2)],
            4: tiles[0:2],
            5: tiles[6:8],
        }
        for f, rows in sets.items():
            high, rest = split2(jnp.concatenate(rows, axis=0))
            trace_ref[f, 16 * v : 16 * v + 16, cols] = high
            trace_ref[f, 80 + 16 * v : 96 + 16 * v, cols] = rest


def one_hot(index, size, width):
    rows = lax.broadcasted_iota(jnp.int32, (size, width), 0).astype(jnp.int16)
    index = jnp.broadcast_to(index, (16, width)).astype(jnp.int16)
    index = jnp.concatenate([index] * (size // 16), axis=0)
    return jnp.where(
        rows == index, jnp.ones((size, width), BF16), jnp.zeros((size, width), BF16)
    )


def gather_sends(send_ref, trace_ref, out_ref):
    packed = jnp.broadcast_to(send_ref[...].reshape(1, 4 * SLOTS), (8, 4 * SLOTS))
    for pair in range(2):
        moved = [
            packed if block == 0 else pltpu.roll(packed, 4 * SLOTS - SLOTS * block, 1)
            for block in (2 * pair, 2 * pair + 1)
        ]
        index = jnp.concatenate([m[0:1, 0:LANES] for m in moved], axis=1)
        total = jnp.zeros((160, 2 * LANES), F32)
        for f in range(6):
            total = total + jnp.dot(
                trace_ref[f],
                one_hot(index - f * E_DEV, E_DEV, 2 * LANES),
                preferred_element_type=F32,
            )
        total = total[0:80] + total[80:160]
        for half in range(2):
            out_ref[2 * pair + half] = total[:, half * LANES : (half + 1) * LANES]


def pair_sum(ui, um, si, sm):
    return (si + sm) + ui * um


def line_update(u, coef):
    ca, cb, c02, c03, cd = coef
    s = [x * x for x in u]
    m = [jnp.abs(x) for x in u]
    e = []
    for n, c in ((0, ca), (1, cb), (2, ca)):
        g = pair_sum(u[n], u[n + 1], s[n], s[n + 1])
        e.append(c * g - cd * (jnp.maximum(m[n], m[n + 1]) * (u[n + 1] - u[n])))
    r02 = c02 * pair_sum(u[0], u[2], s[0], s[2])
    r13 = c02 * pair_sum(u[1], u[3], s[1], s[3])
    r03 = c03 * pair_sum(u[0], u[3], s[0], s[3])
    t0 = -(e[0] + r02 + r03)
    t1 = e[0] - e[1] - r13
    t2 = e[1] - e[2] + r02
    t3 = e[2] + r13 + r03
    return t0, t1, t2, t3


def edge(u, o, cg, cd):
    g = pair_sum(u, o, u * u, o * o)
    return cg * g - cd * (jnp.maximum(jnp.abs(u), jnp.abs(o)) * (u - o))


def rows8(x):
    return jnp.broadcast_to(x, (8, LANES))


def blend_rates(tile_ref, modes_ref, jac_ref, rate_ref):
    n = lax.broadcasted_iota(jnp.int32, (64, LANES), 0)
    top = ((n & 3) == 3) | ((n & 12) == 12) | (n >= 48)
    for g in range(GROUPS):
        cols = slice(g * LANES, (g + 1) * LANES)
        modal = jnp.dot(
            modes_ref[...], tile_ref[g, 0:64, :], precision=lax.Precision.HIGHEST,
            preferred_element_type=F32,
        )
        energy = modal * modal
        high = jnp.sum(jnp.where(top, energy, 0.0), axis=0, keepdims=True)
        full = jnp.sum(energy, axis=0, keepdims=True)
        ratio = high / (full + 1e-06)
        blend = 0.5 * ratio / (ratio + 0.1)
        step = TIME_STEP * jac_ref[0:1, cols]
        rate_ref[0:1, cols] = step * (1.0 - blend)
        rate_ref[1:2, cols] = step * blend
        rate_ref[2:3, cols] = step


def outside_near(source_ref, trace_ref, far_ref, outside_ref):
    for f in range(6):
        index = source_ref[f : f + 1, :]
        total = jnp.dot(
            trace_ref[f ^ 1],
            one_hot(index - (f ^ 1) * E_DEV, E_DEV, E_DEV),
            preferred_element_type=F32,
        )
        outside_ref[f] = total[0:80] + total[80:160]
        far = index - 6 * E_DEV
        slot = (
            (far >= SLOTS).astype(jnp.int32)
            + (far >= 2 * SLOTS).astype(jnp.int32)
            + (far >= 3 * SLOTS).astype(jnp.int32)
        )
        hot = one_hot(jnp.where(far >= 0, far + (LANES - SLOTS) * slot, -1), E_DEV, E_DEV)
        for g in range(GROUPS):
            far_ref[g, :, f * LANES : (f + 1) * LANES] = hot[:, g * LANES : (g + 1) * LANES]


def split_ghost(ghost_ref, ghost_bf):
    for slot in range(4):
        high, rest = split2(ghost_ref[slot])
        ghost_bf[0:80, slot * LANES : (slot + 1) * LANES] = high
        ghost_bf[80:160, slot * LANES : (slot + 1) * LANES] = rest


def outside_far(group, far_ref, ghost_bf, outside_ref):
    cols = pl.ds(pl.multiple_of(LANES * group, LANES), LANES)
    total = jnp.dot(ghost_bf[...], far_ref[group], preferred_element_type=F32)
    for f in range(6):
        part = slice(f * LANES, (f + 1) * LANES)
        outside_ref[f, :, cols] += total[0:80, part] + total[80:160, part]


def coefs_of(d, v, speed_ref, hi, lo):
    a = speed_ref[d, v]
    third = (a / 3.0) * hi
    sixth = (a / 6.0) * lo
    return [
        rows8(c)
        for c in (
            Q01 * third + sixth, Q12 * third + sixth, Q02 * third, Q03 * third,
            (0.5 * jnp.abs(a)) * lo,
        )
    ]


def interior_block(v, g, tile_ref, speed_ref, rate_ref, state_ref):
    base = pl.multiple_of(64 * v, 64)
    cols = pl.ds(pl.multiple_of(g * LANES, LANES), LANES)
    hi = rate_ref[0:1, cols]
    lo = rate_ref[1:2, cols]
    low = low_half((8, LANES))
    coef = coefs_of(0, v, speed_ref, hi, lo)
    for h in range(2):
        u = [tile_ref[g, pl.ds(base + 32 * h + i, 8, stride=4), :] for i in range(4)]
        t = line_update(u, coef)
        for i, w in enumerate((END, MID, MID, END)):
            state_ref[g, pl.ds(base + 32 * h + i, 8, stride=4), :] = u[i] + w * t[i]
    tiles = [tile_ref[g, pl.ds(base + 8 * t, 8), :] for t in range(8)]
    coef = coefs_of(2, v, speed_ref, hi, lo)
    total = [None] * 8
    for h in range(2):
        t = line_update([tiles[2 * k + h] for k in range(4)], coef)
        for k, w in enumerate((END, MID, MID, END)):
            total[2 * k + h] = w * t[k]
    ca, cb, c02, c03, cd = coefs_of(1, v, speed_ref, hi, lo)
    signed = jnp.where(low, -ca, ca)
    cross = jnp.where(low, -c03, -cb)
    cross_d = jnp.where(low, 0.0, cd)
    wa = jnp.where(low, END, MID)
    wb = jnp.where(low, MID, END)
    for k in range(4):
        a, b = tiles[2 * k], tiles[2 * k + 1]
        at, bt = turn(a), turn(b)
        sa, sb, sat, sbt = a * a, b * b, at * at, bt * bt
        ma, mb, mat, mbt = jnp.abs(a), jnp.abs(b), jnp.abs(at), jnp.abs(bt)
        x1 = signed * pair_sum(a, at, sa, sat) + cd * (jnp.maximum(ma, mat) * (at - a))
        x2 = signed * pair_sum(b, bt, sb, sbt) + cd * (jnp.maximum(mb, mbt) * (bt - b))
        x3 = c02 * pair_sum(a, b, sa, sb)
        x4 = cross * pair_sum(a, bt, sa, sbt) + cross_d * (jnp.maximum(ma, mbt) * (bt - a))
        total[2 * k] += wa * (x1 - x3 + x4)
        total[2 * k + 1] += wb * (x2 + x3 - turn(x4))
    for t in range(8):
        state_ref[g, pl.ds(base + 8 * t, 8), :] += total[t]


def edge_block(v, g, tile_ref, speed_ref, rate_ref, outside_ref, state_ref, up_ref):
    base = 64 * v
    face = 16 * v
    cols = pl.ds(pl.multiple_of(g * LANES, LANES), LANES)
    step = rate_ref[2:3, cols]
    low = low_half((8, LANES))

    def coefs(d):
        a = speed_ref[d, v]
        return rows8((a * (END / 6.0)) * step), rows8((0.5 * END) * jnp.abs(a) * step)

    bg, bd = coefs(0)
    for h in range(2):
        for f, i, sign in ((0, 0, bg), (1, 3, -bg)):
            rows = pl.ds(base + 32 * h + i, 8, stride=4)
            outer = outside_ref[f, pl.ds(face + 8 * h, 8), cols]
            state_ref[g, rows, :] += edge(tile_ref[g, rows, :], outer, sign, bd)
    tiles = [tile_ref[g, pl.ds(base + 8 * t, 8), :] for t in range(8)]
    total = [state_ref[g, pl.ds(base + 8 * t, 8), :] for t in range(8)]
    bg, bd = coefs(2)
    for h in range(2):
        for f, k, sign in ((4, 0, bg), (5, 3, -bg)):
            outer = outside_ref[f, pl.ds(face + 8 * h, 8), cols]
            total[2 * k + h] += edge(tiles[2 * k + h], outer, sign, bd)
    bg, bd = coefs(1)
    bgs = jnp.where(low, bg, -bg)
    outer_l = [outside_ref[2, pl.ds(face + 8 * h, 8), cols] for h in range(2)]
    outer_r = [outside_ref[3, pl.ds(face + 8 * h, 8), cols] for h in range(2)]
    for k in range(4):
        ol = outer_l[k // 2]
        orr = outer_r[k // 2]
        outer = jnp.where(low, ol, turn(orr)) if k % 2 == 0 else jnp.where(low, turn(ol), orr)
        bound = edge(jnp.where(low, tiles[2 * k], tiles[2 * k + 1]), outer, bgs, bd)
        total[2 * k] += jnp.where(low, bound, 0.0)
        total[2 * k + 1] += jnp.where(low, 0.0, bound)
    for t in range(4):
        high, rest = split2(jnp.concatenate(total[2 * t : 2 * t + 2], axis=0))
        up_ref[base + 16 * t : base + 16 * t + 16, cols] = high
        up_ref[ROWS + base + 16 * t : ROWS + base + 16 * t + 16, cols] = rest


def refine_tables(flag_ref, jac_ref, start_ref, aux_ref):
    flags = flag_ref[...].astype(F32)
    wide = jnp.broadcast_to(flags, (LANES, E_DEV)).astype(BF16)
    row = lax.broadcasted_iota(jnp.int32, (E_DEV, E_DEV), 0)
    col = lax.broadcasted_iota(jnp.int32, (E_DEV, E_DEV), 1)
    ahead = jnp.where(col < row, 1.0, 0.0).astype(BF16)
    within = jnp.where(col <= row, 1.0, 0.0).astype(BF16)
    dims = (((1,), (1,)), ((), ()))
    place = lax.broadcasted_iota(jnp.int32, (E_DEV, LANES), 0).astype(F32)
    start_ref[0] = place + 7.0 * lax.dot_general(ahead, wide, dims, preferred_element_type=F32)
    start_ref[1] = (
        place + 1.0 + 7.0 * lax.dot_general(within, wide, dims, preferred_element_type=F32)
    )
    count = lax.dot_general(wide[0:16], ahead, dims, preferred_element_type=F32)[0:1]
    at = lax.broadcasted_iota(jnp.int32, (1, E_DEV), 1).astype(F32) + 7.0 * count
    at_high = jnp.floor(at * (1.0 / 16.0))
    jac = jac_ref[...]
    j0, rest = split2(jac)
    rest = jac - j0.astype(F32)
    j1 = rest.astype(BF16)
    j2 = (rest - j1.astype(F32)).astype(BF16)
    zero = jnp.zeros((10, E_DEV), F32)
    aux_ref[...] = jnp.concatenate(
        [
            at_high, at - 16.0 * at_high, flags, j0.astype(F32), j1.astype(F32), j2.astype(F32),
            zero,
        ],
        axis=0,
    ).astype(BF16)


def column_tables(tile, first, start_ref, aux_ref, coef_ref, hot_ref):
    place = lax.broadcasted_iota(jnp.int32, (1, LANES), 1).astype(F32) + first
    inside = (place >= start_ref[0]) & (place < start_ref[1])
    hot = jnp.where(inside, 1.0, 0.0).astype(BF16)
    cols = pl.ds(pl.multiple_of((tile % 2) * LANES, LANES), LANES)
    hot_ref[tile // 2, :, cols] = hot
    aux = jnp.dot(aux_ref[...], hot, preferred_element_type=F32)
    child = place - (16.0 * aux[0:1] + aux[1:2])
    refined = aux[2:3] > 0.5
    z = child >= 4.0
    child = child - jnp.where(z, 4.0, 0.0)
    y = child >= 2.0
    child = child - jnp.where(y, 2.0, 0.0)
    x = child >= 1.0
    jac = (aux[3:4] + aux[4:5] + aux[5:6]) * jnp.where(refined, 2.0, 1.0)

    def table(bit):
        return [
            [
                rows8(
                    jnp.where(
                        refined,
                        jnp.where(bit, float(SIDES[1][i, m]), float(SIDES[0][i, m])),
                        1.0 if i == m else 0.0,
                    )
                )
                for m in range(4)
            ]
            for i in range(4)
        ]

    cx, cy, cz = table(x), table(y), table(z)
    low = low_half((8, LANES))
    n = 0
    for i in range(4):
        for m in range(4):
            coef_ref[tile, n] = cx[i][m]
            coef_ref[tile, 16 + n] = cz[i][m]
            n += 1
    order = [(0, 1), (1, 0), (2, 3), (3, 2)]
    for at, (first_j, last_j) in enumerate(((0, 1), (2, 3))):
        for k, (lo_m, hi_m) in enumerate(order):
            coef_ref[tile, 32 + 4 * at + k] = jnp.where(low, cy[first_j][lo_m], cy[last_j][hi_m])
    return jac


def combine4(c, u):
    return (c[0] * u[0] + c[1] * u[1]) + (c[2] * u[2] + c[3] * u[3])


def interpolate(v, tile, half, pick_ref, coef_ref, line_ref, put):
    base = 64 * v
    cols = slice(half * LANES, half * LANES + LANES)
    tiles = [
        pick_ref[base + 8 * t : base + 8 * t + 8, cols]
        + pick_ref[ROWS + base + 8 * t : ROWS + base + 8 * t + 8, cols]
        for t in range(8)
    ]
    mid = [None] * 8
    for h in range(2):
        u = [tiles[2 * k + h] for k in range(4)]
        for k in range(4):
            mid[2 * k + h] = combine4([coef_ref[tile, 16 + 4 * k + m] for m in range(4)], u)
    for k in range(4):
        a, b = mid[2 * k], mid[2 * k + 1]
        u = [a, turn(a), b, turn(b)]
        for at in range(2):
            line_ref[v, 16 * k + 8 * at : 16 * k + 8 * at + 8, :] = combine4(
                [coef_ref[tile, 32 + 4 * at + m] for m in range(4)], u
            )
    for h in range(2):
        u = [line_ref[v, pl.ds(32 * h + i, 8, stride=4), :] for i in range(4)]
        for i in range(4):
            put(base + 32 * h + i, combine4([coef_ref[tile, 4 * i + m] for m in range(4)], u))


TILES = 13
FRAME = ROWS + 8
PACKED = ROWS // 4 * 3 + 8


def pack(frame_ref, tile, pack_ref, part):
    lane = lax.broadcasted_iota(jnp.int32, (8, LANES), 1)
    unused = jnp.where(part == 1, lane, LANES - 1 - lane) < 32
    for n in range(ROWS // 32):
        fourth = frame_ref[tile, 32 * n + 24 : 32 * n + 32, :]
        for j in range(3):
            rows = frame_ref[tile, 32 * n + 8 * j : 32 * n + 8 * j + 8, :]
            pack_ref[part, 24 * n + 8 * j : 24 * n + 8 * j + 8, :] = jnp.where(
                unused, pltpu.roll(fourth, 96 - 32 * j, 1), rows
            )
    pack_ref[part, PACKED - 8 : PACKED, :] = frame_ref[tile, ROWS:FRAME, :]


def unpack(land_ref, part, dst_ref, tile):
    lane = lax.broadcasted_iota(jnp.int32, (8, LANES), 1)
    for n in range(ROWS // 32):
        rows = [land_ref[part, 24 * n + 8 * j : 24 * n + 8 * j + 8, :] for j in range(3)]
        turned = [pltpu.roll(rows[j], 32 + 32 * j, 1) for j in range(3)]
        for j in range(3):
            dst_ref[tile, 32 * n + 8 * j : 32 * n + 8 * j + 8, :] = rows[j]
        dst_ref[tile, 32 * n + 24 : 32 * n + 32, :] = jnp.where(
            lane < 32 + 32 * part, turned[0],
            jnp.where(lane < 64 + 32 * part, turned[1], turned[2]),
        )
    dst_ref[tile, ROWS:FRAME, :] = land_ref[part, PACKED - 8 : PACKED, :]


def kernel(
    x_hbm, jac_hbm, speed_hbm, flag_hbm, send_hbm, source_hbm, modes_hbm,
    frame_ref, head_ref, info_ref,
    jac_ref, speed_ref, flag_ref, send_ref, source_ref, modes_ref,
    tile_ref, trace_ref, out_buf, ghost_ref, ghost_bf, outside_ref, rate_ref, state_ref, up_ref,
    start_ref, aux_ref, coef_ref, hot_ref, pick_a, pick_b, line_ref, far_ref, pack_ref, land_ref,
    row_buf, z_buf, y_buf, mine, row_sum, plane_sum, behind_ref,
    small_sems, fetch_sems, send_sems, recv_sems, row_send, row_recv, z_send, z_recv,
    y_send, y_recv,
    head_send, head_recv, tail_send, tail_recv, reply,
):
    me = lax.axis_index("curve")
    devices = ROW_OF * SIDE * SIDE
    row_at = me % ROW_OF
    z_at = me // ROW_OF % SIDE
    y_at = me // (ROW_OF * SIDE)
    near = [(me + devices + o) % devices for o in (-2, -1, 1, 2)]
    row_mates = [me - row_at + (row_at + k) % ROW_OF for k in range(1, ROW_OF)]
    z_mates = [me + ROW_OF * ((z_at + k) % SIDE - z_at) for k in range(1, SIDE)]
    early = me % (ROW_OF * SIDE) < 2
    idle = early | (me % (ROW_OF * SIDE) >= ROW_OF * SIDE - 2)
    awaited = me >= devices - 4
    barrier = pltpu.get_barrier_semaphore()
    for b, partner in enumerate(near):

        @pl.when(me + (-2, -1, 1, 2)[b] < devices)
        def _(partner=partner):
            pl.semaphore_signal(barrier, inc=1, device_id=(partner,), device_id_type=MESH)

    fetches = fetch_state(x_hbm, tile_ref, fetch_sems)
    for partner in row_mates + z_mates:
        pl.semaphore_signal(barrier, inc=1, device_id=(partner,), device_id_type=MESH)
    for k in range(1, SIDE):

        @pl.when(y_at >= k)
        def _(k=k):
            pl.semaphore_signal(
                barrier, inc=1, device_id=(me - k * ROW_OF * SIDE,), device_id_type=MESH
            )

    small = []
    for at, (src, dst) in enumerate(
        (
            (send_hbm, send_ref), (flag_hbm, flag_ref), (source_hbm, source_ref),
            (jac_hbm, jac_ref), (modes_hbm, modes_ref), (speed_hbm, speed_ref),
        )
    ):
        copy = pltpu.make_async_copy(src, dst, small_sems.at[at])
        copy.start()
        small.append(copy)

    def send(src, dst, send_sem, recv_sem, mate):
        copy = remote(src, dst, send_sem, recv_sem, mate)
        copy.start()
        return copy

    def remote(src, dst, send_sem, recv_sem, mate):
        return pltpu.make_async_remote_copy(
            src_ref=src, dst_ref=dst, send_sem=send_sem, recv_sem=recv_sem,
            device_id=(mate,), device_id_type=MESH,
        )

    for g in range(GROUPS):
        fetches[g].wait()
        build_traces(tile_ref, trace_ref, g)
    small[0].wait()
    gather_sends(send_ref, trace_ref, out_buf)
    for copy in small[1:]:
        copy.wait()
    count = jnp.sum(flag_ref[...].astype(F32), axis=1, keepdims=True)
    mine[...] = jnp.broadcast_to(count, (1, LANES)).astype(jnp.int32) - 64
    total_new = 7.0 * jnp.broadcast_to(count, (1, LANES)) + float(E_DEV)

    def near_work():
        outside_near(source_ref, trace_ref, far_ref, outside_ref)
        blend_rates(tile_ref, modes_ref, jac_ref, rate_ref)

    def table_step(tile, carry):
        shift = (jnp.full((1, LANES), tile, jnp.int32) * LANES).astype(F32)
        first = shift - 2.0 * LANES + jnp.where(tile < 2, total_new, 0.0)
        jac_row = rows8(column_tables(tile, first, start_ref, aux_ref, coef_ref, hot_ref))
        frame_ref[jnp.where(tile < 2, TILES + tile, tile), ROWS:FRAME, :] = jac_row
        return carry

    def inner_work():
        def interior_step(n, carry):
            interior_block(n // GROUPS, n % GROUPS, tile_ref, speed_ref, rate_ref, state_ref)
            return carry

        lax.fori_loop(0, VARS * GROUPS, interior_step, 0)
        refine_tables(flag_ref, jac_ref, start_ref, aux_ref)
        lax.fori_loop(0, 4, table_step, 0)

    def own_tables():
        lax.fori_loop(4, TILES, table_step, 0)

    pl.when(jnp.logical_not(awaited))(near_work)
    pl.when(early)(inner_work)
    pl.semaphore_wait(
        barrier, 4 - jnp.maximum(2 - me, 0) + ROW_OF - 1 + SIDE - 1 + SIDE - 1 - y_at
    )
    for b in (2, 3):

        @pl.when(me + b - 1 >= devices)
        def _(b=b):
            pl.semaphore_signal(reply, inc=1, device_id=(near[b],), device_id_type=MESH)

    halo = {
        b: remote(
            out_buf.at[b], ghost_ref.at[3 - b], send_sems.at[b], recv_sems.at[3 - b], near[b]
        )
        for b in (1, 3, 0, 2)
    }
    for b in (1, 3, 0, 2):
        pl.when(me >= 2 - b)(halo[b].start)
    row_copies = [
        send(mine, row_buf.at[k], row_send.at[k], row_recv.at[k], mate)
        for k, mate in enumerate(row_mates)
    ]
    pl.when(awaited)(near_work)
    pl.when(jnp.logical_not(early))(inner_work)
    pl.when(idle)(own_tables)

    @pl.when(me < 2)
    def _():
        pl.semaphore_wait(reply, 2 - me)
        for b in range(2):
            pl.when(me < 2 - b)(halo[b].start)

    def gathered(copies, own_ref, buf_ref, at, sum_ref):
        for copy in copies:
            copy.wait()
        total = own_ref[...]
        behind = behind_ref[...]
        for k in range(len(copies)):
            value = buf_ref[k]
            total = total + value
            behind = behind + jnp.where(at >= k + 1, value, 0)
        sum_ref[...] = total
        behind_ref[...] = behind

    behind_ref[...] = jnp.zeros((1, LANES), jnp.int32)
    z_copies = [
        remote(row_sum, z_buf.at[k], z_send.at[k], z_recv.at[k], mate)
        for k, mate in enumerate(z_mates)
    ]
    y_copies = [
        remote(
            plane_sum, y_buf.at[k - 1], y_send.at[k - 1], y_recv.at[k - 1],
            (me + k * ROW_OF * SIDE) % devices,
        )
        for k in range(1, SIDE)
    ]

    def row_stage():
        gathered(row_copies, mine, row_buf, row_at, row_sum)
        for copy in z_copies:
            copy.start()

    row_stage()
    for b in range(4):
        halo[b].wait_send()
        halo[3 - b].wait_recv()
    split_ghost(ghost_ref, ghost_bf)
    first, last = me == 0, me == devices - 1

    outer_tail = remote(
        frame_ref.at[TILES + 1], frame_ref.at[1], tail_send.at[1], tail_recv.at[1], near[2]
    )
    outer_head = remote(
        frame_ref.at[2], head_ref.at[0], head_send.at[0], head_recv.at[0], near[1]
    )
    inner_tail = remote(
        pack_ref.at[1], land_ref.at[1], tail_send.at[0], tail_recv.at[0], near[2]
    )
    inner_head = remote(
        pack_ref.at[0], land_ref.at[0], head_send.at[1], head_recv.at[1], near[1]
    )

    def fill(dst, tile, half, pick_ref):
        for v in range(VARS):

            def put(row, value):
                frame_ref[dst, pl.ds(row, 8, stride=4), :] = value

            interpolate(v, tile, half, pick_ref, coef_ref, line_ref, put)

    for order in range(2):
        part = me % 2 if order == 0 else 1 - me % 2

        for step in range(2):
            half = jnp.where(part == 1, 1 - step, step)
            group = 2 * part + half
            outside_far(group, far_ref, ghost_bf, outside_ref)

            for v in range(VARS):
                edge_block(
                    v, group, tile_ref, speed_ref, rate_ref, outside_ref, state_ref, up_ref
                )
            within = (
                pl.ds(pl.multiple_of(LANES * group, LANES), LANES)
                if step == 0
                else pl.ds(pl.multiple_of(2 * LANES * part, 2 * LANES), 2 * LANES)
            )
            cols = pl.ds(pl.multiple_of(LANES * half, LANES), LANES)
            pick_a[:, 0:LANES] = jnp.dot(
                up_ref[:, within], hot_ref[1 - part, within, cols], preferred_element_type=F32
            )
            fill(jnp.where(part == 1, TILES, 2) + half, 2 * (1 - part) + half, 0, pick_a)
            if step == 0:
                pl.when((part == 1) & jnp.logical_not(last))(outer_tail.start)
                pl.when((part == 0) & jnp.logical_not(first))(outer_head.start)
            else:
                pack(frame_ref, jnp.where(part == 1, TILES, 3), pack_ref, part)
                pl.when((part == 1) & jnp.logical_not(last))(inner_tail.start)
                pl.when((part == 0) & jnp.logical_not(first))(inner_head.start)

    pl.when(jnp.logical_not(idle))(own_tables)
    gathered(z_copies, row_sum, z_buf, z_at, plane_sum)
    for k in range(1, SIDE):
        pl.when(y_at + k < SIDE)(y_copies[k - 1].start)

    picks = [pick_a, pick_b]
    pick_a[...] = jnp.dot(up_ref[...], hot_ref[2], preferred_element_type=F32)
    for pair in range(2, 7):
        now, later = picks[pair % 2], picks[(pair + 1) % 2]
        if pair < 5:
            later[...] = jnp.dot(up_ref[...], hot_ref[pair + 1], preferred_element_type=F32)
        if pair == 5:
            later[:, 0:LANES] = jnp.dot(
                up_ref[...], hot_ref[6, :, 0:LANES], preferred_element_type=F32
            )
        for half in range(2 if pair < 6 else 1):
            fill(2 * pair + half, 2 * pair + half, half, now)

    behind = behind_ref[...]
    for k in range(1, SIDE):
        pl.when(y_at + k < SIDE)(y_copies[k - 1].wait_send)
        pl.when(y_at >= k)(y_copies[k - 1].wait_recv)
        behind = behind + jnp.where(y_at >= k, y_buf[k - 1], 0)
    info_ref[0:1, :] = behind
    info_ref[1:2, :] = total_new.astype(jnp.int32)

    @pl.when(jnp.logical_not(last))
    def _():
        outer_tail.wait_send()
        inner_tail.wait_send()
        outer_head.wait_recv()
        inner_head.wait_recv()
        unpack(land_ref, 0, head_ref, 1)

    @pl.when(jnp.logical_not(first))
    def _():
        outer_head.wait_send()
        inner_head.wait_send()
        outer_tail.wait_recv()
        inner_tail.wait_recv()
        unpack(land_ref, 1, frame_ref, 0)


CHUNK = 64


def place_kernel(frame_ref, head_ref, info_ref, out_hbm, jac_hbm, out_ref, jac_ref, sems):
    shift = 7 * info_ref[0, 0]
    size = info_ref[1, 0]
    begin = 2 * LANES - shift
    tile = begin // LANES
    turn_by = begin - tile * LANES
    over = -(size + shift)
    head_tile = over // LANES
    head_turn = over - head_tile * LANES
    lane = lax.broadcasted_iota(jnp.int32, (8, LANES), 1)
    kept = lane < LANES - turn_by
    head_kept = lane < LANES - head_turn
    back = (LANES - turn_by) % LANES
    head_back = (LANES - head_turn) % LANES
    picked = [jnp.where(head_kept, head_tile + 5 + c, head_tile + 6 + c) for c in range(3)]
    zeroth = [p == 0 for p in picked]
    oneth = [p == 1 for p in picked]

    def row_tile(rows):
        parts = [pltpu.roll(frame_ref[tile + c, rows, :], back, 1) for c in range(9)]
        out = [jnp.where(kept, parts[c], parts[c + 1]) for c in range(8)]
        heads = [pltpu.roll(head_ref[c, rows, :], head_back, 1) for c in range(2)]
        for c in range(3):
            out[5 + c] += jnp.where(zeroth[c], heads[0], jnp.where(oneth[c], heads[1], 0.0))
        return out

    copies = []
    for chunk in range(ROWS // CHUNK):
        for n in range(CHUNK // 8):
            row = chunk * CHUNK + 8 * n
            out = row_tile(pl.ds(row, 8))
            for c in range(7):
                out_ref[row : row + 8, c * LANES : (c + 1) * LANES] = out[c]
            out_ref[row : row + 8, 7 * LANES : E_NEW] = out[7][:, : E_NEW - 7 * LANES]
        rows = pl.ds(chunk * CHUNK, CHUNK)
        copy = pltpu.make_async_copy(out_ref.at[rows], out_hbm.at[rows], sems.at[chunk])
        copy.start()
        copies.append(copy)
    out = row_tile(pl.ds(ROWS, 8))
    for c in range(8):
        width = min(LANES, E_NEW - c * LANES)
        jac_ref[0:1, c * LANES : c * LANES + width] = out[c][0:1, :width]
    copies.append(pltpu.make_async_copy(jac_ref, jac_hbm, sems.at[ROWS // CHUNK]))
    copies[-1].start()
    for copy in copies:
        copy.wait()


def vmem(count):
    return [pl.BlockSpec(memory_space=pltpu.VMEM)] * count


def shards(nodal_state, inverse_jacobian, speeds, refine_flags, send_index, face_source):
    x = nodal_state.reshape(ROWS, E_DEV)
    jac = inverse_jacobian.reshape(1, E_DEV)
    flags = refine_flags.reshape(1, E_DEV)
    dma = pltpu.SemaphoreType.DMA
    frame, head, info = pl.pallas_call(
        kernel,
        out_shape=(
            jax.ShapeDtypeStruct((TILES + 2, FRAME, LANES), F32),
            jax.ShapeDtypeStruct((2, FRAME, LANES), F32),
            jax.ShapeDtypeStruct((2, LANES), jnp.int32),
        ),
        in_specs=[pl.BlockSpec(memory_space=pltpu.HBM)] * 7,
        out_specs=tuple(vmem(3)),
        scratch_shapes=[
            pltpu.VMEM((1, E_DEV), F32),
            pltpu.SMEM((3, VARS), F32),
            pltpu.VMEM((1, E_DEV), jnp.int32),
            pltpu.VMEM((4 * SLOTS,), jnp.int32),
            pltpu.VMEM((6, E_DEV), jnp.int32),
            pltpu.VMEM((64, 64), F32),
            pltpu.VMEM((GROUPS, ROWS, LANES), F32),
            pltpu.VMEM((6, 160, E_DEV), BF16),
            pltpu.VMEM((4, 80, LANES), F32),
            pltpu.VMEM((4, 80, LANES), F32),
            pltpu.VMEM((160, E_DEV), BF16),
            pltpu.VMEM((6, 80, E_DEV), F32),
            pltpu.VMEM((8, E_DEV), F32),
            pltpu.VMEM((GROUPS, ROWS, LANES), F32),
            pltpu.VMEM((2 * ROWS, E_DEV), BF16),
            pltpu.VMEM((2, E_DEV, LANES), F32),
            pltpu.VMEM((16, E_DEV), BF16),
            pltpu.VMEM((TILES, 40, 8, LANES), F32),
            pltpu.VMEM((7, E_DEV, 2 * LANES), BF16),
            pltpu.VMEM((2 * ROWS, 2 * LANES), F32),
            pltpu.VMEM((2 * ROWS, 2 * LANES), F32),
            pltpu.VMEM((VARS, 64, LANES), F32),
            pltpu.VMEM((GROUPS, E_DEV, 6 * LANES), BF16),
            pltpu.VMEM((2, PACKED, LANES), F32),
            pltpu.VMEM((2, PACKED, LANES), F32),
            pltpu.VMEM((ROW_OF - 1, 1, LANES), jnp.int32),
            pltpu.VMEM((SIDE - 1, 1, LANES), jnp.int32),
            pltpu.VMEM((SIDE - 1, 1, LANES), jnp.int32),
            pltpu.VMEM((1, LANES), jnp.int32),
            pltpu.VMEM((1, LANES), jnp.int32),
            pltpu.VMEM((1, LANES), jnp.int32),
            pltpu.VMEM((1, LANES), jnp.int32),
            dma((6,)), dma((GROUPS,)), dma((4,)), dma((4,)), dma((ROW_OF - 1,)),
            dma((ROW_OF - 1,)), dma((SIDE - 1,)), dma((SIDE - 1,)), dma((SIDE - 1,)),
            dma((SIDE - 1,)),
            dma((2,)), dma((2,)), dma((2,)), dma((2,)), pltpu.SemaphoreType.REGULAR,
        ],
        compiler_params=pltpu.CompilerParams(
            collective_id=0, has_side_effects=True, vmem_limit_bytes=28 << 20
        ),
        name="step",
    )(*[
        pltpu.with_memory_space_constraint(a, pltpu.HBM)
        for a in (x, jac, speeds, flags, send_index, face_source, jnp.asarray(MODES, F32))
    ])
    out, out_jac = pl.pallas_call(
        place_kernel,
        out_shape=(
            jax.ShapeDtypeStruct((ROWS, E_NEW), F32),
            jax.ShapeDtypeStruct((1, E_NEW), F32),
        ),
        in_specs=vmem(3),
        out_specs=(
            pl.BlockSpec(memory_space=pltpu.HBM), pl.BlockSpec(memory_space=pltpu.HBM)
        ),
        scratch_shapes=[
            pltpu.VMEM((ROWS, E_NEW), F32), pltpu.VMEM((1, E_NEW), F32), dma((ROWS // CHUNK + 1,))
        ],
        compiler_params=pltpu.CompilerParams(vmem_limit_bytes=16 << 20),
        name="place",
    )(frame, head, info)
    return out.reshape(VARS, 64, E_NEW), out_jac.reshape(E_NEW)


def solution(mesh):
    axis = P("curve")
    wide = P(None, None, "curve")
    return jax.shard_map(
        shards,
        mesh=mesh,
        in_specs=(wide, axis, P(), axis, axis, P(None, "curve")),
        out_specs=(wide, axis),
        check_vma=False,
    )
```
